32 devices in a mesh: dp: 4 (over y, core), seq: 8 (over z, x).
Axes of the slice: x: 2, y: 2, z: 4, core: 2. Of those that a mesh axis runs over, the one named last changes fastest.
Arguments:
- inputs: bfloat16 [2, 1024, 4, 1280], P(None, 'seq', 'dp'), may hold values from -6 to 6
- cotangent: bfloat16 [2, 1024, 4, 1280], P(None, 'seq', 'dp'), may hold values from -6 to 6
- attention_gain: bfloat16 [1280], P(('dp', 'seq')), may hold values from 0.5 to 1.5
- query_weight: bfloat16 [1280, 1280], P(('dp', 'seq')), may hold values from -0.15625 to 0.15625
- query_bias: bfloat16 [1280], P(('dp', 'seq')), may hold values from -3 to 3
- key_weight: bfloat16 [1280, 1280], P(('dp', 'seq')), may hold values from -0.15625 to 0.15625
- value_weight: bfloat16 [1280, 1280], P(('dp', 'seq')), may hold values from -0.15625 to 0.15625
- value_bias: bfloat16 [1280], P(('dp', 'seq')), may hold values from -3 to 3
- output_weight: bfloat16 [1280, 1280], P(('dp', 'seq')), may hold values from -1.25 to 1.25
- output_bias: bfloat16 [1280], P(('dp', 'seq')), may hold values from -3 to 3
- feedforward_gain: bfloat16 [1280], P(('dp', 'seq')), may hold values from 0.5 to 1.5
- hidden_weight: bfloat16 [1280, 1280], P(('dp', 'seq')), may hold values from -0.15625 to 0.15625
- hidden_bias: bfloat16 [1280], P(('dp', 'seq')), may hold values from -3 to 3
- project_weight: bfloat16 [1280, 1280], P(('dp', 'seq')), may hold values from -0.15625 to 0.15625
- project_bias: bfloat16 [1280], P(('dp', 'seq')), may hold values from -3 to 3
- depth_scale: bfloat16 [80], replicated, may hold values from -1 to 1
Outputs:
- outputs: bfloat16 [2, 1024, 4, 1280], P(None, 'seq', 'dp')
- inputs_gradient: bfloat16 [2, 1024, 4, 1280], P(None, 'seq', 'dp')
- attention_gain_gradient: float32 [1280], P(('dp', 'seq'))
- query_weight_gradient: float32 [1280, 1280], P(('dp', 'seq'))
- query_bias_gradient: float32 [1280], P(('dp', 'seq'))
- key_weight_gradient: float32 [1280, 1280], P(('dp', 'seq'))
- value_weight_gradient: float32 [1280, 1280], P(('dp', 'seq'))
- value_bias_gradient: float32 [1280], P(('dp', 'seq'))
- output_weight_gradient: float32 [1280, 1280], P(('dp', 'seq'))
- output_bias_gradient: float32 [1280], P(('dp', 'seq'))
- feedforward_gain_gradient: float32 [1280], P(('dp', 'seq'))
- hidden_weight_gradient: float32 [1280, 1280], P(('dp', 'seq'))
- hidden_bias_gradient: float32 [1280], P(('dp', 'seq'))
- project_weight_gradient: float32 [1280, 1280], P(('dp', 'seq'))
- project_bias_gradient: float32 [1280], P(('dp', 'seq'))
- depth_scale_gradient: float32 [80], replicated
The draws below stay inside these ranges and needn't reach their ends.
All inputs are finite; a program needn't handle non-finite values.
Results may differ from the reference program's by a relative error of at most 0.019.
Values may be sent and summed in bfloat16 or wider, within the bound.
A program may use at most 256 MiB of HBM per device.

```python
import math
import jax
import jax.numpy as jnp
from jax import lax

D = 1280
HEADS = 16
HEAD_DIM = 80
FF = 1280
ATT_BLOCK = 256
MB = 2
LEN = 1024
SEQ_ALL = 4


def block_scale(stream_key, dims, split, least, top_value):
    level = 1.0
    for axis_at, parts in split:
        steps = jax.random.uniform(jax.random.fold_in(jax.random.fold_in(stream_key, 6), axis_at), (parts,), jnp.float32, least / len(split), top_value / len(split))
        level = level * jnp.repeat(jnp.exp(steps), dims[axis_at] // parts).reshape((-1,) + (1,) * (len(dims) - 1 - axis_at))
    return level


def noise(own_key, extent, width, most, cuts=(), held_as=jnp.bfloat16):
    array = jax.random.normal(own_key, extent, jnp.float32) * width
    if len(cuts) > 0:
        array = block_scale(own_key, extent, cuts, -0.22, 0.18) * array
    return jnp.clip(array, min=-most, max=most).astype(held_as)


def setup_inputs(seed: int = 0) -> dict:
    key_of = jax.random.split(jax.random.key(seed), 17)
    inputs = noise(key_of[0], (MB, LEN, SEQ_ALL, D), 1.0, 6.0, ((1, 8), (2, 4)))
    cotangent = noise(key_of[1], (MB, LEN, SEQ_ALL, D), 1.0, 6.0, ((1, 8), (2, 4)))
    attention_gain = jnp.clip(1.0 + 0.1 * jax.random.normal(key_of[2], (D,), jnp.float32), 0.5, 1.5).astype(jnp.bfloat16)
    query_weight = noise(key_of[3], (D, D), D ** -0.5, 0.15625, ((0, 32),))
    query_bias = noise(key_of[4], (D,), 0.5, 3.0, ((0, 32),))
    key_weight = noise(key_of[5], (D, D), D ** -0.5, 0.15625, ((0, 32),))
    value_weight = noise(key_of[6], (D, D), D ** -0.5, 0.15625, ((0, 32),))
    value_bias = noise(key_of[7], (D,), 0.5, 3.0, ((0, 32),))
    output_weight = noise(key_of[8], (D, D), (max(1, D * 16 // LEN)) ** -0.5, 1.25, ((0, 32),))
    output_bias = noise(key_of[9], (D,), 0.5, 3.0, ((0, 32),))
    feedforward_gain = jnp.clip(1.0 + 0.1 * jax.random.normal(key_of[10], (D,), jnp.float32), 0.5, 1.5).astype(jnp.bfloat16)
    hidden_weight = noise(key_of[11], (D, FF), D ** -0.5, 0.15625, ((0, 32),))
    hidden_bias = noise(key_of[12], (FF,), 0.5, 3.0, ((0, 32),))
    project_weight = noise(key_of[13], (FF, D), FF ** -0.5, 0.15625, ((0, 32),))
    project_bias = noise(key_of[14], (D,), 0.5, 3.0, ((0, 32),))
    depth_scale = jnp.clip(jax.random.uniform(key_of[15], (HEAD_DIM,), jnp.float32, -1.0, 1.0), -1.0, 1.0).astype(jnp.bfloat16)
    return {"inputs": inputs, "cotangent": cotangent, "attention_gain": attention_gain, "query_weight": query_weight, "query_bias": query_bias, "key_weight": key_weight, "value_weight": value_weight, "value_bias": value_bias, "output_weight": output_weight, "output_bias": output_bias, "feedforward_gain": feedforward_gain, "hidden_weight": hidden_weight, "hidden_bias": hidden_bias, "project_weight": project_weight, "project_bias": project_bias, "depth_scale": depth_scale}


HIGH = lax.Precision.HIGHEST
SOFT_BASE = 1.442695041
EPSILON = 1e-06

@jax.custom_vjp
def low(v):
    return lax.optimization_barrier(v.astype(jnp.bfloat16)).astype(jnp.float32)

@jax.custom_vjp
def low_back(v):
    return v

def low_keep(v):
    return (low(v), None)

def low_pass(kept, grad):
    return (grad,)

def back_keep(v):
    return (v, None)

def back_low(kept, grad):
    return (low(grad),)
low.defvjp(low_keep, low_pass)
low_back.defvjp(back_keep, back_low)

def matmul(left, right):
    return jnp.dot(left, right, precision=HIGH)

def rms_norm(values, gain):
    scale = lax.rsqrt(lax.optimization_barrier(jnp.mean(values * values, axis=-1, keepdims=True)) + EPSILON)
    return values * scale * gain

def attention(queries, keys, values):
    seqs = queries.shape[0]
    length = queries.shape[1]
    block_rows = min(512, length)
    count = length // block_rows
    query_blocks = queries.reshape(seqs, count, block_rows, HEADS, HEAD_DIM).transpose(1, 0, 2, 3, 4)
    key_heads = keys.reshape(seqs, length, HEADS, HEAD_DIM)
    value_heads = values.reshape(seqs, length, HEADS, HEAD_DIM)
    starts = jnp.arange(count, dtype=jnp.int32) * block_rows

    def one_block(pair):
        block, start = pair
        scores = low_back(jnp.einsum('sqhd,skhd->shqk', block, key_heads, precision=HIGH))
        query_place = start + jnp.arange(block_rows, dtype=jnp.int32)
        key_place = jnp.arange(length, dtype=jnp.int32)
        allowed = key_place[None, :] // ATT_BLOCK <= query_place[:, None] // ATT_BLOCK
        weights = jnp.where(allowed[None, None], jnp.exp(scores), 0.0)
        total = lax.optimization_barrier(jnp.sum(weights, axis=-1))
        numer = low_back(jnp.einsum('shqk,skhd->sqhd', low(weights), value_heads, precision=HIGH))
        return numer / jnp.transpose(total, (0, 2, 1))[..., None]
    blocks = lax.map(jax.checkpoint(one_block), (query_blocks, starts))
    return blocks.transpose(1, 0, 2, 3, 4).reshape(seqs, length, HEADS * HEAD_DIM)

def layer(params, inputs):
    norm_one, query_mat, query_add, key_mat, value_mat, value_add, output_mat, output_add, norm_two, hidden_mat, hidden_add, project_mat, project_add, depth = params
    normed = low(rms_norm(inputs, norm_one))
    query_pre = low_back(matmul(normed, query_mat) + query_add)
    rate = jnp.tile(SOFT_BASE / math.sqrt(HEAD_DIM) * jax.nn.softplus(depth), HEADS)
    queries = low(query_pre * rate)
    keys = low_back(low(matmul(normed, key_mat)))
    values = low_back(low(matmul(normed, value_mat) + value_add))
    attended = attention(queries, keys, values)
    mixed = low_back(low(attended))
    residual = inputs + low_back(matmul(mixed, output_mat) + output_add)
    second = low(rms_norm(residual, norm_two))
    hidden_pre = low_back(matmul(second, hidden_mat) + hidden_add)
    active = low(jax.nn.silu(hidden_pre))
    return residual + (matmul(active, project_mat) + project_add)

def reference(inputs, cotangent, attention_gain, query_weight, query_bias, key_weight, value_weight, value_bias, output_weight, output_bias, feedforward_gain, hidden_weight, hidden_bias, project_weight, project_bias, depth_scale):
    params = tuple((p.astype(jnp.float32) for p in (attention_gain, query_weight, query_bias, key_weight, value_weight, value_bias, output_weight, output_bias, feedforward_gain, hidden_weight, hidden_bias, project_weight, project_bias, depth_scale)))
    groups = MB * SEQ_ALL // 2
    sources = inputs.astype(jnp.float32).transpose(0, 2, 1, 3).reshape(groups, 2, LEN, D)
    slopes = cotangent.astype(jnp.float32).transpose(0, 2, 1, 3).reshape(groups, 2, LEN, D)

    def step(totals, pair):
        source, slope = pair
        result, pull = jax.vjp(layer, params, source)
        param_grads, source_grad = pull(slope)
        totals = jax.tree.map(jnp.add, totals, param_grads)
        return (totals, (result.astype(jnp.bfloat16), source_grad.astype(jnp.bfloat16)))
    zeros = tuple((jnp.zeros_like(p) for p in params))
    grads, (results, source_grads) = lax.scan(step, zeros, (sources, slopes))
    results = results.reshape(MB, SEQ_ALL, LEN, D).transpose(0, 2, 1, 3)
    source_grads = source_grads.reshape(MB, SEQ_ALL, LEN, D).transpose(0, 2, 1, 3)
    return (results, source_grads, grads[0], grads[1], grads[2], grads[3], grads[4], grads[5], grads[6], grads[7], grads[8], grads[9], grads[10], grads[11], grads[12], grads[13])
```

```python
import functools
import itertools
import math

import jax
import jax.numpy as jnp
from jax import lax
from jax.experimental import pallas as pl
from jax.experimental.pallas import tpu as pltpu
from jax.sharding import PartitionSpec as P

HEADS = 16
HEAD_DIM = 80
ATT_BLOCK = 256
SOFT_BASE = 1.442695041
EPSILON = 1e-06
MESH = pl.DeviceIdType.MESH
VMEM_BYTES = 60 * 1024 * 1024


class Place:
    def __init__(self, dp, seq):
        self.cores = 2 if dp % 2 == 0 else 1
        self.lines = dp // self.cores
        self.levels = 4 if seq % 4 == 0 else seq
        self.across = seq // self.levels
        self.sizes = {
            "y": self.lines,
            "c": self.cores,
            "z": self.levels,
            "x": self.across,
        }

    def here(self):
        dp = lax.axis_index("dp")
        seq = lax.axis_index("seq")
        return {
            "y": dp // self.cores,
            "c": dp % self.cores,
            "z": seq // self.across,
            "x": seq % self.across,
        }

    def shift(self, spot, axis, step):
        moved = dict(spot)
        moved[axis] = lax.rem(spot[axis] + step, self.sizes[axis])
        return moved

    def device(self, spot):
        return (
            spot["y"] * self.cores + spot["c"],
            spot["z"] * self.across + spot["x"],
        )

    def grid(self):
        return (self.lines, self.cores, self.levels, self.across)

    def copies(self, halves):
        sizes = self.sizes
        return (sizes["z"] - 1) + halves * (sizes["x"] + sizes["y"] + sizes["c"] - 3)

    def greet(self, spot):
        barrier = pltpu.get_barrier_semaphore()
        count = 0
        for axis in "zxyc":
            for step in range(1, self.sizes[axis]):
                pl.semaphore_signal(
                    barrier,
                    inc=1,
                    device_id=self.device(self.shift(spot, axis, step)),
                    device_id_type=MESH,
                )
                count += 1
        pl.semaphore_wait(barrier, count)


def halves_of(cols):
    if cols % 256 == 0:
        return ((slice(0, cols // 2), "xy"), (slice(cols // 2, cols), "yx"))
    return ((slice(0, cols), "xy"),)


class Sender:
    def __init__(self, place, spot, send_sem, recv_sem):
        self.place = place
        self.spot = spot
        self.send_sem = send_sem
        self.recv_sem = recv_sem
        self.count = itertools.count()
        self.open = {}
        self.every = []

    def go(self, key, axis, source, target):
        made = []
        for step in range(1, self.place.sizes[axis]):
            at = next(self.count)
            peer = self.place.shift(self.spot, axis, step)
            copy = pltpu.make_async_remote_copy(
                src_ref=source(peer),
                dst_ref=target(step),
                send_sem=self.send_sem.at[at],
                recv_sem=self.recv_sem.at[at],
                device_id=self.place.device(peer),
                device_id_type=MESH,
            )
            copy.start()
            made.append(copy)
        self.open[key] = made
        self.every.extend(made)

    def landed(self, key):
        for copy in self.open[key]:
            copy.wait_recv()

    def finish(self):
        for copy in self.every:
            copy.wait_send()


def gather_kernel(place, count, *refs):
    shards, wholes = refs[:count], refs[count : 2 * count]
    own_sem, send_sem, recv_sem = refs[2 * count :]
    spot = place.here()
    y, c, z, x = (spot[k] for k in "yczx")
    own = []
    for n in range(count):
        copy = pltpu.make_async_copy(shards[n], wholes[n].at[y, c, z, x], own_sem.at[n])
        copy.start()
        own.append(copy)
    place.greet(spot)
    out = Sender(place, spot, send_sem, recv_sem)

    def one(n):
        part = wholes[n].at[y, c, z, x]
        out.go((n, "z"), "z", lambda peer: shards[n], lambda step: part)

    def two(n):
        out.landed((n, "z"))
        own[n].wait()
        for half, (cols, order) in enumerate(halves_of(shards[n].shape[-1])):
            part = wholes[n].at[y, c, :, x, :, cols]
            out.go((n, half, 2), order[0], lambda peer: part, lambda step: part)

    def three(n):
        for half, (cols, order) in enumerate(halves_of(shards[n].shape[-1])):
            out.landed((n, half, 2))
            if order == "xy":
                part = wholes[n].at[y, c, :, :, :, cols]
            else:
                part = wholes[n].at[:, c, :, x, :, cols]
            out.go((n, half, 3), order[1], lambda peer: part, lambda step: part)

    def four(n):
        for half, (cols, order) in enumerate(halves_of(shards[n].shape[-1])):
            out.landed((n, half, 3))
            part = wholes[n].at[:, c, :, :, :, cols]
            out.go((n, half, 4), "c", lambda peer: part, lambda step: part)

    def five(n):
        for half in range(len(halves_of(shards[n].shape[-1]))):
            out.landed((n, half, 4))

    ahead = 2
    for n in range(min(ahead, count)):
        one(n)
    for step in range(count + 3):
        if step < count:
            two(step)
        if step + ahead < count:
            one(step + ahead)
        for stage, late in ((three, 1), (four, 2), (five, 3)):
            if 0 <= step - late < count:
                stage(step - late)
    out.finish()


def gather_whole(place, shards, collective_id):
    count = len(shards)
    copies = sum(place.copies(len(halves_of(s.shape[-1]))) for s in shards)
    return pl.pallas_call(
        functools.partial(gather_kernel, place, count),
        out_shape=[jax.ShapeDtypeStruct(place.grid() + s.shape, s.dtype) for s in shards],
        in_specs=[pl.BlockSpec(memory_space=pl.ANY)] * count,
        out_specs=[pl.BlockSpec(memory_space=pl.ANY)] * count,
        scratch_shapes=[
            pltpu.SemaphoreType.DMA((count,)),
            pltpu.SemaphoreType.DMA((copies,)),
            pltpu.SemaphoreType.DMA((copies,)),
        ],
        compiler_params=pltpu.CompilerParams(
            collective_id=collective_id, has_side_effects=True
        ),
        name="gather_whole",
    )(*shards)


def scatter_kernel(place, count, *refs):
    parts, totals = refs[:count], refs[count : 2 * count]
    rest = list(refs[2 * count :])
    sums = [rest.pop(0) for _ in range(count)]
    cores = [rest.pop(0) for _ in range(count)]
    seconds, thirds, fourths = [], [], []
    for n in range(count):
        halves = halves_of(parts[n].shape[-1])
        seconds.append([rest.pop(0) for _ in halves])
        thirds.append([rest.pop(0) for _ in halves])
        fourths.append(rest.pop(0))
    own_sem, send_sem, recv_sem = rest
    spot = place.here()
    y, c, z, x = (spot[k] for k in "yczx")
    own = []
    for n in range(count):
        copy = pltpu.make_async_copy(parts[n].at[:, c], sums[n], own_sem.at[n])
        copy.start()
        own.append(copy)
    place.greet(spot)
    out = Sender(place, spot, send_sem, recv_sem)
    lines, _, levels, across = place.grid()

    def total(values):
        result = values[0].astype(jnp.float32)
        for value in values[1:]:
            result = result + value.astype(jnp.float32)
        return result

    def one(n):
        out.go(
            (n, 1), "c", lambda peer: parts[n].at[:, peer["c"]], lambda step: cores[n]
        )

    def two(n):
        own[n].wait()
        out.landed((n, 1))
        if place.cores > 1:

            @pl.loop(0, lines * levels * across)
            def _(at):
                where = (at // (levels * across), (at // across) % levels, at % across)
                sums[n][where] = total([sums[n][where], cores[n][where]]).astype(
                    sums[n].dtype
                )

        for half, (cols, order) in enumerate(halves_of(parts[n].shape[-1])):
            if order == "xy":
                out.go(
                    (n, half, 2),
                    "y",
                    lambda peer: sums[n].at[peer["y"], :, :, :, cols],
                    lambda step: seconds[n][half].at[step - 1],
                )
            else:
                out.go(
                    (n, half, 2),
                    "x",
                    lambda peer: sums[n].at[:, :, peer["x"], :, cols],
                    lambda step: seconds[n][half].at[step - 1],
                )

    def three(n):
        for half, (cols, order) in enumerate(halves_of(parts[n].shape[-1])):
            out.landed((n, half, 2))
            box = seconds[n][half]
            if order == "xy":

                @pl.loop(0, levels * across)
                def _(at):
                    zz, xx = at // across, at % across
                    values = [sums[n][y, zz, xx, :, cols]]
                    values += [box[k, zz, xx] for k in range(lines - 1)]
                    sums[n][y, zz, xx, :, cols] = total(values).astype(sums[n].dtype)

                out.go(
                    (n, half, 3),
                    "x",
                    lambda peer: sums[n].at[y, :, peer["x"], :, cols],
                    lambda step: thirds[n][half].at[step - 1],
                )
            else:

                @pl.loop(0, lines * levels)
                def _(at):
                    yy, zz = at // levels, at % levels
                    values = [sums[n][yy, zz, x, :, cols]]
                    values += [box[k, yy, zz] for k in range(across - 1)]
                    sums[n][yy, zz, x, :, cols] = total(values).astype(sums[n].dtype)

                out.go(
                    (n, half, 3),
                    "y",
                    lambda peer: sums[n].at[peer["y"], :, x, :, cols],
                    lambda step: thirds[n][half].at[step - 1],
                )

    def four(n):
        for half, (cols, order) in enumerate(halves_of(parts[n].shape[-1])):
            out.landed((n, half, 3))
            box = thirds[n][half]

            @pl.loop(0, levels)
            def _(zz):
                values = [sums[n][y, zz, x, :, cols]]
                values += [box[k, zz] for k in range(box.shape[0])]
                sums[n][y, zz, x, :, cols] = total(values).astype(sums[n].dtype)

        out.go(
            (n, 4),
            "z",
            lambda peer: sums[n].at[y, peer["z"], x],
            lambda step: fourths[n].at[step - 1],
        )

    def five(n):
        out.landed((n, 4))
        values = [sums[n][y, z, x]] + [fourths[n][k] for k in range(levels - 1)]
        totals[n][...] = total(values)

    for step in range(count + 4):
        for stage, late in ((one, 0), (two, 1), (three, 2), (four, 3), (five, 4)):
            if 0 <= step - late < count:
                stage(step - late)
    out.finish()


def scatter_sum(place, parts, collective_id):
    count = len(parts)
    lines, cores, levels, across = place.grid()
    boxes = []
    copies = 0
    for p in parts:
        rows, cols = p.shape[-2:]
        halves = halves_of(cols)
        copies += (levels - 1) + (cores - 1) + len(halves) * (lines + across - 2)
        for piece, order in halves:
            wide = piece.stop - piece.start
            first = (lines - 1, levels, across) if order == "xy" else (across - 1, lines, levels)
            later = (across - 1, levels) if order == "xy" else (lines - 1, levels)
            boxes.append(pltpu.VMEM(first + (rows, wide), p.dtype))
            boxes.append(pltpu.VMEM(later + (rows, wide), p.dtype))
        if len(halves) == 2:
            boxes[-3], boxes[-2] = boxes[-2], boxes[-3]
        boxes.append(pltpu.VMEM((levels - 1, rows, cols), p.dtype))
    block = [pltpu.VMEM((lines, levels, across) + p.shape[-2:], p.dtype) for p in parts]
    return pl.pallas_call(
        functools.partial(scatter_kernel, place, count),
        out_shape=[jax.ShapeDtypeStruct(p.shape[-2:], jnp.float32) for p in parts],
        in_specs=[pl.BlockSpec(memory_space=pl.ANY)] * count,
        out_specs=[pl.BlockSpec(memory_space=pltpu.VMEM)] * count,
        scratch_shapes=block
        + block
        + boxes
        + [
            pltpu.SemaphoreType.DMA((count,)),
            pltpu.SemaphoreType.DMA((copies,)),
            pltpu.SemaphoreType.DMA((copies,)),
        ],
        compiler_params=pltpu.CompilerParams(
            collective_id=collective_id,
            has_side_effects=True,
            vmem_limit_bytes=VMEM_BYTES,
        ),
        name="scatter_sum",
    )(*parts)


def swap_kernel(devices, count, *refs):
    sent, got = refs[:count], refs[count : 2 * count]
    own_sem, send_sem, recv_sem = refs[2 * count :]
    dp, me = lax.axis_index("dp"), lax.axis_index("seq")
    own = []
    for n in range(count):
        copy = pltpu.make_async_copy(sent[n].at[me], got[n].at[me], own_sem.at[n])
        copy.start()
        own.append(copy)
    barrier = pltpu.get_barrier_semaphore()
    for step in range(1, devices):
        pl.semaphore_signal(
            barrier,
            inc=1,
            device_id=(dp, lax.rem(me + step, devices)),
            device_id_type=MESH,
        )
    pl.semaphore_wait(barrier, devices - 1)
    copies = []
    for n in range(count):
        for step in range(1, devices):
            peer = lax.rem(me + step, devices)
            copy = pltpu.make_async_remote_copy(
                src_ref=sent[n].at[peer],
                dst_ref=got[n].at[me],
                send_sem=send_sem.at[n, step - 1],
                recv_sem=recv_sem.at[n, step - 1],
                device_id=(dp, peer),
                device_id_type=MESH,
            )
            copy.start()
            copies.append(copy)
    for copy in own:
        copy.wait()
    for copy in copies:
        copy.wait()


def swap_heads(arrays, devices, collective_id):
    count = len(arrays)
    return pl.pallas_call(
        functools.partial(swap_kernel, devices, count),
        out_shape=[jax.ShapeDtypeStruct(a.shape, a.dtype) for a in arrays],
        in_specs=[pl.BlockSpec(memory_space=pl.ANY)] * count,
        out_specs=[pl.BlockSpec(memory_space=pl.ANY)] * count,
        scratch_shapes=[
            pltpu.SemaphoreType.DMA((count,)),
            pltpu.SemaphoreType.DMA((count, devices - 1)),
            pltpu.SemaphoreType.DMA((count, devices - 1)),
        ],
        compiler_params=pltpu.CompilerParams(
            collective_id=collective_id, has_side_effects=True
        ),
        name="swap_heads",
    )(*arrays)


def side_by_side(ref):
    return jnp.concatenate([ref[s] for s in range(ref.shape[0])], axis=1)


def dot_first(left, right):
    return lax.dot_general(
        left, right, (((0,), (0,)), ((), ())), preferred_element_type=jnp.float32
    )


def dot_last(left, right):
    return lax.dot_general(
        left, right, (((1,), (1,)), ((), ())), preferred_element_type=jnp.float32
    )


def attend_kernel(q_ref, k_ref, v_ref, o_ref, full_ref, sum_ref):
    tokens = q_ref.shape[-1]
    each = ATT_BLOCK // tokens
    keys, values = side_by_side(k_ref), side_by_side(v_ref)
    for block in range(q_ref.shape[0] // each):
        first = block * each
        limit = (block + 1) * ATT_BLOCK
        queries = jnp.concatenate([q_ref[first + s] for s in range(each)], axis=1)
        weights = jnp.exp(dot_first(keys[:, :limit], queries))
        sums = jnp.sum(weights, axis=0, keepdims=True)
        mixed = jnp.dot(
            values[:, :limit],
            weights.astype(jnp.bfloat16),
            preferred_element_type=jnp.float32,
        )
        mixed = mixed / sums
        sum_ref[0, 0, :, pl.ds(block * ATT_BLOCK, ATT_BLOCK)] = sums
        for s in range(each):
            piece = mixed[:, s * tokens : (s + 1) * tokens]
            full_ref[first + s] = piece
            o_ref[first + s] = piece.astype(jnp.bfloat16)


def attend_specs(devices, tokens):
    piece = pl.BlockSpec((devices, HEAD_DIM, tokens), lambda m, h: (0, h, m))
    sums = pl.BlockSpec((1, 1, 1, devices * tokens), lambda m, h: (m, h, 0, 0))
    return piece, sums


def attend(queries, keys, values, tokens):
    devices, rows, cols = queries.shape
    grid = (cols // tokens, rows // HEAD_DIM)
    piece, sums = attend_specs(devices, tokens)
    return pl.pallas_call(
        attend_kernel,
        grid=grid,
        out_shape=[
            jax.ShapeDtypeStruct(queries.shape, jnp.bfloat16),
            jax.ShapeDtypeStruct(queries.shape, jnp.float32),
            jax.ShapeDtypeStruct(grid + (1, devices * tokens), jnp.float32),
        ],
        in_specs=[piece] * 3,
        out_specs=[piece, piece, sums],
        compiler_params=pltpu.CompilerParams(vmem_limit_bytes=VMEM_BYTES),
        name="attend",
    )(queries, keys, values)


def slopes_kernel(
    q_ref, k_ref, v_ref, do_ref, full_ref, sum_ref, rate_ref, dq_ref, dk_ref, dv_ref
):
    tokens = q_ref.shape[-1]
    each = ATT_BLOCK // tokens
    keys, values = side_by_side(k_ref), side_by_side(v_ref)
    rate = rate_ref[...]
    key_total = value_total = None
    for block in reversed(range(q_ref.shape[0] // each)):
        first = block * each
        limit = (block + 1) * ATT_BLOCK

        def pick(ref):
            return jnp.concatenate([ref[first + s] for s in range(each)], axis=1)

        queries = pick(q_ref)
        slope = pick(do_ref).astype(jnp.float32)
        sums = sum_ref[0, 0, :, pl.ds(block * ATT_BLOCK, ATT_BLOCK)]
        scaled = (slope / sums).astype(jnp.bfloat16)
        centre = jnp.sum(slope * pick(full_ref), axis=0, keepdims=True) / sums
        weights = jnp.exp(dot_first(keys[:, :limit], queries))
        dots = dot_first(values[:, :limit], scaled)
        slopes = (weights * (dots - centre)).astype(jnp.bfloat16)
        weights = weights.astype(jnp.bfloat16)
        query_part = jnp.dot(keys[:, :limit], slopes, preferred_element_type=jnp.float32)
        query_part = (query_part * rate).astype(jnp.bfloat16)
        for s in range(each):
            dq_ref[first + s] = query_part[:, s * tokens : (s + 1) * tokens]
        key_part = dot_last(queries, slopes)
        value_part = dot_last(scaled, weights)
        if key_total is None:
            key_total, value_total = key_part, value_part
        else:
            key_total = jnp.concatenate(
                [key_total[:, :limit] + key_part, key_total[:, limit:]], axis=1
            )
            value_total = jnp.concatenate(
                [value_total[:, :limit] + value_part, value_total[:, limit:]], axis=1
            )
    for s in range(q_ref.shape[0]):
        cols = slice(s * tokens, (s + 1) * tokens)
        dk_ref[s] = key_total[:, cols].astype(jnp.bfloat16)
        dv_ref[s] = value_total[:, cols].astype(jnp.bfloat16)


def slopes(queries, keys, values, slope, full, sums, rate, tokens):
    devices, rows, cols = queries.shape
    grid = (cols // tokens, rows // HEAD_DIM)
    piece, sum_spec = attend_specs(devices, tokens)
    return pl.pallas_call(
        slopes_kernel,
        grid=grid,
        out_shape=[jax.ShapeDtypeStruct(queries.shape, jnp.bfloat16)] * 3,
        in_specs=[piece] * 5
        + [sum_spec, pl.BlockSpec((HEAD_DIM, 1), lambda m, h: (0, 0))],
        out_specs=[piece] * 3,
        compiler_params=pltpu.CompilerParams(vmem_limit_bytes=VMEM_BYTES),
        name="slopes",
    )(queries, keys, values, slope, full, sums, rate)


def rms_scale(values):
    return lax.rsqrt(jnp.mean(values * values, axis=-1, keepdims=True) + EPSILON)


def contract(spec, left, right):
    return jnp.einsum(spec, left, right, preferred_element_type=jnp.float32)


def on_device(place, devices, *args):
    inputs, cotangent = args[:2]
    (
        norm_one,
        query_mat,
        query_add,
        key_mat,
        value_mat,
        value_add,
        output_mat,
        output_add,
        norm_two,
        hidden_mat,
        hidden_add,
        project_mat,
        project_add,
    ) = args[2:15]
    depth = args[15].astype(jnp.float32)
    micro, tokens, seqs, width = inputs.shape
    rows = micro * tokens * seqs
    vectors = (norm_one, query_add, value_add, output_add, norm_two, hidden_add, project_add)
    share = norm_one.shape[0]
    small = jnp.pad(jnp.stack(vectors), ((0, 16 - len(vectors)), (0, 128 - share)))
    mats = (query_mat, key_mat, value_mat, output_mat, hidden_mat, project_mat)
    gathered = gather_whole(place, (small,) + mats, 0)
    small = gathered[0].reshape(-1, 16, 128)[:, : len(vectors), :share]
    small = small.transpose(1, 0, 2).reshape(len(vectors), width).astype(jnp.float32)
    gain_one, query_add, value_add, output_add, gain_two, hidden_add, project_add = small
    query_mat, key_mat, value_mat, output_mat, hidden_mat, project_mat = (
        g.reshape(width, width) for g in gathered[1:]
    )

    def to_rows(array):
        return array.transpose(0, 2, 1, 3).reshape(rows, width)

    def from_rows(array):
        return array.reshape(micro, seqs, tokens, width).transpose(0, 2, 1, 3)

    rate = SOFT_BASE / math.sqrt(HEAD_DIM) * jax.nn.softplus(depth)
    rate_full = jnp.tile(rate, HEADS)[:, None]
    xfloat = to_rows(inputs).astype(jnp.float32)
    inv_one = rms_scale(xfloat)
    normed = (xfloat * inv_one * gain_one).astype(jnp.bfloat16)
    query_pre = contract("df,rd->fr", query_mat, normed) + query_add[:, None]
    queries = (query_pre * rate_full).astype(jnp.bfloat16)
    keys = contract("df,rd->fr", key_mat, normed).astype(jnp.bfloat16)
    values = (contract("df,rd->fr", value_mat, normed) + value_add[:, None]).astype(jnp.bfloat16)

    def split(array):
        return array.reshape(devices, width // devices, rows)

    q_in, k_in, v_in = swap_heads([split(queries), split(keys), split(values)], devices, 1)
    mixed, full, sums = attend(q_in, k_in, v_in, tokens)
    (mixed,) = swap_heads([mixed], devices, 2)
    mixed = mixed.reshape(width, rows)
    residual = xfloat + (contract("fr,fd->rd", mixed, output_mat) + output_add)
    inv_two = rms_scale(residual)
    second = (residual * inv_two * gain_two).astype(jnp.bfloat16)
    hidden_pre = contract("rd,df->rf", second, hidden_mat) + hidden_add
    active = jax.nn.silu(hidden_pre).astype(jnp.bfloat16)
    result = residual + (contract("rf,fd->rd", active, project_mat) + project_add)
    result = from_rows(result.astype(jnp.bfloat16))

    upper = to_rows(cotangent)
    project_grad = contract("rf,rd->fd", active, upper)
    project_bias_grad = jnp.sum(upper.astype(jnp.float32), axis=0)
    active_grad = contract("rd,fd->rf", upper, project_mat)
    logistic = jax.nn.sigmoid(hidden_pre)
    hidden_grad = (active_grad * logistic * (1.0 + hidden_pre * (1.0 - logistic))).astype(
        jnp.bfloat16
    )
    hidden_mat_grad = contract("rd,rf->df", second, hidden_grad)
    hidden_bias_grad = jnp.sum(hidden_grad.astype(jnp.float32), axis=0)
    second_grad = contract("rf,df->rd", hidden_grad, hidden_mat)
    normal_two = residual * inv_two
    scaled_two = second_grad * gain_two
    norm_two_grad = jnp.sum(second_grad * normal_two, axis=0)
    residual_grad = upper.astype(jnp.float32) + inv_two * (
        scaled_two - normal_two * jnp.mean(scaled_two * normal_two, axis=-1, keepdims=True)
    )
    branch_grad = residual_grad.astype(jnp.bfloat16)
    output_mat_grad = contract("fr,rd->fd", mixed, branch_grad)
    output_bias_grad = jnp.sum(branch_grad.astype(jnp.float32), axis=0)
    mixed_grad = contract("fd,rd->fr", output_mat, branch_grad).astype(jnp.bfloat16)

    (do_in,) = swap_heads([split(mixed_grad)], devices, 3)
    slopes_out = slopes(q_in, k_in, v_in, do_in, full, sums, rate[:, None], tokens)
    query_slope, key_grad, value_grad = (
        a.reshape(width, rows) for a in swap_heads(slopes_out, devices, 4)
    )
    query_float = query_slope.astype(jnp.float32)
    scale_part = jnp.sum(query_float / rate_full * query_pre, axis=1)
    scale_part = jnp.sum(scale_part.reshape(HEADS, HEAD_DIM), axis=0)
    query_mat_grad = contract("rd,fr->df", normed, query_slope)
    query_bias_grad = jnp.sum(query_float, axis=1)
    key_mat_grad = contract("rd,fr->df", normed, key_grad)
    value_mat_grad = contract("rd,fr->df", normed, value_grad)
    value_bias_grad = jnp.sum(value_grad.astype(jnp.float32), axis=1)
    normed_grad = (
        contract("fr,df->rd", query_slope, query_mat)
        + contract("fr,df->rd", key_grad, key_mat)
        + contract("fr,df->rd", value_grad, value_mat)
    )
    normal_one = xfloat * inv_one
    scaled_one = normed_grad * gain_one
    norm_one_grad = jnp.sum(normed_grad * normal_one, axis=0)
    source_grad = residual_grad + inv_one * (
        scaled_one - normal_one * jnp.mean(scaled_one * normal_one, axis=-1, keepdims=True)
    )
    source_grad = from_rows(source_grad.astype(jnp.bfloat16))

    vector_grads = jnp.stack(
        (
            norm_one_grad,
            query_bias_grad,
            value_bias_grad,
            output_bias_grad,
            norm_two_grad,
            hidden_bias_grad,
            project_bias_grad,
        )
    )
    vector_grads = vector_grads.reshape(7, -1, share).transpose(1, 0, 2)
    vector_grads = jnp.pad(vector_grads, ((0, 0), (0, 0), (0, 128 - share)))
    scale_row = jnp.pad(scale_part, (0, 128 - HEAD_DIM))
    scale_row = jnp.broadcast_to(scale_row, (vector_grads.shape[0], 1, 128))
    vector_grads = jnp.concatenate([vector_grads, scale_row], axis=1)
    vector_grads = vector_grads.reshape(place.grid() + (8, 128))
    mat_grads = (
        project_grad,
        hidden_mat_grad,
        output_mat_grad,
        query_mat_grad,
        key_mat_grad,
        value_mat_grad,
    )
    parts = [
        g.astype(jnp.bfloat16).reshape(place.grid() + (share, width)) for g in mat_grads
    ]
    if share % 8 == 0:
        summed = scatter_sum(place, parts + [vector_grads], 5)
        shares, vector_sums = summed[:-1], summed[-1]
    else:
        (vector_sums,) = scatter_sum(place, [vector_grads], 5)
        shares = [scatter_sum(place, [p], 6)[0] for p in parts]
    project_grad, hidden_mat_grad, output_mat_grad = shares[:3]
    query_mat_grad, key_mat_grad, value_mat_grad = shares[3:]
    g_one, g_query, g_value, g_output, g_two, g_hidden, g_project = (
        vector_sums[n, :share] for n in range(7)
    )
    scale_summed = vector_sums[7, :HEAD_DIM]
    depth_grad = scale_summed * (SOFT_BASE / math.sqrt(HEAD_DIM)) * jax.nn.sigmoid(depth)
    return (
        result,
        source_grad,
        g_one,
        query_mat_grad,
        g_query,
        key_mat_grad,
        value_mat_grad,
        g_value,
        output_mat_grad,
        g_output,
        g_two,
        hidden_mat_grad,
        g_hidden,
        project_grad,
        g_project,
        depth_grad,
    )


def solution(mesh):
    both = ("dp", "seq")
    token, vector, matrix = P(None, "seq", "dp", None), P(both), P(both, None)
    weights = (
        vector,
        matrix,
        vector,
        matrix,
        matrix,
        vector,
        matrix,
        vector,
        vector,
        matrix,
        vector,
        matrix,
        vector,
    )
    specs = (token, token) + weights + (P(),)
    place = Place(mesh.shape["dp"], mesh.shape["seq"])
    return jax.shard_map(
        functools.partial(on_device, place, mesh.shape["seq"]),
        mesh=mesh,
        in_specs=specs,
        out_specs=specs,
        check_vma=False,
    )
```

```python
import functools
import itertools
import math

import jax
import jax.numpy as jnp
from jax import lax
from jax.experimental import pallas as pl
from jax.experimental.pallas import tpu as pltpu
from jax.sharding import PartitionSpec as P

HEADS = 16
HEAD_DIM = 80
ATT_BLOCK = 256
SOFT_BASE = 1.442695041
EPSILON = 1e-06
MESH = pl.DeviceIdType.MESH
VMEM_BYTES = 60 * 1024 * 1024


class Place:
    def __init__(self, dp, seq):
        self.cores = 2 if dp % 2 == 0 else 1
        self.lines = dp // self.cores
        self.levels = 4 if seq % 4 == 0 else seq
        self.across = seq // self.levels
        self.sizes = {
            "y": self.lines,
            "c": self.cores,
            "z": self.levels,
            "x": self.across,
        }

    def here(self):
        dp = lax.axis_index("dp")
        seq = lax.axis_index("seq")
        return {
            "y": dp // self.cores,
            "c": dp % self.cores,
            "z": seq // self.across,
            "x": seq % self.across,
        }

    def shift(self, spot, axis, step):
        moved = dict(spot)
        moved[axis] = lax.rem(spot[axis] + step, self.sizes[axis])
        return moved

    def device(self, spot):
        return (
            spot["y"] * self.cores + spot["c"],
            spot["z"] * self.across + spot["x"],
        )

    def grid(self):
        return (self.lines, self.cores, self.levels, self.across)

    def greet(self, spot, wide):
        barrier = pltpu.get_barrier_semaphore()
        dp, seq = self.device(spot)
        peers = [
            self.device(self.shift(spot, axis, step))
            for axis in ("yc" if wide else "zxyc")
            for step in range(1, self.sizes[axis])
        ]
        if wide:
            devices = self.levels * self.across
            peers += [(dp, lax.rem(seq + step, devices)) for step in range(1, devices)]
        for peer in peers:
            pl.semaphore_signal(barrier, inc=1, device_id=peer, device_id_type=MESH)
        pl.semaphore_wait(barrier, len(peers))


def halves_of(cols, lean):
    if lean and cols % 640 == 0:
        cut = cols * 4 // 5
    elif cols % 256 == 0:
        cut = cols // 2
    else:
        return ((slice(0, cols), "xy"),)
    return ((slice(0, cut), "xy"), (slice(cut, cols), "yx"))


def chunks_of(rows):
    if rows % 8 == 0 and rows >= 32:
        cut = rows // 32 * 16
        return (slice(0, cut), slice(cut, rows))
    return (slice(0, rows),)


class Sender:
    def __init__(self, place, spot, send_sem, recv_sem):
        self.place = place
        self.spot = spot
        self.send_sem = send_sem
        self.recv_sem = recv_sem
        self.count = itertools.count()
        self.open = {}
        self.every = []

    def put(self, key, device, source, target):
        at = next(self.count)
        copy = pltpu.make_async_remote_copy(
            src_ref=source,
            dst_ref=target,
            send_sem=self.send_sem.at[at],
            recv_sem=self.recv_sem.at[at],
            device_id=device,
            device_id_type=MESH,
        )
        copy.start()
        self.open.setdefault(key, []).append(copy)
        self.every.append(copy)

    def go(self, key, axis, source, target):
        self.open[key] = []
        for step in range(1, self.place.sizes[axis]):
            peer = self.place.shift(self.spot, axis, step)
            self.put(key, self.place.device(peer), source(peer), target(step))

    def landed(self, key):
        for copy in self.open[key]:
            copy.wait_recv()

    def finish(self):
        for copy in self.every:
            copy.wait_send()


class Gather:
    def __init__(self, place, spot, lean, shards, wholes, own_sem):
        self.place, self.spot, self.lean = place, spot, lean
        self.shards, self.wholes = shards, wholes
        self.jobs = [(n, r) for n, s in enumerate(shards) for r in chunks_of(s.shape[0])]
        y, c, z, x = (spot[k] for k in "yczx")
        self.own = []
        for n, shard in enumerate(shards):
            copy = pltpu.make_async_copy(shard, wholes[n].at[y, c, z, x], own_sem[n])
            copy.start()
            self.own.append(copy)

    def run(self, out):
        shards, wholes = self.shards, self.wholes
        y, c, z, x = (self.spot[k] for k in "yczx")
        filled = set()

        def halves(n):
            return enumerate(halves_of(shards[n].shape[-1], self.lean))

        def one(job, n, rows):
            part = wholes[n].at[y, c, z, x, rows]
            out.go((job, "z"), "z", lambda peer: shards[n].at[rows], lambda step: part)

        def two(job, n, rows):
            out.landed((job, "z"))
            if n not in filled:
                filled.add(n)
                self.own[n].wait()
            for half, (cols, order) in halves(n):
                part = wholes[n].at[y, c, :, x, rows, cols]
                out.go((job, half, 2), order[0], lambda peer: part, lambda step: part)

        def three(job, n, rows):
            for half, (cols, order) in halves(n):
                out.landed((job, half, 2))
                if order == "xy":
                    part = wholes[n].at[y, c, :, :, rows, cols]
                else:
                    part = wholes[n].at[:, c, :, x, rows, cols]
                out.go((job, half, 3), order[1], lambda peer: part, lambda step: part)

        def four(job, n, rows):
            for half, (cols, order) in halves(n):
                out.landed((job, half, 3))
                part = wholes[n].at[:, c, :, :, rows, cols]
                out.go((job, half, 4), "c", lambda peer: part, lambda step: part)

        def five(job, n, rows):
            for half, _ in halves(n):
                out.landed((job, half, 4))

        jobs = [(("gather", at),) + job for at, job in enumerate(self.jobs)]
        ahead = min(3, len(jobs))
        for job in jobs[:ahead]:
            one(*job)
        for step in range(len(jobs) + 3):
            if step < len(jobs):
                two(*jobs[step])
            if step + ahead < len(jobs):
                one(*jobs[step + ahead])
            for stage, late in ((three, 1), (four, 2), (five, 3)):
                if 0 <= step - late < len(jobs):
                    stage(*jobs[step - late])


def total(values):
    result = values[0].astype(jnp.float32)
    for value in values[1:]:
        result = result + value.astype(jnp.float32)
    return result


class Scatter:
    def __init__(self, place, spot, lean, parts, totals, boxes, own_sem):
        self.place, self.spot, self.lean = place, spot, lean
        self.parts, self.totals = parts, totals
        self.jobs = [(n, r) for n, p in enumerate(parts) for r in chunks_of(p.shape[-2])]
        self.own_sem = own_sem
        self.sums, self.cores, self.seconds, self.thirds, self.fourths = [], [], [], [], []
        self.results, self.own = [], []
        for n, part in enumerate(parts):
            self.sums.append(boxes.pop(0))
            self.cores.append(boxes.pop(0))
            halves = halves_of(part.shape[-1], lean)
            self.seconds.append([boxes.pop(0) for _ in halves])
            self.thirds.append([boxes.pop(0) for _ in halves])
            self.fourths.append(boxes.pop(0))
            self.results.append(boxes.pop(0))
            copy = pltpu.make_async_copy(
                part.at[:, spot["c"]], self.sums[n], own_sem[n]
            )
            copy.start()
            self.own.append(copy)

    def run(self, out):
        place, parts, sums = self.place, self.parts, self.sums
        cores, results = self.cores, self.results
        y, c, z, x = (self.spot[k] for k in "yczx")
        lines, _, levels, across = place.grid()
        filled = set()

        def halves(n):
            return enumerate(halves_of(parts[n].shape[-1], self.lean))

        def one(job, n, rows):
            out.go(
                (job, 1),
                "c",
                lambda peer: parts[n].at[:, peer["c"], :, :, rows],
                lambda step: cores[n].at[:, :, :, rows],
            )

        def two(job, n, rows):
            if n not in filled:
                filled.add(n)
                self.own[n].wait()
            out.landed((job, 1))
            if place.cores > 1:

                @pl.loop(0, lines * levels * across)
                def _(at):
                    where = (at // (levels * across), (at // across) % levels, at % across)
                    sums[n][where + (rows,)] = total(
                        [sums[n][where + (rows,)], cores[n][where + (rows,)]]
                    ).astype(sums[n].dtype)

            for half, (cols, order) in halves(n):
                box = self.seconds[n][half]
                if order == "xy":
                    out.go(
                        (job, half, 2),
                        "y",
                        lambda peer: sums[n].at[peer["y"], :, :, rows, cols],
                        lambda step: box.at[step - 1, :, :, rows],
                    )
                else:
                    out.go(
                        (job, half, 2),
                        "x",
                        lambda peer: sums[n].at[:, :, peer["x"], rows, cols],
                        lambda step: box.at[step - 1, :, :, rows],
                    )

        def three(job, n, rows):
            for half, (cols, order) in halves(n):
                out.landed((job, half, 2))
                box, later = self.seconds[n][half], self.thirds[n][half]
                if order == "xy":

                    @pl.loop(0, levels * across)
                    def _(at):
                        zz, xx = at // across, at % across
                        values = [sums[n][y, zz, xx, rows, cols]]
                        values += [box[k, zz, xx, rows] for k in range(lines - 1)]
                        sums[n][y, zz, xx, rows, cols] = total(values).astype(sums[n].dtype)

                    out.go(
                        (job, half, 3),
                        "x",
                        lambda peer: sums[n].at[y, :, peer["x"], rows, cols],
                        lambda step: later.at[step - 1, :, rows],
                    )
                else:

                    @pl.loop(0, lines * levels)
                    def _(at):
                        yy, zz = at // levels, at % levels
                        values = [sums[n][yy, zz, x, rows, cols]]
                        values += [box[k, yy, zz, rows] for k in range(across - 1)]
                        sums[n][yy, zz, x, rows, cols] = total(values).astype(sums[n].dtype)

                    out.go(
                        (job, half, 3),
                        "y",
                        lambda peer: sums[n].at[peer["y"], :, x, rows, cols],
                        lambda step: later.at[step - 1, :, rows],
                    )

        def four(job, n, rows):
            for half, (cols, order) in halves(n):
                out.landed((job, half, 3))
                box = self.thirds[n][half]

                @pl.loop(0, levels)
                def _(zz):
                    values = [sums[n][y, zz, x, rows, cols]]
                    values += [box[k, zz, rows] for k in range(box.shape[0])]
                    sums[n][y, zz, x, rows, cols] = total(values).astype(sums[n].dtype)

            out.go(
                (job, 4),
                "z",
                lambda peer: sums[n].at[y, peer["z"], x, rows],
                lambda step: self.fourths[n].at[step - 1, rows],
            )

        def five(job, n, rows):
            out.landed((job, 4))
            values = [sums[n][y, z, x, rows]]
            values += [self.fourths[n][k, rows] for k in range(levels - 1)]
            results[n][rows] = total(values)

        jobs = [(("scatter", at),) + job for at, job in enumerate(self.jobs)]
        for step in range(len(jobs) + 4):
            for stage, late in ((one, 0), (two, 1), (three, 2), (four, 3), (five, 4)):
                if 0 <= step - late < len(jobs):
                    stage(*jobs[step - late])
        last = []
        for n, result in enumerate(results):
            copy = pltpu.make_async_copy(result, self.totals[n], self.own_sem[n])
            copy.start()
            last.append(copy)
        for copy in last:
            copy.wait()


def scatter_boxes(place, part, lean):
    lines, _, levels, across = place.grid()
    rows, cols = part.shape[-2:]
    block = pltpu.VMEM((lines, levels, across, rows, cols), part.dtype)
    first, later = [], []
    for piece, order in halves_of(cols, lean):
        size = (rows, piece.stop - piece.start)
        steps = (lines - 1, across - 1) if order == "xy" else (across - 1, lines - 1)
        middle = (levels, across) if order == "xy" else (lines, levels)
        first.append(pltpu.VMEM((steps[0],) + middle + size, part.dtype))
        later.append(pltpu.VMEM((steps[1], levels) + size, part.dtype))
    last = pltpu.VMEM((levels - 1, rows, cols), part.dtype)
    return [block, block] + first + later + [last, pltpu.VMEM((rows, cols), jnp.float32)]


def move_kernel(place, counts, lean, *refs):
    refs = list(refs)
    swaps, gathers, scatters = counts
    whole = swaps + gathers + scatters
    ins, outs, rest = refs[:whole], refs[whole : 2 * whole], refs[2 * whole :]
    own_sem, send_sem, recv_sem = rest[-3:]
    spot = place.here()
    dp, me = place.device(spot)
    devices = place.levels * place.across
    sent, got = ins[:swaps], outs[:swaps]
    own = []
    for n in range(swaps):
        copy = pltpu.make_async_copy(sent[n].at[me], got[n].at[me], own_sem.at[n])
        copy.start()
        own.append(copy)
    cut = swaps + gathers
    gather = Gather(
        place, spot, lean, ins[swaps:cut], outs[swaps:cut], [own_sem.at[n] for n in range(swaps, cut)]
    )
    scatter = Scatter(
        place, spot, lean, ins[cut:], outs[cut:], rest[:-3], [own_sem.at[n] for n in range(cut, whole)]
    )
    place.greet(spot, swaps > 0)
    out = Sender(place, spot, send_sem, recv_sem)
    for n in range(swaps):
        for step in range(1, devices):
            peer = lax.rem(me + step, devices)
            out.put("swap", (dp, peer), sent[n].at[peer], got[n].at[me])
    gather.run(out)
    scatter.run(out)
    for copy in own:
        copy.wait()
    if swaps:
        out.landed("swap")
    out.finish()


def move(place, collective_id, swaps=(), gathers=(), scatters=()):
    lean = len(swaps) > 0
    copies = len(swaps) * (place.levels * place.across - 1)
    boxes = []
    lines, cores, levels, across = place.grid()
    for shard in gathers:
        count = (levels - 1) + len(halves_of(shard.shape[-1], lean)) * (
            across + lines + cores - 3
        )
        copies += len(chunks_of(shard.shape[0])) * count
    for part in scatters:
        count = (levels - 1) + (cores - 1)
        count += len(halves_of(part.shape[-1], lean)) * (lines + across - 2)
        copies += len(chunks_of(part.shape[-2])) * count
        boxes += scatter_boxes(place, part, lean)
    shapes = [jax.ShapeDtypeStruct(a.shape, a.dtype) for a in swaps]
    shapes += [jax.ShapeDtypeStruct(place.grid() + s.shape, s.dtype) for s in gathers]
    shapes += [jax.ShapeDtypeStruct(p.shape[-2:], jnp.float32) for p in scatters]
    return pl.pallas_call(
        functools.partial(
            move_kernel, place, (len(swaps), len(gathers), len(scatters)), lean
        ),
        out_shape=shapes,
        in_specs=[pl.BlockSpec(memory_space=pl.ANY)] * len(shapes),
        out_specs=[pl.BlockSpec(memory_space=pl.ANY)] * len(shapes),
        scratch_shapes=boxes
        + [
            pltpu.SemaphoreType.DMA((len(shapes),)),
            pltpu.SemaphoreType.DMA((copies,)),
            pltpu.SemaphoreType.DMA((copies,)),
        ],
        compiler_params=pltpu.CompilerParams(
            collective_id=collective_id,
            has_side_effects=True,
            vmem_limit_bytes=VMEM_BYTES,
        ),
        name=f"move_{collective_id}",
    )(*swaps, *gathers, *scatters)


def side_by_side(ref):
    return jnp.concatenate([ref[s] for s in range(ref.shape[0])], axis=1)


def dot_first(left, right):
    return lax.dot_general(
        left, right, (((0,), (0,)), ((), ())), preferred_element_type=jnp.float32
    )


def dot_last(left, right):
    return lax.dot_general(
        left, right, (((1,), (1,)), ((), ())), preferred_element_type=jnp.float32
    )


def attend_kernel(q_ref, k_ref, v_ref, o_ref, full_ref, sum_ref):
    tokens = q_ref.shape[-1]
    each = ATT_BLOCK // tokens
    keys, values = side_by_side(k_ref), side_by_side(v_ref)
    for block in range(q_ref.shape[0] // each):
        first = block * each
        limit = (block + 1) * ATT_BLOCK
        queries = jnp.concatenate([q_ref[first + s] for s in range(each)], axis=1)
        weights = jnp.exp(dot_first(keys[:, :limit], queries))
        sums = jnp.sum(weights, axis=0, keepdims=True)
        mixed = jnp.dot(
            values[:, :limit],
            weights.astype(jnp.bfloat16),
            preferred_element_type=jnp.float32,
        )
        mixed = mixed / sums
        sum_ref[0, 0, :, pl.ds(block * ATT_BLOCK, ATT_BLOCK)] = sums
        for s in range(each):
            piece = mixed[:, s * tokens : (s + 1) * tokens]
            full_ref[first + s] = piece
            o_ref[first + s] = piece.astype(jnp.bfloat16)


def attend_specs(devices, tokens):
    piece = pl.BlockSpec((devices, HEAD_DIM, tokens), lambda m, h: (0, h, m))
    sums = pl.BlockSpec((1, 1, 1, devices * tokens), lambda m, h: (m, h, 0, 0))
    return piece, sums


def attend(queries, keys, values, tokens):
    devices, rows, cols = queries.shape
    grid = (cols // tokens, rows // HEAD_DIM)
    piece, sums = attend_specs(devices, tokens)
    return pl.pallas_call(
        attend_kernel,
        grid=grid,
        out_shape=[
            jax.ShapeDtypeStruct(queries.shape, jnp.bfloat16),
            jax.ShapeDtypeStruct(queries.shape, jnp.float32),
            jax.ShapeDtypeStruct(grid + (1, devices * tokens), jnp.float32),
        ],
        in_specs=[piece] * 3,
        out_specs=[piece, piece, sums],
        compiler_params=pltpu.CompilerParams(vmem_limit_bytes=VMEM_BYTES),
        name="attend",
    )(queries, keys, values)


def slopes_kernel(
    q_ref, k_ref, v_ref, do_ref, full_ref, sum_ref, rate_ref, dq_ref, dk_ref, dv_ref
):
    tokens = q_ref.shape[-1]
    each = ATT_BLOCK // tokens
    keys, values = side_by_side(k_ref), side_by_side(v_ref)
    rate = rate_ref[...]
    key_total = value_total = None
    for block in reversed(range(q_ref.shape[0] // each)):
        first = block * each
        limit = (block + 1) * ATT_BLOCK

        def pick(ref):
            return jnp.concatenate([ref[first + s] for s in range(each)], axis=1)

        queries = pick(q_ref)
        slope = pick(do_ref).astype(jnp.float32)
        sums = sum_ref[0, 0, :, pl.ds(block * ATT_BLOCK, ATT_BLOCK)]
        scaled = (slope / sums).astype(jnp.bfloat16)
        centre = jnp.sum(slope * pick(full_ref), axis=0, keepdims=True) / sums
        weights = jnp.exp(dot_first(keys[:, :limit], queries))
        dots = dot_first(values[:, :limit], scaled)
        slopes = (weights * (dots - centre)).astype(jnp.bfloat16)
        weights = weights.astype(jnp.bfloat16)
        query_part = jnp.dot(keys[:, :limit], slopes, preferred_element_type=jnp.float32)
        query_part = (query_part * rate).astype(jnp.bfloat16)
        for s in range(each):
            dq_ref[first + s] = query_part[:, s * tokens : (s + 1) * tokens]
        key_part = dot_last(queries, slopes)
        value_part = dot_last(scaled, weights)
        if key_total is None:
            key_total, value_total = key_part, value_part
        else:
            key_total = jnp.concatenate(
                [key_total[:, :limit] + key_part, key_total[:, limit:]], axis=1
            )
            value_total = jnp.concatenate(
                [value_total[:, :limit] + value_part, value_total[:, limit:]], axis=1
            )
    for s in range(q_ref.shape[0]):
        cols = slice(s * tokens, (s + 1) * tokens)
        dk_ref[s] = key_total[:, cols].astype(jnp.bfloat16)
        dv_ref[s] = value_total[:, cols].astype(jnp.bfloat16)


def slopes(queries, keys, values, slope, full, sums, rate, tokens):
    devices, rows, cols = queries.shape
    grid = (cols // tokens, rows // HEAD_DIM)
    piece, sum_spec = attend_specs(devices, tokens)
    return pl.pallas_call(
        slopes_kernel,
        grid=grid,
        out_shape=[jax.ShapeDtypeStruct(queries.shape, jnp.bfloat16)] * 3,
        in_specs=[piece] * 5
        + [sum_spec, pl.BlockSpec((HEAD_DIM, 1), lambda m, h: (0, 0))],
        out_specs=[piece] * 3,
        compiler_params=pltpu.CompilerParams(vmem_limit_bytes=VMEM_BYTES),
        name="slopes",
    )(queries, keys, values, slope, full, sums, rate)


def rms_scale(values):
    return lax.rsqrt(jnp.mean(values * values, axis=-1, keepdims=True) + EPSILON)


def contract(spec, left, right):
    return jnp.einsum(spec, left, right, preferred_element_type=jnp.float32)


def on_device(place, devices, *args):
    inputs, cotangent = args[:2]
    (
        norm_one,
        query_mat,
        query_add,
        key_mat,
        value_mat,
        value_add,
        output_mat,
        output_add,
        norm_two,
        hidden_mat,
        hidden_add,
        project_mat,
        project_add,
    ) = args[2:15]
    depth = args[15].astype(jnp.float32)
    micro, tokens, seqs, width = inputs.shape
    rows = micro * tokens * seqs
    vectors = (norm_one, query_add, value_add, output_add, norm_two, hidden_add, project_add)
    share = norm_one.shape[0]
    small = jnp.pad(jnp.stack(vectors), ((0, 16 - len(vectors)), (0, 128 - share)))
    gathered = move(place, 0, gathers=(small, query_mat, key_mat, value_mat))
    small = gathered[0].reshape(-1, 16, 128)[:, : len(vectors), :share]
    small = small.transpose(1, 0, 2).reshape(len(vectors), width).astype(jnp.float32)
    gain_one, query_add, value_add, output_add, gain_two, hidden_add, project_add = small
    query_mat, key_mat, value_mat = (g.reshape(width, width) for g in gathered[1:])

    def to_rows(array):
        return array.transpose(0, 2, 1, 3).reshape(rows, width)

    def from_rows(array):
        return array.reshape(micro, seqs, tokens, width).transpose(0, 2, 1, 3)

    rate = SOFT_BASE / math.sqrt(HEAD_DIM) * jax.nn.softplus(depth)
    rate_full = jnp.tile(rate, HEADS)[:, None]
    xfloat = to_rows(inputs).astype(jnp.float32)
    inv_one = rms_scale(xfloat)
    normed = (xfloat * inv_one * gain_one).astype(jnp.bfloat16)
    query_pre = contract("df,rd->fr", query_mat, normed) + query_add[:, None]
    queries = (query_pre * rate_full).astype(jnp.bfloat16)
    keys = contract("df,rd->fr", key_mat, normed).astype(jnp.bfloat16)
    values = (contract("df,rd->fr", value_mat, normed) + value_add[:, None]).astype(jnp.bfloat16)

    def split(array):
        return array.reshape(devices, width // devices, rows)

    q_in, k_in, v_in, output_mat, hidden_mat = move(
        place, 1, (split(queries), split(keys), split(values)), (output_mat, hidden_mat)
    )
    output_mat, hidden_mat = (g.reshape(width, width) for g in (output_mat, hidden_mat))
    mixed, full, sums = attend(q_in, k_in, v_in, tokens)
    mixed, project_mat = move(place, 2, (mixed,), (project_mat,))
    mixed, project_mat = mixed.reshape(width, rows), project_mat.reshape(width, width)
    residual = xfloat + (contract("fr,fd->rd", mixed, output_mat) + output_add)
    inv_two = rms_scale(residual)
    second = (residual * inv_two * gain_two).astype(jnp.bfloat16)
    hidden_pre = contract("rd,df->rf", second, hidden_mat) + hidden_add
    active = jax.nn.silu(hidden_pre).astype(jnp.bfloat16)
    result = residual + (contract("rf,fd->rd", active, project_mat) + project_add)
    result = from_rows(result.astype(jnp.bfloat16))

    upper = to_rows(cotangent)
    project_grad = contract("rf,rd->fd", active, upper)
    project_bias_grad = jnp.sum(upper.astype(jnp.float32), axis=0)
    active_grad = contract("rd,fd->rf", upper, project_mat)
    logistic = jax.nn.sigmoid(hidden_pre)
    hidden_grad = (active_grad * logistic * (1.0 + hidden_pre * (1.0 - logistic))).astype(
        jnp.bfloat16
    )
    hidden_mat_grad = contract("rd,rf->df", second, hidden_grad)
    hidden_bias_grad = jnp.sum(hidden_grad.astype(jnp.float32), axis=0)
    second_grad = contract("rf,df->rd", hidden_grad, hidden_mat)
    normal_two = residual * inv_two
    scaled_two = second_grad * gain_two
    norm_two_grad = jnp.sum(second_grad * normal_two, axis=0)
    residual_grad = upper.astype(jnp.float32) + inv_two * (
        scaled_two - normal_two * jnp.mean(scaled_two * normal_two, axis=-1, keepdims=True)
    )
    branch_grad = residual_grad.astype(jnp.bfloat16)
    output_mat_grad = contract("fr,rd->fd", mixed, branch_grad)
    output_bias_grad = jnp.sum(branch_grad.astype(jnp.float32), axis=0)
    mixed_grad = contract("fd,rd->fr", output_mat, branch_grad).astype(jnp.bfloat16)

    def as_parts(*grads):
        return tuple(
            g.astype(jnp.bfloat16).reshape(place.grid() + (share, width)) for g in grads
        )

    merged = share % 8 == 0
    early = as_parts(project_grad) if merged else ()
    do_in, *early = move(place, 3, (split(mixed_grad),), (), early)
    slopes_out = slopes(q_in, k_in, v_in, do_in, full, sums, rate[:, None], tokens)
    middle = as_parts(hidden_mat_grad, output_mat_grad) if merged else ()
    query_slope, key_grad, value_grad, *middle = move(place, 4, slopes_out, (), middle)
    query_slope, key_grad, value_grad = (
        a.reshape(width, rows) for a in (query_slope, key_grad, value_grad)
    )
    query_float = query_slope.astype(jnp.float32)
    scale_part = jnp.sum(query_float / rate_full * query_pre, axis=1)
    scale_part = jnp.sum(scale_part.reshape(HEADS, HEAD_DIM), axis=0)
    query_mat_grad = contract("rd,fr->df", normed, query_slope)
    query_bias_grad = jnp.sum(query_float, axis=1)
    key_mat_grad = contract("rd,fr->df", normed, key_grad)
    value_mat_grad = contract("rd,fr->df", normed, value_grad)
    value_bias_grad = jnp.sum(value_grad.astype(jnp.float32), axis=1)
    normed_grad = (
        contract("fr,df->rd", query_slope, query_mat)
        + contract("fr,df->rd", key_grad, key_mat)
        + contract("fr,df->rd", value_grad, value_mat)
    )
    normal_one = xfloat * inv_one
    scaled_one = normed_grad * gain_one
    norm_one_grad = jnp.sum(normed_grad * normal_one, axis=0)
    source_grad = residual_grad + inv_one * (
        scaled_one - normal_one * jnp.mean(scaled_one * normal_one, axis=-1, keepdims=True)
    )
    source_grad = from_rows(source_grad.astype(jnp.bfloat16))

    vector_grads = jnp.stack(
        (
            norm_one_grad,
            query_bias_grad,
            value_bias_grad,
            output_bias_grad,
            norm_two_grad,
            hidden_bias_grad,
            project_bias_grad,
        )
    )
    vector_grads = vector_grads.reshape(7, -1, share).transpose(1, 0, 2)
    vector_grads = jnp.pad(vector_grads, ((0, 0), (0, 0), (0, 128 - share)))
    scale_row = jnp.pad(scale_part, (0, 128 - HEAD_DIM))
    scale_row = jnp.broadcast_to(scale_row, (vector_grads.shape[0], 1, 128))
    vector_grads = jnp.concatenate([vector_grads, scale_row], axis=1)
    vector_grads = vector_grads.reshape(place.grid() + (8, 128))
    late = as_parts(query_mat_grad, key_mat_grad, value_mat_grad)
    if merged:
        *late, vector_sums = move(place, 5, scatters=late + (vector_grads,))
    else:
        (vector_sums,) = move(place, 5, scatters=(vector_grads,))
        early = as_parts(project_grad, hidden_mat_grad, output_mat_grad)
        early, *middle = ([move(place, 6, scatters=(p,))[0] for p in early])
        early = [early]
        late = [move(place, 6, scatters=(p,))[0] for p in late]
    (project_grad,) = early
    hidden_mat_grad, output_mat_grad = middle
    query_mat_grad, key_mat_grad, value_mat_grad = late
    g_one, g_query, g_value, g_output, g_two, g_hidden, g_project = (
        vector_sums[n, :share] for n in range(7)
    )
    scale_summed = vector_sums[7, :HEAD_DIM]
    depth_grad = scale_summed * (SOFT_BASE / math.sqrt(HEAD_DIM)) * jax.nn.sigmoid(depth)
    return (
        result,
        source_grad,
        g_one,
        query_mat_grad,
        g_query,
        key_mat_grad,
        value_mat_grad,
        g_value,
        output_mat_grad,
        g_output,
        g_two,
        hidden_mat_grad,
        g_hidden,
        project_grad,
        g_project,
        depth_grad,
    )


def solution(mesh):
    both = ("dp", "seq")
    token, vector, matrix = P(None, "seq", "dp", None), P(both), P(both, None)
    weights = (
        vector,
        matrix,
        vector,
        matrix,
        matrix,
        vector,
        matrix,
        vector,
        vector,
        matrix,
        vector,
        matrix,
        vector,
    )
    specs = (token, token) + weights + (P(),)
    place = Place(mesh.shape["dp"], mesh.shape["seq"])
    return jax.shard_map(
        functools.partial(on_device, place, mesh.shape["seq"]),
        mesh=mesh,
        in_specs=specs,
        out_specs=specs,
        check_vma=False,
    )
```

```python
import functools
import itertools
import math

import jax
import jax.numpy as jnp
from jax import lax
from jax.experimental import pallas as pl
from jax.experimental.pallas import tpu as pltpu
from jax.sharding import PartitionSpec as P

HEADS = 16
HEAD_DIM = 80
ATT_BLOCK = 256
SOFT_BASE = 1.442695041
EPSILON = 1e-06
MESH = pl.DeviceIdType.MESH
VMEM_BYTES = 60 * 1024 * 1024
FEED_STEPS = 4


class Place:
    def __init__(self, dp, seq):
        self.cores = 2 if dp % 2 == 0 else 1
        self.lines = dp // self.cores
        self.levels = 4 if seq % 4 == 0 else seq
        self.across = seq // self.levels
        self.sizes = {
            "y": self.lines,
            "c": self.cores,
            "z": self.levels,
            "x": self.across,
        }

    def here(self):
        dp = lax.axis_index("dp")
        seq = lax.axis_index("seq")
        return {
            "y": dp // self.cores,
            "c": dp % self.cores,
            "z": seq // self.across,
            "x": seq % self.across,
        }

    def shift(self, spot, axis, step):
        moved = dict(spot)
        moved[axis] = lax.rem(spot[axis] + step, self.sizes[axis])
        return moved

    def device(self, spot):
        return (
            spot["y"] * self.cores + spot["c"],
            spot["z"] * self.across + spot["x"],
        )

    def grid(self):
        return (self.lines, self.cores, self.levels, self.across)

    def greet(self, spot, wide):
        barrier = pltpu.get_barrier_semaphore()
        dp, seq = self.device(spot)
        peers = [
            self.device(self.shift(spot, axis, step))
            for axis in ("yc" if wide else "zxyc")
            for step in range(1, self.sizes[axis])
        ]
        if wide:
            devices = self.levels * self.across
            peers += [(dp, lax.rem(seq + step, devices)) for step in range(1, devices)]
        for peer in peers:
            pl.semaphore_signal(barrier, inc=1, device_id=peer, device_id_type=MESH)
        pl.semaphore_wait(barrier, len(peers))


def halves_of(cols, lean):
    if lean and cols % 640 == 0:
        cut = cols * 4 // 5
    elif cols % 256 == 0:
        cut = cols // 2
    else:
        return ((slice(0, cols), "xy"),)
    return ((slice(0, cut), "xy"), (slice(cut, cols), "yx"))


def chunks_of(rows):
    if rows % 8 == 0 and rows >= 32:
        cut = rows // 32 * 16
        return (slice(0, cut), slice(cut, rows))
    return (slice(0, rows),)


class Sender:
    def __init__(self, place, spot, send_sem, recv_sem):
        self.place = place
        self.spot = spot
        self.send_sem = send_sem
        self.recv_sem = recv_sem
        self.count = itertools.count()
        self.open = {}
        self.every = []

    def put(self, key, device, source, target, leaves=None, comes=None):
        at = next(self.count)
        copy = pltpu.make_async_remote_copy(
            src_ref=source,
            dst_ref=target,
            send_sem=self.send_sem.at[at],
            recv_sem=self.recv_sem.at[at],
            device_id=device,
            device_id_type=MESH,
        )
        self.guard(leaves, copy.start)
        self.open.setdefault(key, []).append((comes, copy))
        self.every.append((leaves, copy))

    def guard(self, when, act):
        if when is None:
            act()
        else:
            pl.when(when)(act)

    def go(self, key, axis, source, target):
        self.open[key] = []
        for step in range(1, self.place.sizes[axis]):
            peer = self.place.shift(self.spot, axis, step)
            self.put(key, self.place.device(peer), source(peer), target(step))

    def chain(self, key, turn, own, slot):
        levels, z = self.place.levels, self.spot["z"]
        self.open[key] = []

        def inside(at):
            return jnp.logical_and(at >= 0, at < levels)

        for way in (1, -1):
            shard, to, back = z - turn * way, z + way, z - (turn + 1) * way
            part = slot(lax.rem(shard + levels, levels))
            peer = dict(self.spot, z=lax.rem(to + levels, levels))
            self.put(
                key,
                self.place.device(peer),
                own if turn == 0 else part,
                part,
                jnp.logical_and(inside(shard), inside(to)),
                inside(back),
            )

    def landed(self, key):
        for comes, copy in self.open[key]:
            self.guard(comes, copy.wait_recv)

    def finish(self):
        for leaves, copy in self.every:
            self.guard(leaves, copy.wait_send)


class Gather:
    def __init__(self, place, spot, lean, tails, shards, wholes, own_sem):
        self.place, self.spot, self.lean, self.tails = place, spot, lean, tails
        self.shards, self.wholes = shards, wholes
        y, c, z, x = (spot[k] for k in "yczx")
        self.own = []
        for n, shard in enumerate(shards):
            if n >= len(shards) - tails:
                target = wholes[n].at[z]
            elif len(shard.shape) == 3:
                target = wholes[n].at[y, c, :, x]
            else:
                target = wholes[n].at[y, c, z, x]
            copy = pltpu.make_async_copy(shard, target, own_sem[n])
            copy.start()
            self.own.append(copy)

    def run(self, out, feed):
        shards, wholes = self.shards, self.wholes
        y, c, _, x = (self.spot[k] for k in "yczx")
        turns = self.place.levels - 1
        full = len(shards) - self.tails
        raw = [n for n, s in enumerate(shards) if len(s.shape) == 2]
        jobs = [(n, r) for n in range(full) for r in chunks_of(shards[n].shape[-2])]
        filled = set()

        def halves(n):
            return enumerate(halves_of(shards[n].shape[-1], self.lean))

        def along(turn, n):
            def slot(level):
                return wholes[n].at[y, c, level, x] if n < full else wholes[n].at[level]

            if turn > 0:
                out.landed(("z", n, turn - 1))
            if turn < turns:
                out.chain(("z", n, turn), turn, shards[n], slot)

        def fill(n):
            if n not in filled:
                filled.add(n)
                self.own[n].wait()

        def two(job, n, rows):
            lined = len(shards[n].shape) == 3
            if not lined:
                fill(n)
            for half, (cols, order) in halves(n):
                part = wholes[n].at[y, c, :, x, rows, cols]
                source = shards[n].at[:, rows, cols] if lined else part
                out.go((job, half, 2), order[0], lambda peer: source, lambda step: part)

        def three(job, n, rows):
            fill(n)
            for half, (cols, order) in halves(n):
                out.landed((job, half, 2))
                if order == "xy":
                    part = wholes[n].at[y, c, :, :, rows, cols]
                else:
                    part = wholes[n].at[:, c, :, x, rows, cols]
                out.go((job, half, 3), order[1], lambda peer: part, lambda step: part)

        def four(job, n, rows):
            for half, (cols, order) in halves(n):
                out.landed((job, half, 3))
                part = wholes[n].at[:, c, :, :, rows, cols]
                out.go((job, half, 4), "c", lambda peer: part, lambda step: part)

        def five(job, n, rows):
            for half, _ in halves(n):
                out.landed((job, half, 4))

        steps = iter(range(len(jobs) + 3))

        def advance():
            step = next(steps, None)
            if step is not None:
                for stage, late in ((two, 0), (three, 1), (four, 2), (five, 3)):
                    if 0 <= step - late < len(jobs):
                        stage(("gather", step - late), *jobs[step - late])

        if raw:
            for time in range(len(raw) + turns):
                for turn in range(turns + 1):
                    if 0 <= time - turn < len(raw):
                        along(turn, raw[time - turn])
                done = time - turns
                if 0 <= done < full:
                    for _ in chunks_of(shards[raw[done]].shape[-2]):
                        advance()
        for _ in range(len(jobs) + 3):
            advance()
            feed()
        for n in range(len(shards)):
            fill(n)


def total(values):
    result = values[0].astype(jnp.float32)
    for value in values[1:]:
        result = result + value.astype(jnp.float32)
    return result


class Scatter:
    def __init__(self, place, spot, lean, parts, totals, boxes, own_sem):
        self.place, self.spot, self.lean = place, spot, lean
        self.parts, self.totals = parts, totals
        self.jobs = [(n, r) for n, p in enumerate(parts) for r in chunks_of(p.shape[-2])]
        self.own_sem = own_sem
        self.sums, self.cores, self.seconds, self.thirds, self.fourths = [], [], [], [], []
        self.results, self.own = [], []
        for n, part in enumerate(parts):
            self.sums.append(boxes.pop(0))
            self.cores.append(boxes.pop(0))
            halves = halves_of(part.shape[-1], lean)
            self.seconds.append([boxes.pop(0) for _ in halves])
            self.thirds.append([boxes.pop(0) for _ in halves])
            self.fourths.append(boxes.pop(0))
            self.results.append(boxes.pop(0))
            copy = pltpu.make_async_copy(
                part.at[:, spot["c"]], self.sums[n], own_sem[n]
            )
            copy.start()
            self.own.append(copy)

    def run(self, out, feed):
        place, parts, sums = self.place, self.parts, self.sums
        cores, results = self.cores, self.results
        y, c, z, x = (self.spot[k] for k in "yczx")
        lines, _, levels, across = place.grid()
        filled = set()

        def halves(n):
            return enumerate(halves_of(parts[n].shape[-1], self.lean))

        def one(job, n, rows):
            out.go(
                (job, 1),
                "c",
                lambda peer: parts[n].at[:, peer["c"], :, :, rows],
                lambda step: cores[n].at[:, :, :, rows],
            )

        def two(job, n, rows):
            if n not in filled:
                filled.add(n)
                self.own[n].wait()
            out.landed((job, 1))
            if place.cores > 1:

                @pl.loop(0, lines * levels * across)
                def _(at):
                    where = (at // (levels * across), (at // across) % levels, at % across)
                    sums[n][where + (rows,)] = total(
                        [sums[n][where + (rows,)], cores[n][where + (rows,)]]
                    ).astype(sums[n].dtype)

            for half, (cols, order) in halves(n):
                box = self.seconds[n][half]
                if order == "xy":
                    out.go(
                        (job, half, 2),
                        "y",
                        lambda peer: sums[n].at[peer["y"], :, :, rows, cols],
                        lambda step: box.at[step - 1, :, :, rows],
                    )
                else:
                    out.go(
                        (job, half, 2),
                        "x",
                        lambda peer: sums[n].at[:, :, peer["x"], rows, cols],
                        lambda step: box.at[step - 1, :, :, rows],
                    )

        def three(job, n, rows):
            for half, (cols, order) in halves(n):
                out.landed((job, half, 2))
                box, later = self.seconds[n][half], self.thirds[n][half]
                if order == "xy":

                    @pl.loop(0, levels * across)
                    def _(at):
                        zz, xx = at // across, at % across
                        values = [sums[n][y, zz, xx, rows, cols]]
                        values += [box[k, zz, xx, rows] for k in range(lines - 1)]
                        sums[n][y, zz, xx, rows, cols] = total(values).astype(sums[n].dtype)

                    out.go(
                        (job, half, 3),
                        "x",
                        lambda peer: sums[n].at[y, :, peer["x"], rows, cols],
                        lambda step: later.at[step - 1, :, rows],
                    )
                else:

                    @pl.loop(0, lines * levels)
                    def _(at):
                        yy, zz = at // levels, at % levels
                        values = [sums[n][yy, zz, x, rows, cols]]
                        values += [box[k, yy, zz, rows] for k in range(across - 1)]
                        sums[n][yy, zz, x, rows, cols] = total(values).astype(sums[n].dtype)

                    out.go(
                        (job, half, 3),
                        "y",
                        lambda peer: sums[n].at[peer["y"], :, x, rows, cols],
                        lambda step: later.at[step - 1, :, rows],
                    )

        def four(job, n, rows):
            for half, (cols, order) in halves(n):
                out.landed((job, half, 3))
                box = self.thirds[n][half]

                @pl.loop(0, levels)
                def _(zz):
                    values = [sums[n][y, zz, x, rows, cols]]
                    values += [box[k, zz, rows] for k in range(box.shape[0])]
                    sums[n][y, zz, x, rows, cols] = total(values).astype(sums[n].dtype)

            out.go(
                (job, 4),
                "z",
                lambda peer: sums[n].at[y, peer["z"], x, rows],
                lambda step: self.fourths[n].at[step - 1, rows],
            )

        def five(job, n, rows):
            out.landed((job, 4))
            values = [sums[n][y, z, x, rows]]
            values += [self.fourths[n][k, rows] for k in range(levels - 1)]
            results[n][rows] = total(values)

        jobs = [(("scatter", at),) + job for at, job in enumerate(self.jobs)]
        for step in range(len(jobs) + 4):
            for stage, late in ((one, 0), (two, 1), (three, 2), (four, 3), (five, 4)):
                if 0 <= step - late < len(jobs):
                    stage(*jobs[step - late])
            feed()
        last = []
        for n, result in enumerate(results):
            copy = pltpu.make_async_copy(result, self.totals[n], self.own_sem[n])
            copy.start()
            last.append(copy)
        for copy in last:
            copy.wait()


def scatter_boxes(place, part, lean):
    lines, _, levels, across = place.grid()
    rows, cols = part.shape[-2:]
    block = pltpu.VMEM((lines, levels, across, rows, cols), part.dtype)
    first, later = [], []
    for piece, order in halves_of(cols, lean):
        size = (rows, piece.stop - piece.start)
        steps = (lines - 1, across - 1) if order == "xy" else (across - 1, lines - 1)
        middle = (levels, across) if order == "xy" else (lines, levels)
        first.append(pltpu.VMEM((steps[0],) + middle + size, part.dtype))
        later.append(pltpu.VMEM((steps[1], levels) + size, part.dtype))
    last = pltpu.VMEM((levels - 1, rows, cols), part.dtype)
    return [block, block] + first + later + [last, pltpu.VMEM((rows, cols), jnp.float32)]


def move_kernel(place, counts, lean, tails, *refs):
    refs = list(refs)
    swaps, gathers, scatters = counts
    whole = swaps + gathers + scatters
    ins, outs, rest = refs[:whole], refs[whole : 2 * whole], refs[2 * whole :]
    own_sem, send_sem, recv_sem = rest[-3:]
    spot = place.here()
    dp, me = place.device(spot)
    devices = place.levels * place.across
    sent, got = ins[:swaps], outs[:swaps]
    own = []
    for n in range(swaps):
        copy = pltpu.make_async_copy(sent[n].at[me], got[n].at[me], own_sem.at[n])
        copy.start()
        own.append(copy)
    cut = swaps + gathers
    gather = Gather(
        place, spot, lean, tails, ins[swaps:cut], outs[swaps:cut], [own_sem.at[n] for n in range(swaps, cut)]
    )
    scatter = Scatter(
        place, spot, lean, ins[cut:], outs[cut:], rest[:-3], [own_sem.at[n] for n in range(cut, whole)]
    )
    place.greet(spot, swaps > 0)
    out = Sender(place, spot, send_sem, recv_sem)
    pending = [(n, step) for n in range(swaps) for step in range(1, devices)]
    each = pl.cdiv(len(pending), FEED_STEPS)

    def feed():
        for n, step in pending[:each]:
            peer = lax.rem(me + step, devices)
            out.put("swap", (dp, peer), sent[n].at[peer], got[n].at[me])
        del pending[:each]

    if gathers:
        gather.run(out, feed)
    if scatters:
        scatter.run(out, feed)
    while pending:
        feed()
    for copy in own:
        copy.wait()
    if swaps:
        out.landed("swap")
    out.finish()


def move(place, collective_id, swaps=(), gathers=(), scatters=(), tails=0):
    lean = len(swaps) > 0
    copies = len(swaps) * (place.levels * place.across - 1)
    boxes = []
    lines, cores, levels, across = place.grid()
    shapes = [jax.ShapeDtypeStruct(a.shape, a.dtype) for a in swaps]
    for n, shard in enumerate(gathers):
        rows, cols = shard.shape[-2:]
        if shard.ndim == 2:
            copies += 2 * (levels - 1)
        grid = place.grid()
        if n < len(gathers) - tails:
            count = len(halves_of(cols, lean)) * (across + lines + cores - 3)
            copies += len(chunks_of(rows)) * count
        else:
            grid = (levels,)
        shapes.append(jax.ShapeDtypeStruct(grid + (rows, cols), shard.dtype))
    for part in scatters:
        count = (levels - 1) + (cores - 1)
        count += len(halves_of(part.shape[-1], lean)) * (lines + across - 2)
        copies += len(chunks_of(part.shape[-2])) * count
        boxes += scatter_boxes(place, part, lean)
    shapes += [jax.ShapeDtypeStruct(p.shape[-2:], jnp.float32) for p in scatters]
    return pl.pallas_call(
        functools.partial(
            move_kernel, place, (len(swaps), len(gathers), len(scatters)), lean, tails
        ),
        out_shape=shapes,
        in_specs=[pl.BlockSpec(memory_space=pl.ANY)] * len(shapes),
        out_specs=[pl.BlockSpec(memory_space=pl.ANY)] * len(shapes),
        scratch_shapes=boxes
        + [
            pltpu.SemaphoreType.DMA((len(shapes),)),
            pltpu.SemaphoreType.DMA((copies,)),
            pltpu.SemaphoreType.DMA((copies,)),
        ],
        compiler_params=pltpu.CompilerParams(
            collective_id=collective_id,
            has_side_effects=True,
            vmem_limit_bytes=VMEM_BYTES,
        ),
        name=f"move_{collective_id}",
    )(*swaps, *gathers, *scatters)


def side_by_side(ref):
    return jnp.concatenate([ref[s] for s in range(ref.shape[0])], axis=1)


def dot_first(left, right):
    return lax.dot_general(
        left, right, (((0,), (0,)), ((), ())), preferred_element_type=jnp.float32
    )


def dot_last(left, right):
    return lax.dot_general(
        left, right, (((1,), (1,)), ((), ())), preferred_element_type=jnp.float32
    )


def attend_kernel(q_ref, k_ref, v_ref, o_ref, full_ref, sum_ref):
    tokens = q_ref.shape[-1]
    each = ATT_BLOCK // tokens
    keys, values = side_by_side(k_ref), side_by_side(v_ref)
    for block in range(q_ref.shape[0] // each):
        first = block * each
        limit = (block + 1) * ATT_BLOCK
        queries = jnp.concatenate([q_ref[first + s] for s in range(each)], axis=1)
        weights = jnp.exp(dot_first(keys[:, :limit], queries))
        sums = jnp.sum(weights, axis=0, keepdims=True)
        mixed = jnp.dot(
            values[:, :limit],
            weights.astype(jnp.bfloat16),
            preferred_element_type=jnp.float32,
        )
        mixed = mixed / sums
        sum_ref[0, 0, :, pl.ds(block * ATT_BLOCK, ATT_BLOCK)] = sums
        for s in range(each):
            piece = mixed[:, s * tokens : (s + 1) * tokens]
            full_ref[first + s] = piece
            o_ref[first + s] = piece.astype(jnp.bfloat16)


def attend_specs(devices, tokens):
    piece = pl.BlockSpec((devices, HEAD_DIM, tokens), lambda m, h: (0, h, m))
    sums = pl.BlockSpec((1, 1, 1, devices * tokens), lambda m, h: (m, h, 0, 0))
    return piece, sums


def attend(queries, keys, values, tokens):
    devices, rows, cols = queries.shape
    grid = (cols // tokens, rows // HEAD_DIM)
    piece, sums = attend_specs(devices, tokens)
    return pl.pallas_call(
        attend_kernel,
        grid=grid,
        out_shape=[
            jax.ShapeDtypeStruct(queries.shape, jnp.bfloat16),
            jax.ShapeDtypeStruct(queries.shape, jnp.float32),
            jax.ShapeDtypeStruct(grid + (1, devices * tokens), jnp.float32),
        ],
        in_specs=[piece] * 3,
        out_specs=[piece, piece, sums],
        compiler_params=pltpu.CompilerParams(vmem_limit_bytes=VMEM_BYTES),
        name="attend",
    )(queries, keys, values)


def slopes_kernel(
    q_ref, k_ref, v_ref, do_ref, full_ref, sum_ref, rate_ref, dq_ref, dk_ref, dv_ref
):
    tokens = q_ref.shape[-1]
    each = ATT_BLOCK // tokens
    keys, values = side_by_side(k_ref), side_by_side(v_ref)
    rate = rate_ref[...]
    key_total = value_total = None
    for block in reversed(range(q_ref.shape[0] // each)):
        first = block * each
        limit = (block + 1) * ATT_BLOCK

        def pick(ref):
            return jnp.concatenate([ref[first + s] for s in range(each)], axis=1)

        queries = pick(q_ref)
        slope = pick(do_ref).astype(jnp.float32)
        sums = sum_ref[0, 0, :, pl.ds(block * ATT_BLOCK, ATT_BLOCK)]
        scaled = (slope / sums).astype(jnp.bfloat16)
        centre = jnp.sum(slope * pick(full_ref), axis=0, keepdims=True) / sums
        weights = jnp.exp(dot_first(keys[:, :limit], queries))
        dots = dot_first(values[:, :limit], scaled)
        slopes = (weights * (dots - centre)).astype(jnp.bfloat16)
        weights = weights.astype(jnp.bfloat16)
        query_part = jnp.dot(keys[:, :limit], slopes, preferred_element_type=jnp.float32)
        query_part = (query_part * rate).astype(jnp.bfloat16)
        for s in range(each):
            dq_ref[first + s] = query_part[:, s * tokens : (s + 1) * tokens]
        key_part = dot_last(queries, slopes)
        value_part = dot_last(scaled, weights)
        if key_total is None:
            key_total, value_total = key_part, value_part
        else:
            key_total = jnp.concatenate(
                [key_total[:, :limit] + key_part, key_total[:, limit:]], axis=1
            )
            value_total = jnp.concatenate(
                [value_total[:, :limit] + value_part, value_total[:, limit:]], axis=1
            )
    for s in range(q_ref.shape[0]):
        cols = slice(s * tokens, (s + 1) * tokens)
        dk_ref[s] = key_total[:, cols].astype(jnp.bfloat16)
        dv_ref[s] = value_total[:, cols].astype(jnp.bfloat16)


def slopes(queries, keys, values, slope, full, sums, rate, tokens):
    devices, rows, cols = queries.shape
    grid = (cols // tokens, rows // HEAD_DIM)
    piece, sum_spec = attend_specs(devices, tokens)
    return pl.pallas_call(
        slopes_kernel,
        grid=grid,
        out_shape=[jax.ShapeDtypeStruct(queries.shape, jnp.bfloat16)] * 3,
        in_specs=[piece] * 5
        + [sum_spec, pl.BlockSpec((HEAD_DIM, 1), lambda m, h: (0, 0))],
        out_specs=[piece] * 3,
        compiler_params=pltpu.CompilerParams(vmem_limit_bytes=VMEM_BYTES),
        name="slopes",
    )(queries, keys, values, slope, full, sums, rate)


def rms_scale(values):
    return lax.rsqrt(jnp.mean(values * values, axis=-1, keepdims=True) + EPSILON)


def contract(spec, left, right):
    return jnp.einsum(spec, left, right, preferred_element_type=jnp.float32)


def on_device(place, devices, *args):
    inputs, cotangent = args[:2]
    (
        norm_one,
        query_mat,
        query_add,
        key_mat,
        value_mat,
        value_add,
        output_mat,
        output_add,
        norm_two,
        hidden_mat,
        hidden_add,
        project_mat,
        project_add,
    ) = args[2:15]
    depth = args[15].astype(jnp.float32)
    micro, tokens, seqs, width = inputs.shape
    rows = micro * tokens * seqs
    vectors = (norm_one, query_add, value_add, output_add, norm_two, hidden_add, project_add)
    share = norm_one.shape[0]
    small = jnp.pad(jnp.stack(vectors), ((0, 16 - len(vectors)), (0, 128 - share)))
    query_mat, small, key_mat, value_mat, output_mat, hidden_mat, project_mat = move(
        place,
        0,
        gathers=(query_mat, small, key_mat, value_mat, output_mat, hidden_mat, project_mat),
        tails=3,
    )
    small = small.reshape(-1, 16, 128)[:, : len(vectors), :share]
    small = small.transpose(1, 0, 2).reshape(len(vectors), width).astype(jnp.float32)
    gain_one, query_add, value_add, output_add, gain_two, hidden_add, project_add = small
    query_mat, key_mat, value_mat = (
        g.reshape(width, width) for g in (query_mat, key_mat, value_mat)
    )

    def to_rows(array):
        return array.transpose(0, 2, 1, 3).reshape(rows, width)

    def from_rows(array):
        return array.reshape(micro, seqs, tokens, width).transpose(0, 2, 1, 3)

    rate = SOFT_BASE / math.sqrt(HEAD_DIM) * jax.nn.softplus(depth)
    rate_full = jnp.tile(rate, HEADS)[:, None]
    xfloat = to_rows(inputs).astype(jnp.float32)
    inv_one = rms_scale(xfloat)
    normed = (xfloat * inv_one * gain_one).astype(jnp.bfloat16)
    query_pre = contract("df,rd->fr", query_mat, normed) + query_add[:, None]
    queries = (query_pre * rate_full).astype(jnp.bfloat16)
    keys = contract("df,rd->fr", key_mat, normed).astype(jnp.bfloat16)
    values = (contract("df,rd->fr", value_mat, normed) + value_add[:, None]).astype(jnp.bfloat16)

    def split(array):
        return array.reshape(devices, width // devices, rows)

    q_in, k_in, v_in, output_mat, hidden_mat = move(
        place, 1, (split(queries), split(keys), split(values)), (output_mat, hidden_mat)
    )
    output_mat, hidden_mat = (g.reshape(width, width) for g in (output_mat, hidden_mat))
    mixed, full, sums = attend(q_in, k_in, v_in, tokens)
    mixed, project_mat = move(place, 2, (mixed,), (project_mat,))
    mixed, project_mat = mixed.reshape(width, rows), project_mat.reshape(width, width)
    residual = xfloat + (contract("fr,fd->rd", mixed, output_mat) + output_add)
    inv_two = rms_scale(residual)
    second = (residual * inv_two * gain_two).astype(jnp.bfloat16)
    hidden_pre = contract("rd,df->rf", second, hidden_mat) + hidden_add
    active = jax.nn.silu(hidden_pre).astype(jnp.bfloat16)
    result = residual + (contract("rf,fd->rd", active, project_mat) + project_add)
    result = from_rows(result.astype(jnp.bfloat16))

    upper = to_rows(cotangent)
    project_grad = contract("rf,rd->fd", active, upper)
    project_bias_grad = jnp.sum(upper.astype(jnp.float32), axis=0)
    active_grad = contract("rd,fd->rf", upper, project_mat)
    logistic = jax.nn.sigmoid(hidden_pre)
    hidden_grad = (active_grad * logistic * (1.0 + hidden_pre * (1.0 - logistic))).astype(
        jnp.bfloat16
    )
    hidden_mat_grad = contract("rd,rf->df", second, hidden_grad)
    hidden_bias_grad = jnp.sum(hidden_grad.astype(jnp.float32), axis=0)
    second_grad = contract("rf,df->rd", hidden_grad, hidden_mat)
    normal_two = residual * inv_two
    scaled_two = second_grad * gain_two
    norm_two_grad = jnp.sum(second_grad * normal_two, axis=0)
    residual_grad = upper.astype(jnp.float32) + inv_two * (
        scaled_two - normal_two * jnp.mean(scaled_two * normal_two, axis=-1, keepdims=True)
    )
    branch_grad = residual_grad.astype(jnp.bfloat16)
    output_mat_grad = contract("fr,rd->fd", mixed, branch_grad)
    output_bias_grad = jnp.sum(branch_grad.astype(jnp.float32), axis=0)
    mixed_grad = contract("fd,rd->fr", output_mat, branch_grad).astype(jnp.bfloat16)

    def as_parts(*grads):
        return tuple(
            g.astype(jnp.bfloat16).reshape(place.grid() + (share, width)) for g in grads
        )

    merged = share % 8 == 0
    early = as_parts(project_grad) if merged else ()
    do_in, *early = move(place, 3, (split(mixed_grad),), (), early)
    slopes_out = slopes(q_in, k_in, v_in, do_in, full, sums, rate[:, None], tokens)
    middle = as_parts(hidden_mat_grad, output_mat_grad) if merged else ()
    query_slope, key_grad, value_grad, *middle = move(place, 4, slopes_out, (), middle)
    query_slope, key_grad, value_grad = (
        a.reshape(width, rows) for a in (query_slope, key_grad, value_grad)
    )
    query_float = query_slope.astype(jnp.float32)
    scale_part = jnp.sum(query_float / rate_full * query_pre, axis=1)
    scale_part = jnp.sum(scale_part.reshape(HEADS, HEAD_DIM), axis=0)
    query_mat_grad = contract("rd,fr->df", normed, query_slope)
    query_bias_grad = jnp.sum(query_float, axis=1)
    key_mat_grad = contract("rd,fr->df", normed, key_grad)
    value_mat_grad = contract("rd,fr->df", normed, value_grad)
    value_bias_grad = jnp.sum(value_grad.astype(jnp.float32), axis=1)
    normed_grad = (
        contract("fr,df->rd", query_slope, query_mat)
        + contract("fr,df->rd", key_grad, key_mat)
        + contract("fr,df->rd", value_grad, value_mat)
    )
    normal_one = xfloat * inv_one
    scaled_one = normed_grad * gain_one
    norm_one_grad = jnp.sum(normed_grad * normal_one, axis=0)
    source_grad = residual_grad + inv_one * (
        scaled_one - normal_one * jnp.mean(scaled_one * normal_one, axis=-1, keepdims=True)
    )
    source_grad = from_rows(source_grad.astype(jnp.bfloat16))

    vector_grads = jnp.stack(
        (
            norm_one_grad,
            query_bias_grad,
            value_bias_grad,
            output_bias_grad,
            norm_two_grad,
            hidden_bias_grad,
            project_bias_grad,
        )
    )
    vector_grads = vector_grads.reshape(7, -1, share).transpose(1, 0, 2)
    vector_grads = jnp.pad(vector_grads, ((0, 0), (0, 0), (0, 128 - share)))
    scale_row = jnp.pad(scale_part, (0, 128 - HEAD_DIM))
    scale_row = jnp.broadcast_to(scale_row, (vector_grads.shape[0], 1, 128))
    vector_grads = jnp.concatenate([vector_grads, scale_row], axis=1)
    vector_grads = vector_grads.reshape(place.grid() + (8, 128))
    late = as_parts(query_mat_grad, key_mat_grad, value_mat_grad)
    if merged:
        *late, vector_sums = move(place, 5, scatters=late + (vector_grads,))
    else:
        (vector_sums,) = move(place, 5, scatters=(vector_grads,))
        early = as_parts(project_grad, hidden_mat_grad, output_mat_grad)
        early, *middle = ([move(place, 6, scatters=(p,))[0] for p in early])
        early = [early]
        late = [move(place, 6, scatters=(p,))[0] for p in late]
    (project_grad,) = early
    hidden_mat_grad, output_mat_grad = middle
    query_mat_grad, key_mat_grad, value_mat_grad = late
    g_one, g_query, g_value, g_output, g_two, g_hidden, g_project = (
        vector_sums[n, :share] for n in range(7)
    )
    scale_summed = vector_sums[7, :HEAD_DIM]
    depth_grad = scale_summed * (SOFT_BASE / math.sqrt(HEAD_DIM)) * jax.nn.sigmoid(depth)
    return (
        result,
        source_grad,
        g_one,
        query_mat_grad,
        g_query,
        key_mat_grad,
        value_mat_grad,
        g_value,
        output_mat_grad,
        g_output,
        g_two,
        hidden_mat_grad,
        g_hidden,
        project_grad,
        g_project,
        depth_grad,
    )


def solution(mesh):
    both = ("dp", "seq")
    token, vector, matrix = P(None, "seq", "dp", None), P(both), P(both, None)
    weights = (
        vector,
        matrix,
        vector,
        matrix,
        matrix,
        vector,
        matrix,
        vector,
        vector,
        matrix,
        vector,
        matrix,
        vector,
    )
    specs = (token, token) + weights + (P(),)
    place = Place(mesh.shape["dp"], mesh.shape["seq"])
    return jax.shard_map(
        functools.partial(on_device, place, mesh.shape["seq"]),
        mesh=mesh,
        in_specs=specs,
        out_specs=specs,
        check_vma=False,
    )
```

```python
import functools
import itertools
import math

import jax
import jax.numpy as jnp
from jax import lax
from jax.experimental import pallas as pl
from jax.experimental.pallas import tpu as pltpu
from jax.sharding import PartitionSpec as P

HEADS = 16
HEAD_DIM = 80
ATT_BLOCK = 256
SOFT_BASE = 1.442695041
EPSILON = 1e-06
MESH = pl.DeviceIdType.MESH
VMEM_BYTES = 60 * 1024 * 1024
FEED_STEPS = 4


class Place:
    def __init__(self, dp, seq):
        self.cores = 2 if dp % 2 == 0 else 1
        self.lines = dp // self.cores
        self.levels = 4 if seq % 4 == 0 else seq
        self.across = seq // self.levels
        self.sizes = {
            "y": self.lines,
            "c": self.cores,
            "z": self.levels,
            "x": self.across,
        }

    def here(self):
        dp = lax.axis_index("dp")
        seq = lax.axis_index("seq")
        return {
            "y": dp // self.cores,
            "c": dp % self.cores,
            "z": seq // self.across,
            "x": seq % self.across,
        }

    def shift(self, spot, axis, step):
        moved = dict(spot)
        moved[axis] = lax.rem(spot[axis] + step, self.sizes[axis])
        return moved

    def device(self, spot):
        return (
            spot["y"] * self.cores + spot["c"],
            spot["z"] * self.across + spot["x"],
        )

    def grid(self):
        return (self.lines, self.cores, self.levels, self.across)

    def greet(self, spot, wide):
        barrier = pltpu.get_barrier_semaphore()
        dp, seq = self.device(spot)
        peers = [
            self.device(self.shift(spot, axis, step))
            for axis in ("yc" if wide else "zxyc")
            for step in range(1, self.sizes[axis])
        ]
        if wide:
            devices = self.levels * self.across
            peers += [(dp, lax.rem(seq + step, devices)) for step in range(1, devices)]
        for peer in peers:
            pl.semaphore_signal(barrier, inc=1, device_id=peer, device_id_type=MESH)
        pl.semaphore_wait(barrier, len(peers))


def halves_of(cols, lean):
    if lean and cols % 640 == 0:
        cut = cols * 4 // 5
    elif cols % 256 == 0:
        cut = cols // 2
    else:
        return ((slice(0, cols), "xy"),)
    return ((slice(0, cut), "xy"), (slice(cut, cols), "yx"))


def chunks_of(rows):
    if rows % 8 == 0 and rows >= 32:
        cut = rows // 32 * 16
        return (slice(0, cut), slice(cut, rows))
    return (slice(0, rows),)


class Sender:
    def __init__(self, place, spot, send_sem, recv_sem):
        self.place = place
        self.spot = spot
        self.send_sem = send_sem
        self.recv_sem = recv_sem
        self.count = itertools.count()
        self.open = {}
        self.every = []

    def put(self, key, device, source, target, leaves=None, comes=None):
        at = next(self.count)
        copy = pltpu.make_async_remote_copy(
            src_ref=source,
            dst_ref=target,
            send_sem=self.send_sem.at[at],
            recv_sem=self.recv_sem.at[at],
            device_id=device,
            device_id_type=MESH,
        )
        self.guard(leaves, copy.start)
        self.open.setdefault(key, []).append((comes, copy))
        self.every.append((leaves, copy))

    def guard(self, when, act):
        if when is None:
            act()
        else:
            pl.when(when)(act)

    def go(self, key, axis, source, target):
        self.open[key] = []
        for step in range(1, self.place.sizes[axis]):
            peer = self.place.shift(self.spot, axis, step)
            self.put(key, self.place.device(peer), source(peer), target(step))

    def chain(self, key, turn, own, slot):
        levels, z = self.place.levels, self.spot["z"]
        self.open[key] = []

        def inside(at):
            return jnp.logical_and(at >= 0, at < levels)

        for way in (1, -1):
            shard, to, back = z - turn * way, z + way, z - (turn + 1) * way
            part = slot(lax.rem(shard + levels, levels))
            peer = dict(self.spot, z=lax.rem(to + levels, levels))
            self.put(
                key,
                self.place.device(peer),
                own if turn == 0 else part,
                part,
                jnp.logical_and(inside(shard), inside(to)),
                inside(back),
            )

    def landed(self, key):
        for comes, copy in self.open[key]:
            self.guard(comes, copy.wait_recv)

    def finish(self):
        for leaves, copy in self.every:
            self.guard(leaves, copy.wait_send)


class Gather:
    def __init__(self, place, spot, lean, tails, shards, wholes, own_sem):
        self.place, self.spot, self.lean, self.tails = place, spot, lean, tails
        self.shards, self.wholes = shards, wholes
        y, c, z, x = (spot[k] for k in "yczx")
        self.own = []
        for n, shard in enumerate(shards):
            if n >= len(shards) - tails:
                target = wholes[n].at[z]
            elif len(shard.shape) == 3:
                target = wholes[n].at[y, c, :, x]
            else:
                target = wholes[n].at[y, c, z, x]
            copy = pltpu.make_async_copy(shard, target, own_sem[n])
            copy.start()
            self.own.append(copy)

    def run(self, out, feed):
        shards, wholes = self.shards, self.wholes
        y, c, _, x = (self.spot[k] for k in "yczx")
        turns = self.place.levels - 1
        full = len(shards) - self.tails
        raw = [n for n, s in enumerate(shards) if len(s.shape) == 2]
        jobs = [(n, r) for n in range(full) for r in chunks_of(shards[n].shape[-2])]
        filled = set()

        def halves(n):
            return enumerate(halves_of(shards[n].shape[-1], self.lean))

        def along(turn, n):
            def slot(level):
                return wholes[n].at[y, c, level, x] if n < full else wholes[n].at[level]

            if turn > 0:
                out.landed(("z", n, turn - 1))
            if turn < turns:
                out.chain(("z", n, turn), turn, shards[n], slot)

        def fill(n):
            if n not in filled:
                filled.add(n)
                self.own[n].wait()

        def two(job, n, rows):
            lined = len(shards[n].shape) == 3
            if not lined:
                fill(n)
            for half, (cols, order) in halves(n):
                part = wholes[n].at[y, c, :, x, rows, cols]
                source = shards[n].at[:, rows, cols] if lined else part
                out.go((job, half, 2), order[0], lambda peer: source, lambda step: part)

        def three(job, n, rows):
            fill(n)
            for half, (cols, order) in halves(n):
                out.landed((job, half, 2))
                if order == "xy":
                    part = wholes[n].at[y, c, :, :, rows, cols]
                else:
                    part = wholes[n].at[:, c, :, x, rows, cols]
                out.go((job, half, 3), order[1], lambda peer: part, lambda step: part)

        def four(job, n, rows):
            for half, (cols, order) in halves(n):
                out.landed((job, half, 3))
                part = wholes[n].at[:, c, :, :, rows, cols]
                out.go((job, half, 4), "c", lambda peer: part, lambda step: part)

        def five(job, n, rows):
            for half, _ in halves(n):
                out.landed((job, half, 4))

        steps = iter(range(len(jobs) + 3))

        def advance():
            step = next(steps, None)
            if step is not None:
                for stage, late in ((two, 0), (three, 1), (four, 2), (five, 3)):
                    if 0 <= step - late < len(jobs):
                        stage(("gather", step - late), *jobs[step - late])

        if raw:
            for time in range(len(raw) + turns):
                for turn in range(turns + 1):
                    if 0 <= time - turn < len(raw):
                        along(turn, raw[time - turn])
                done = time - turns
                if 0 <= done < full:
                    for _ in chunks_of(shards[raw[done]].shape[-2]):
                        advance()
        for _ in range(len(jobs) + 3):
            advance()
            feed()
        for n in range(len(shards)):
            fill(n)


def total(values):
    result = values[0].astype(jnp.float32)
    for value in values[1:]:
        result = result + value.astype(jnp.float32)
    return result


class Scatter:
    def __init__(self, place, spot, lean, held, parts, totals, boxes, own_sem):
        self.place, self.spot, self.lean = place, spot, lean
        self.parts, self.totals = parts, totals
        self.full = len(parts) - held
        self.jobs = [
            (n, r)
            for n, p in enumerate(parts)
            if len(p.shape) > 3
            for r in chunks_of(p.shape[-2])
        ]
        self.own_sem = own_sem
        self.sums, self.cores, self.seconds, self.thirds, self.fourths = [], [], [], [], []
        self.results, self.own = [], []
        for n, part in enumerate(parts):
            self.sums.append(boxes.pop(0))
            if len(part.shape) > 3:
                self.cores.append(boxes.pop(0))
                halves = halves_of(part.shape[-1], lean)
                self.seconds.append([boxes.pop(0) for _ in halves])
                self.thirds.append([boxes.pop(0) for _ in halves])
                mine = part.at[:, spot["c"]]
            else:
                for boxed in (self.cores, self.seconds, self.thirds):
                    boxed.append(None)
                mine = part.at[spot["z"]]
            if n < self.full:
                self.fourths.append(boxes.pop(0))
                self.results.append(boxes.pop(0))
            else:
                self.fourths.append(None)
                self.results.append(self.sums[n].at[spot["y"], :, spot["x"]])
            copy = pltpu.make_async_copy(mine, self.sums[n], own_sem[n])
            copy.start()
            self.own.append(copy)

    def run(self, out, feed):
        place, parts, sums = self.place, self.parts, self.sums
        cores, results = self.cores, self.results
        y, c, z, x = (self.spot[k] for k in "yczx")
        lines, _, levels, across = place.grid()
        filled = set()

        def halves(n):
            return enumerate(halves_of(parts[n].shape[-1], self.lean))

        def one(job, n, rows):
            out.go(
                (job, 1),
                "c",
                lambda peer: parts[n].at[:, peer["c"], :, :, rows],
                lambda step: cores[n].at[:, :, :, rows],
            )

        def two(job, n, rows):
            if n not in filled:
                filled.add(n)
                self.own[n].wait()
            out.landed((job, 1))
            if place.cores > 1:

                @pl.loop(0, lines * levels * across)
                def _(at):
                    where = (at // (levels * across), (at // across) % levels, at % across)
                    sums[n][where + (rows,)] = total(
                        [sums[n][where + (rows,)], cores[n][where + (rows,)]]
                    ).astype(sums[n].dtype)

            for half, (cols, order) in halves(n):
                box = self.seconds[n][half]
                if order == "xy":
                    out.go(
                        (job, half, 2),
                        "y",
                        lambda peer: sums[n].at[peer["y"], :, :, rows, cols],
                        lambda step: box.at[step - 1, :, :, rows],
                    )
                else:
                    out.go(
                        (job, half, 2),
                        "x",
                        lambda peer: sums[n].at[:, :, peer["x"], rows, cols],
                        lambda step: box.at[step - 1, :, :, rows],
                    )

        def three(job, n, rows):
            for half, (cols, order) in halves(n):
                out.landed((job, half, 2))
                box, later = self.seconds[n][half], self.thirds[n][half]
                if order == "xy":

                    @pl.loop(0, levels * across)
                    def _(at):
                        zz, xx = at // across, at % across
                        values = [sums[n][y, zz, xx, rows, cols]]
                        values += [box[k, zz, xx, rows] for k in range(lines - 1)]
                        sums[n][y, zz, xx, rows, cols] = total(values).astype(sums[n].dtype)

                    out.go(
                        (job, half, 3),
                        "x",
                        lambda peer: sums[n].at[y, :, peer["x"], rows, cols],
                        lambda step: later.at[step - 1, :, rows],
                    )
                else:

                    @pl.loop(0, lines * levels)
                    def _(at):
                        yy, zz = at // levels, at % levels
                        values = [sums[n][yy, zz, x, rows, cols]]
                        values += [box[k, yy, zz, rows] for k in range(across - 1)]
                        sums[n][yy, zz, x, rows, cols] = total(values).astype(sums[n].dtype)

                    out.go(
                        (job, half, 3),
                        "y",
                        lambda peer: sums[n].at[peer["y"], :, x, rows, cols],
                        lambda step: later.at[step - 1, :, rows],
                    )

        def four(job, n, rows):
            for half, (cols, order) in halves(n):
                out.landed((job, half, 3))
                box = self.thirds[n][half]

                @pl.loop(0, levels)
                def _(zz):
                    values = [sums[n][y, zz, x, rows, cols]]
                    values += [box[k, zz, rows] for k in range(box.shape[0])]
                    sums[n][y, zz, x, rows, cols] = total(values).astype(sums[n].dtype)

            if n < self.full:
                out.go(
                    (job, 4),
                    "z",
                    lambda peer: sums[n].at[y, peer["z"], x, rows],
                    lambda step: self.fourths[n].at[step - 1, rows],
                )

        def five(job, n, rows):
            if n >= self.full:
                return
            out.landed((job, 4))
            values = [sums[n][y, z, x, rows]]
            values += [self.fourths[n][k, rows] for k in range(levels - 1)]
            results[n][rows] = total(values)

        def first(n):
            out.go(
                ("tail", n),
                "z",
                lambda peer: parts[n].at[peer["z"]],
                lambda step: self.fourths[n].at[step - 1],
            )

        def final(n):
            self.own[n].wait()
            out.landed(("tail", n))
            values = [sums[n][...]] + [self.fourths[n][k] for k in range(levels - 1)]
            results[n][...] = total(values)

        jobs = [(("scatter", at),) + job for at, job in enumerate(self.jobs)]
        tails = [n for n, p in enumerate(parts) if len(p.shape) == 3]
        for n in tails:
            first(n)
        for step in range(len(jobs) + 4):
            if step > 2 and tails:
                final(tails.pop(0))
            for stage, late in ((one, 0), (two, 1), (three, 2), (four, 3), (five, 4)):
                if 0 <= step - late < len(jobs):
                    stage(*jobs[step - late])
            feed()
        last = []
        for n, result in enumerate(results):
            copy = pltpu.make_async_copy(result, self.totals[n], self.own_sem[n])
            copy.start()
            last.append(copy)
        for copy in last:
            copy.wait()


def scatter_boxes(place, part, lean, held):
    lines, _, levels, across = place.grid()
    rows, cols = part.shape[-2:]
    final = [
        pltpu.VMEM((levels - 1, rows, cols), part.dtype),
        pltpu.VMEM((rows, cols), jnp.float32),
    ]
    if part.ndim == 3:
        return [pltpu.VMEM((rows, cols), part.dtype)] + final
    block = pltpu.VMEM((lines, levels, across, rows, cols), part.dtype)
    first, later = [], []
    for piece, order in halves_of(cols, lean):
        size = (rows, piece.stop - piece.start)
        steps = (lines - 1, across - 1) if order == "xy" else (across - 1, lines - 1)
        middle = (levels, across) if order == "xy" else (lines, levels)
        first.append(pltpu.VMEM((steps[0],) + middle + size, part.dtype))
        later.append(pltpu.VMEM((steps[1], levels) + size, part.dtype))
    return [block, block] + first + later + ([] if held else final)


def move_kernel(place, counts, lean, tails, held, *refs):
    refs = list(refs)
    swaps, gathers, scatters = counts
    whole = swaps + gathers + scatters
    ins, outs, rest = refs[:whole], refs[whole : 2 * whole], refs[2 * whole :]
    own_sem, send_sem, recv_sem = rest[-3:]
    spot = place.here()
    dp, me = place.device(spot)
    devices = place.levels * place.across
    sent, got = ins[:swaps], outs[:swaps]
    own = []
    for n in range(swaps):
        copy = pltpu.make_async_copy(sent[n].at[me], got[n].at[me], own_sem.at[n])
        copy.start()
        own.append(copy)
    cut = swaps + gathers
    gather = Gather(
        place, spot, lean, tails, ins[swaps:cut], outs[swaps:cut], [own_sem.at[n] for n in range(swaps, cut)]
    )
    scatter = Scatter(
        place, spot, lean, held, ins[cut:], outs[cut:], rest[:-3], [own_sem.at[n] for n in range(cut, whole)]
    )
    place.greet(spot, swaps > 0)
    out = Sender(place, spot, send_sem, recv_sem)
    pending = [(n, step) for n in range(swaps) for step in range(1, devices)]
    each = pl.cdiv(len(pending), FEED_STEPS)

    def feed():
        for n, step in pending[:each]:
            peer = lax.rem(me + step, devices)
            out.put("swap", (dp, peer), sent[n].at[peer], got[n].at[me])
        del pending[:each]

    if gathers:
        gather.run(out, feed)
    if scatters:
        scatter.run(out, feed)
    while pending:
        feed()
    for copy in own:
        copy.wait()
    if swaps:
        out.landed("swap")
    out.finish()


def move(place, collective_id, swaps=(), gathers=(), scatters=(), tails=0, held=0):
    lean = len(swaps) > 0
    copies = len(swaps) * (place.levels * place.across - 1)
    boxes = []
    lines, cores, levels, across = place.grid()
    shapes = [jax.ShapeDtypeStruct(a.shape, a.dtype) for a in swaps]
    for n, shard in enumerate(gathers):
        rows, cols = shard.shape[-2:]
        if shard.ndim == 2:
            copies += 2 * (levels - 1)
        grid = place.grid()
        if n < len(gathers) - tails:
            count = len(halves_of(cols, lean)) * (across + lines + cores - 3)
            copies += len(chunks_of(rows)) * count
        else:
            grid = (levels,)
        shapes.append(jax.ShapeDtypeStruct(grid + (rows, cols), shard.dtype))
    for n, part in enumerate(scatters):
        rows, cols = part.shape[-2:]
        keeps = n >= len(scatters) - held
        count = 0 if keeps else levels - 1
        if part.ndim > 3:
            count += (cores - 1) + len(halves_of(cols, lean)) * (lines + across - 2)
            count *= len(chunks_of(rows))
        copies += count
        boxes += scatter_boxes(place, part, lean, keeps)
        shapes.append(
            jax.ShapeDtypeStruct((levels, rows, cols), part.dtype)
            if keeps
            else jax.ShapeDtypeStruct((rows, cols), jnp.float32)
        )

    def is_result(a):
        return a.dtype == jnp.float32 and a.shape[-1] > 128

    return pl.pallas_call(
        functools.partial(
            move_kernel, place, (len(swaps), len(gathers), len(scatters)), lean, tails, held
        ),
        out_shape=shapes,
        in_specs=[pl.BlockSpec(memory_space=pl.ANY)] * len(shapes),
        out_specs=[
            pl.BlockSpec(memory_space=pltpu.HBM if is_result(a) else pl.ANY)
            for a in shapes
        ],
        scratch_shapes=boxes
        + [
            pltpu.SemaphoreType.DMA((len(shapes),)),
            pltpu.SemaphoreType.DMA((copies,)),
            pltpu.SemaphoreType.DMA((copies,)),
        ],
        compiler_params=pltpu.CompilerParams(
            collective_id=collective_id,
            has_side_effects=True,
            vmem_limit_bytes=VMEM_BYTES,
        ),
        name=f"move_{collective_id}",
    )(*swaps, *gathers, *scatters)


def side_by_side(ref):
    return jnp.concatenate([ref[s] for s in range(ref.shape[0])], axis=1)


def dot_first(left, right):
    return lax.dot_general(
        left, right, (((0,), (0,)), ((), ())), preferred_element_type=jnp.float32
    )


def dot_last(left, right):
    return lax.dot_general(
        left, right, (((1,), (1,)), ((), ())), preferred_element_type=jnp.float32
    )


def attend_kernel(q_ref, k_ref, v_ref, o_ref, full_ref, sum_ref):
    tokens = q_ref.shape[-1]
    each = ATT_BLOCK // tokens
    keys, values = side_by_side(k_ref), side_by_side(v_ref)
    for block in range(q_ref.shape[0] // each):
        first = block * each
        limit = (block + 1) * ATT_BLOCK
        queries = jnp.concatenate([q_ref[first + s] for s in range(each)], axis=1)
        weights = jnp.exp(dot_first(keys[:, :limit], queries))
        sums = jnp.sum(weights, axis=0, keepdims=True)
        mixed = jnp.dot(
            values[:, :limit],
            weights.astype(jnp.bfloat16),
            preferred_element_type=jnp.float32,
        )
        mixed = mixed / sums
        sum_ref[0, 0, :, pl.ds(block * ATT_BLOCK, ATT_BLOCK)] = sums
        for s in range(each):
            piece = mixed[:, s * tokens : (s + 1) * tokens]
            full_ref[first + s] = piece
            o_ref[first + s] = piece.astype(jnp.bfloat16)


def attend_specs(devices, tokens):
    piece = pl.BlockSpec((devices, HEAD_DIM, tokens), lambda m, h: (0, h, m))
    sums = pl.BlockSpec((1, 1, 1, devices * tokens), lambda m, h: (m, h, 0, 0))
    return piece, sums


def attend(queries, keys, values, tokens):
    devices, rows, cols = queries.shape
    grid = (cols // tokens, rows // HEAD_DIM)
    piece, sums = attend_specs(devices, tokens)
    return pl.pallas_call(
        attend_kernel,
        grid=grid,
        out_shape=[
            jax.ShapeDtypeStruct(queries.shape, jnp.bfloat16),
            jax.ShapeDtypeStruct(queries.shape, jnp.float32),
            jax.ShapeDtypeStruct(grid + (1, devices * tokens), jnp.float32),
        ],
        in_specs=[piece] * 3,
        out_specs=[piece, piece, sums],
        compiler_params=pltpu.CompilerParams(vmem_limit_bytes=VMEM_BYTES),
        name="attend",
    )(queries, keys, values)


def slopes_kernel(
    q_ref, k_ref, v_ref, do_ref, full_ref, sum_ref, rate_ref, dq_ref, dk_ref, dv_ref
):
    tokens = q_ref.shape[-1]
    each = ATT_BLOCK // tokens
    keys, values = side_by_side(k_ref), side_by_side(v_ref)
    rate = rate_ref[...]
    key_total = value_total = None
    for block in reversed(range(q_ref.shape[0] // each)):
        first = block * each
        limit = (block + 1) * ATT_BLOCK

        def pick(ref):
            return jnp.concatenate([ref[first + s] for s in range(each)], axis=1)

        queries = pick(q_ref)
        slope = pick(do_ref).astype(jnp.float32)
        sums = sum_ref[0, 0, :, pl.ds(block * ATT_BLOCK, ATT_BLOCK)]
        scaled = (slope / sums).astype(jnp.bfloat16)
        centre = jnp.sum(slope * pick(full_ref), axis=0, keepdims=True) / sums
        weights = jnp.exp(dot_first(keys[:, :limit], queries))
        dots = dot_first(values[:, :limit], scaled)
        slopes = (weights * (dots - centre)).astype(jnp.bfloat16)
        weights = weights.astype(jnp.bfloat16)
        query_part = jnp.dot(keys[:, :limit], slopes, preferred_element_type=jnp.float32)
        query_part = (query_part * rate).astype(jnp.bfloat16)
        for s in range(each):
            dq_ref[first + s] = query_part[:, s * tokens : (s + 1) * tokens]
        key_part = dot_last(queries, slopes)
        value_part = dot_last(scaled, weights)
        if key_total is None:
            key_total, value_total = key_part, value_part
        else:
            key_total = jnp.concatenate(
                [key_total[:, :limit] + key_part, key_total[:, limit:]], axis=1
            )
            value_total = jnp.concatenate(
                [value_total[:, :limit] + value_part, value_total[:, limit:]], axis=1
            )
    for s in range(q_ref.shape[0]):
        cols = slice(s * tokens, (s + 1) * tokens)
        dk_ref[s] = key_total[:, cols].astype(jnp.bfloat16)
        dv_ref[s] = value_total[:, cols].astype(jnp.bfloat16)


def slopes(queries, keys, values, slope, full, sums, rate, tokens):
    devices, rows, cols = queries.shape
    grid = (cols // tokens, rows // HEAD_DIM)
    piece, sum_spec = attend_specs(devices, tokens)
    return pl.pallas_call(
        slopes_kernel,
        grid=grid,
        out_shape=[jax.ShapeDtypeStruct(queries.shape, jnp.bfloat16)] * 3,
        in_specs=[piece] * 5
        + [sum_spec, pl.BlockSpec((HEAD_DIM, 1), lambda m, h: (0, 0))],
        out_specs=[piece] * 3,
        compiler_params=pltpu.CompilerParams(vmem_limit_bytes=VMEM_BYTES),
        name="slopes",
    )(queries, keys, values, slope, full, sums, rate)


def rms_scale(values):
    return lax.rsqrt(jnp.mean(values * values, axis=-1, keepdims=True) + EPSILON)


def contract(spec, left, right):
    return jnp.einsum(spec, left, right, preferred_element_type=jnp.float32)


def on_device(place, devices, *args):
    inputs, cotangent = args[:2]
    (
        norm_one,
        query_mat,
        query_add,
        key_mat,
        value_mat,
        value_add,
        output_mat,
        output_add,
        norm_two,
        hidden_mat,
        hidden_add,
        project_mat,
        project_add,
    ) = args[2:15]
    depth = args[15].astype(jnp.float32)
    micro, tokens, seqs, width = inputs.shape
    rows = micro * tokens * seqs
    vectors = (norm_one, query_add, value_add, output_add, norm_two, hidden_add, project_add)
    share = norm_one.shape[0]
    small = jnp.pad(jnp.stack(vectors), ((0, 16 - len(vectors)), (0, 128 - share)))
    query_mat, small, key_mat, value_mat, output_mat, hidden_mat, project_mat = move(
        place,
        0,
        gathers=(query_mat, small, key_mat, value_mat, output_mat, hidden_mat, project_mat),
        tails=3,
    )
    small = small.reshape(-1, 16, 128)[:, : len(vectors), :share]
    small = small.transpose(1, 0, 2).reshape(len(vectors), width).astype(jnp.float32)
    gain_one, query_add, value_add, output_add, gain_two, hidden_add, project_add = small
    query_mat, key_mat, value_mat = (
        g.reshape(width, width) for g in (query_mat, key_mat, value_mat)
    )

    def to_rows(array):
        return array.transpose(0, 2, 1, 3).reshape(rows, width)

    def from_rows(array):
        return array.reshape(micro, seqs, tokens, width).transpose(0, 2, 1, 3)

    rate = SOFT_BASE / math.sqrt(HEAD_DIM) * jax.nn.softplus(depth)
    rate_full = jnp.tile(rate, HEADS)[:, None]
    xfloat = to_rows(inputs).astype(jnp.float32)
    inv_one = rms_scale(xfloat)
    normed = (xfloat * inv_one * gain_one).astype(jnp.bfloat16)
    query_pre = contract("df,rd->fr", query_mat, normed) + query_add[:, None]
    queries = (query_pre * rate_full).astype(jnp.bfloat16)
    keys = contract("df,rd->fr", key_mat, normed).astype(jnp.bfloat16)
    values = (contract("df,rd->fr", value_mat, normed) + value_add[:, None]).astype(jnp.bfloat16)

    def split(array):
        return array.reshape(devices, width // devices, rows)

    q_in, k_in, v_in, output_mat, hidden_mat, project_mat = move(
        place,
        1,
        (split(queries), split(keys), split(values)),
        (output_mat, hidden_mat, project_mat),
    )
    output_mat, hidden_mat, project_mat = (
        g.reshape(width, width) for g in (output_mat, hidden_mat, project_mat)
    )
    mixed, full, sums = attend(q_in, k_in, v_in, tokens)
    (mixed,) = move(place, 2, (mixed,))
    mixed = mixed.reshape(width, rows)
    residual = xfloat + (contract("fr,fd->rd", mixed, output_mat) + output_add)
    inv_two = rms_scale(residual)
    second = (residual * inv_two * gain_two).astype(jnp.bfloat16)
    hidden_pre = contract("rd,df->rf", second, hidden_mat) + hidden_add
    active = jax.nn.silu(hidden_pre).astype(jnp.bfloat16)
    result = residual + (contract("rf,fd->rd", active, project_mat) + project_add)
    result = from_rows(result.astype(jnp.bfloat16))

    upper = to_rows(cotangent)
    project_grad = contract("rf,rd->fd", active, upper)
    project_bias_grad = jnp.sum(upper.astype(jnp.float32), axis=0)
    active_grad = contract("rd,fd->rf", upper, project_mat)
    logistic = jax.nn.sigmoid(hidden_pre)
    hidden_grad = (active_grad * logistic * (1.0 + hidden_pre * (1.0 - logistic))).astype(
        jnp.bfloat16
    )
    hidden_mat_grad = contract("rd,rf->df", second, hidden_grad)
    hidden_bias_grad = jnp.sum(hidden_grad.astype(jnp.float32), axis=0)
    second_grad = contract("rf,df->rd", hidden_grad, hidden_mat)
    normal_two = residual * inv_two
    scaled_two = second_grad * gain_two
    norm_two_grad = jnp.sum(second_grad * normal_two, axis=0)
    residual_grad = upper.astype(jnp.float32) + inv_two * (
        scaled_two - normal_two * jnp.mean(scaled_two * normal_two, axis=-1, keepdims=True)
    )
    branch_grad = residual_grad.astype(jnp.bfloat16)
    output_mat_grad = contract("fr,rd->fd", mixed, branch_grad)
    output_bias_grad = jnp.sum(branch_grad.astype(jnp.float32), axis=0)
    mixed_grad = contract("fd,rd->fr", output_mat, branch_grad).astype(jnp.bfloat16)

    def as_parts(*grads):
        return tuple(
            g.astype(jnp.bfloat16).reshape(place.grid() + (share, width)) for g in grads
        )

    merged = share % 8 == 0
    (do_in,) = move(place, 3, (split(mixed_grad),))
    slopes_out = slopes(q_in, k_in, v_in, do_in, full, sums, rate[:, None], tokens)
    early = as_parts(output_mat_grad, hidden_mat_grad, project_grad) if merged else ()
    query_slope, key_grad, value_grad, *early = move(
        place, 4, slopes_out, (), early, held=2 if merged else 0
    )
    query_slope, key_grad, value_grad = (
        a.reshape(width, rows) for a in (query_slope, key_grad, value_grad)
    )
    query_float = query_slope.astype(jnp.float32)
    scale_part = jnp.sum(query_float / rate_full * query_pre, axis=1)
    scale_part = jnp.sum(scale_part.reshape(HEADS, HEAD_DIM), axis=0)
    query_mat_grad = contract("rd,fr->df", normed, query_slope)
    query_bias_grad = jnp.sum(query_float, axis=1)
    key_mat_grad = contract("rd,fr->df", normed, key_grad)
    value_mat_grad = contract("rd,fr->df", normed, value_grad)
    value_bias_grad = jnp.sum(value_grad.astype(jnp.float32), axis=1)
    normed_grad = (
        contract("fr,df->rd", query_slope, query_mat)
        + contract("fr,df->rd", key_grad, key_mat)
        + contract("fr,df->rd", value_grad, value_mat)
    )
    normal_one = xfloat * inv_one
    scaled_one = normed_grad * gain_one
    norm_one_grad = jnp.sum(normed_grad * normal_one, axis=0)
    source_grad = residual_grad + inv_one * (
        scaled_one - normal_one * jnp.mean(scaled_one * normal_one, axis=-1, keepdims=True)
    )
    source_grad = from_rows(source_grad.astype(jnp.bfloat16))

    vector_grads = jnp.stack(
        (
            norm_one_grad,
            query_bias_grad,
            value_bias_grad,
            output_bias_grad,
            norm_two_grad,
            hidden_bias_grad,
            project_bias_grad,
        )
    )
    vector_grads = vector_grads.reshape(7, -1, share).transpose(1, 0, 2)
    vector_grads = jnp.pad(vector_grads, ((0, 0), (0, 0), (0, 128 - share)))
    scale_row = jnp.pad(scale_part, (0, 128 - HEAD_DIM))
    scale_row = jnp.broadcast_to(scale_row, (vector_grads.shape[0], 1, 128))
    vector_grads = jnp.concatenate([vector_grads, scale_row], axis=1)
    vector_grads = vector_grads.reshape(place.grid() + (8, 128))
    late = as_parts(query_mat_grad, key_mat_grad, value_mat_grad)
    if merged:
        output_mat_grad, *early = early
        hidden_mat_grad, project_grad, *late, vector_sums = move(
            place, 5, scatters=(*early, *late, vector_grads)
        )
    else:
        (vector_sums,) = move(place, 5, scatters=(vector_grads,))
        early = as_parts(output_mat_grad, hidden_mat_grad, project_grad)
        early = [move(place, 6, scatters=(p,))[0] for p in early]
        output_mat_grad, hidden_mat_grad, project_grad = early
        late = [move(place, 6, scatters=(p,))[0] for p in late]
    query_mat_grad, key_mat_grad, value_mat_grad = late
    g_one, g_query, g_value, g_output, g_two, g_hidden, g_project = (
        vector_sums[n, :share] for n in range(7)
    )
    scale_summed = vector_sums[7, :HEAD_DIM]
    depth_grad = scale_summed * (SOFT_BASE / math.sqrt(HEAD_DIM)) * jax.nn.sigmoid(depth)
    return (
        result,
        source_grad,
        g_one,
        query_mat_grad,
        g_query,
        key_mat_grad,
        value_mat_grad,
        g_value,
        output_mat_grad,
        g_output,
        g_two,
        hidden_mat_grad,
        g_hidden,
        project_grad,
        g_project,
        depth_grad,
    )


def solution(mesh):
    both = ("dp", "seq")
    token, vector, matrix = P(None, "seq", "dp", None), P(both), P(both, None)
    weights = (
        vector,
        matrix,
        vector,
        matrix,
        matrix,
        vector,
        matrix,
        vector,
        vector,
        matrix,
        vector,
        matrix,
        vector,
    )
    specs = (token, token) + weights + (P(),)
    place = Place(mesh.shape["dp"], mesh.shape["seq"])
    return jax.shard_map(
        functools.partial(on_device, place, mesh.shape["seq"]),
        mesh=mesh,
        in_specs=specs,
        out_specs=specs,
        check_vma=False,
    )
```

```python
import functools
import itertools
import math

import jax
import jax.numpy as jnp
from jax import lax
from jax.experimental import pallas as pl
from jax.experimental.pallas import tpu as pltpu
from jax.sharding import PartitionSpec as P

HEADS = 16
HEAD_DIM = 80
ATT_BLOCK = 256
SOFT_BASE = 1.442695041
EPSILON = 1e-06
MESH = pl.DeviceIdType.MESH
VMEM_BYTES = 60 * 1024 * 1024


class Place:
    def __init__(self, dp, seq):
        self.cores = 2 if dp % 2 == 0 else 1
        self.lines = dp // self.cores
        self.levels = 4 if seq % 4 == 0 else seq
        self.across = seq // self.levels
        self.sizes = {
            "y": self.lines,
            "c": self.cores,
            "z": self.levels,
            "x": self.across,
        }

    def here(self):
        dp = lax.axis_index("dp")
        seq = lax.axis_index("seq")
        return {
            "y": dp // self.cores,
            "c": dp % self.cores,
            "z": seq // self.across,
            "x": seq % self.across,
        }

    def shift(self, spot, axis, step):
        moved = dict(spot)
        moved[axis] = lax.rem(spot[axis] + step, self.sizes[axis])
        return moved

    def device(self, spot):
        return (
            spot["y"] * self.cores + spot["c"],
            spot["z"] * self.across + spot["x"],
        )

    def grid(self):
        return (self.lines, self.cores, self.levels, self.across)

    def greet(self, spot, wide):
        barrier = pltpu.get_barrier_semaphore()
        dp, seq = self.device(spot)
        peers = [
            self.device(self.shift(spot, axis, step))
            for axis in ("yc" if wide else "zxyc")
            for step in range(1, self.sizes[axis])
        ]
        if wide:
            devices = self.levels * self.across
            peers += [(dp, lax.rem(seq + step, devices)) for step in range(1, devices)]
        for peer in peers:
            pl.semaphore_signal(barrier, inc=1, device_id=peer, device_id_type=MESH)
        pl.semaphore_wait(barrier, len(peers))


def halves_of(cols, lean):
    if lean and cols % 640 == 0:
        cut = cols * 4 // 5
    elif cols % 256 == 0:
        cut = cols // 2
    else:
        return ((slice(0, cols), "xy"),)
    return ((slice(0, cut), "xy"), (slice(cut, cols), "yx"))


def chunks_of(rows):
    if rows % 8 == 0 and rows >= 32:
        cut = rows // 32 * 16
        return (slice(0, cut), slice(cut, rows))
    return (slice(0, rows),)


class Sender:
    def __init__(self, place, spot, send_sem, recv_sem):
        self.place = place
        self.spot = spot
        self.send_sem = send_sem
        self.recv_sem = recv_sem
        self.count = itertools.count()
        self.open = {}
        self.every = []

    def put(self, key, device, source, target, leaves=None, comes=None):
        at = next(self.count)
        copy = pltpu.make_async_remote_copy(
            src_ref=source,
            dst_ref=target,
            send_sem=self.send_sem.at[at],
            recv_sem=self.recv_sem.at[at],
            device_id=device,
            device_id_type=MESH,
        )
        self.guard(leaves, copy.start)
        self.open.setdefault(key, []).append((comes, copy))
        self.every.append((leaves, copy))

    def guard(self, when, act):
        if when is None:
            act()
        else:
            pl.when(when)(act)

    def go(self, key, axis, source, target):
        self.open[key] = []
        for step in range(1, self.place.sizes[axis]):
            peer = self.place.shift(self.spot, axis, step)
            self.put(key, self.place.device(peer), source(peer), target(step))

    def chain(self, key, turn, own, slot):
        levels, z = self.place.levels, self.spot["z"]
        self.open[key] = []

        def inside(at):
            return jnp.logical_and(at >= 0, at < levels)

        for way in (1, -1):
            shard, to, back = z - turn * way, z + way, z - (turn + 1) * way
            part = slot(lax.rem(shard + levels, levels))
            peer = dict(self.spot, z=lax.rem(to + levels, levels))
            self.put(
                key,
                self.place.device(peer),
                own if turn == 0 else part,
                part,
                jnp.logical_and(inside(shard), inside(to)),
                inside(back),
            )

    def landed(self, key):
        for comes, copy in self.open[key]:
            self.guard(comes, copy.wait_recv)

    def finish(self):
        for leaves, copy in self.every:
            self.guard(leaves, copy.wait_send)


class Gather:
    def __init__(self, place, spot, lean, tails, shards, wholes, own_sem):
        self.place, self.spot, self.lean, self.tails = place, spot, lean, tails
        self.shards, self.wholes = shards, wholes
        y, c, z, x = (spot[k] for k in "yczx")
        self.own = []
        for n, shard in enumerate(shards):
            if n >= len(shards) - tails:
                target = wholes[n].at[z]
            elif len(shard.shape) == 3:
                target = wholes[n].at[y, c, :, x]
            else:
                target = wholes[n].at[y, c, z, x]
            copy = pltpu.make_async_copy(shard, target, own_sem[n])
            copy.start()
            self.own.append(copy)

    def run(self, out, feed):
        shards, wholes = self.shards, self.wholes
        y, c, _, x = (self.spot[k] for k in "yczx")
        turns = self.place.levels - 1
        full = len(shards) - self.tails
        raw = [n for n, s in enumerate(shards) if len(s.shape) == 2]
        jobs = [(n, r) for n in range(full) for r in chunks_of(shards[n].shape[-2])]
        filled = set()

        def halves(n):
            return enumerate(halves_of(shards[n].shape[-1], self.lean))

        def along(turn, n):
            def slot(level):
                return wholes[n].at[y, c, level, x] if n < full else wholes[n].at[level]

            if turn > 0:
                out.landed(("z", n, turn - 1))
            if turn < turns:
                out.chain(("z", n, turn), turn, shards[n], slot)

        def fill(n):
            if n not in filled:
                filled.add(n)
                self.own[n].wait()

        def two(job, n, rows):
            lined = len(shards[n].shape) == 3
            if not lined:
                fill(n)
            for half, (cols, order) in halves(n):
                part = wholes[n].at[y, c, :, x, rows, cols]
                source = shards[n].at[:, rows, cols] if lined else part
                out.go((job, half, 2), order[0], lambda peer: source, lambda step: part)

        def three(job, n, rows):
            fill(n)
            for half, (cols, order) in halves(n):
                out.landed((job, half, 2))
                if order == "xy":
                    part = wholes[n].at[y, c, :, :, rows, cols]
                else:
                    part = wholes[n].at[:, c, :, x, rows, cols]
                out.go((job, half, 3), order[1], lambda peer: part, lambda step: part)

        def four(job, n, rows):
            for half, (cols, order) in halves(n):
                out.landed((job, half, 3))
                part = wholes[n].at[:, c, :, :, rows, cols]
                out.go((job, half, 4), "c", lambda peer: part, lambda step: part)

        def five(job, n, rows):
            for half, _ in halves(n):
                out.landed((job, half, 4))

        steps = iter(range(len(jobs) + 3))

        def advance():
            step = next(steps, None)
            if step is not None:
                for stage, late in ((two, 0), (three, 1), (four, 2), (five, 3)):
                    if 0 <= step - late < len(jobs):
                        stage(("gather", step - late), *jobs[step - late])

        if raw:
            for time in range(len(raw) + turns):
                for turn in range(turns + 1):
                    if 0 <= time - turn < len(raw):
                        along(turn, raw[time - turn])
                done = time - turns
                if 0 <= done < full:
                    for _ in chunks_of(shards[raw[done]].shape[-2]):
                        advance()
        for _ in range(len(jobs) + 3):
            advance()
            feed()
        for n in range(len(shards)):
            fill(n)


def total(values):
    result = values[0].astype(jnp.float32)
    for value in values[1:]:
        result = result + value.astype(jnp.float32)
    return result


class Scatter:
    def __init__(self, place, spot, lean, held, parts, totals, boxes, own_sem):
        self.place, self.spot, self.lean = place, spot, lean
        self.parts, self.totals = parts, totals
        self.full = len(parts) - held
        self.jobs = [
            (n, r)
            for n, p in enumerate(parts)
            if len(p.shape) > 3
            for r in chunks_of(p.shape[-2])
        ]
        self.own_sem = own_sem
        self.sums, self.cores, self.seconds, self.thirds, self.fourths = [], [], [], [], []
        self.results, self.own = [], []
        for n, part in enumerate(parts):
            self.sums.append(boxes.pop(0))
            if len(part.shape) > 3:
                self.cores.append(boxes.pop(0))
                halves = halves_of(part.shape[-1], lean)
                self.seconds.append([boxes.pop(0) for _ in halves])
                self.thirds.append([boxes.pop(0) for _ in halves])
                mine = part.at[:, spot["c"]]
            else:
                for boxed in (self.cores, self.seconds, self.thirds):
                    boxed.append(None)
                mine = part.at[spot["z"]]
            if n < self.full:
                self.fourths.append(boxes.pop(0))
                self.results.append(boxes.pop(0))
            else:
                self.fourths.append(None)
                self.results.append(self.sums[n].at[spot["y"], :, spot["x"]])
            copy = pltpu.make_async_copy(mine, self.sums[n], own_sem[n])
            copy.start()
            self.own.append(copy)

    def run(self, out, feed):
        place, parts, sums = self.place, self.parts, self.sums
        cores, results = self.cores, self.results
        y, c, z, x = (self.spot[k] for k in "yczx")
        lines, _, levels, across = place.grid()
        filled = set()

        def halves(n):
            return enumerate(halves_of(parts[n].shape[-1], self.lean))

        def one(job, n, rows):
            out.go(
                (job, 1),
                "c",
                lambda peer: parts[n].at[:, peer["c"], :, :, rows],
                lambda step: cores[n].at[:, :, :, rows],
            )

        def two(job, n, rows):
            if n not in filled:
                filled.add(n)
                self.own[n].wait()
            out.landed((job, 1))
            if place.cores > 1:

                @pl.loop(0, lines * levels * across)
                def _(at):
                    where = (at // (levels * across), (at // across) % levels, at % across)
                    sums[n][where + (rows,)] = total(
                        [sums[n][where + (rows,)], cores[n][where + (rows,)]]
                    ).astype(sums[n].dtype)

            for half, (cols, order) in halves(n):
                box = self.seconds[n][half]
                if order == "xy":
                    out.go(
                        (job, half, 2),
                        "y",
                        lambda peer: sums[n].at[peer["y"], :, :, rows, cols],
                        lambda step: box.at[step - 1, :, :, rows],
                    )
                else:
                    out.go(
                        (job, half, 2),
                        "x",
                        lambda peer: sums[n].at[:, :, peer["x"], rows, cols],
                        lambda step: box.at[step - 1, :, :, rows],
                    )

        def three(job, n, rows):
            for half, (cols, order) in halves(n):
                out.landed((job, half, 2))
                box, later = self.seconds[n][half], self.thirds[n][half]
                if order == "xy":

                    @pl.loop(0, levels * across)
                    def _(at):
                        zz, xx = at // across, at % across
                        values = [sums[n][y, zz, xx, rows, cols]]
                        values += [box[k, zz, xx, rows] for k in range(lines - 1)]
                        sums[n][y, zz, xx, rows, cols] = total(values).astype(sums[n].dtype)

                    out.go(
                        (job, half, 3),
                        "x",
                        lambda peer: sums[n].at[y, :, peer["x"], rows, cols],
                        lambda step: later.at[step - 1, :, rows],
                    )
                else:

                    @pl.loop(0, lines * levels)
                    def _(at):
                        yy, zz = at // levels, at % levels
                        values = [sums[n][yy, zz, x, rows, cols]]
                        values += [box[k, yy, zz, rows] for k in range(across - 1)]
                        sums[n][yy, zz, x, rows, cols] = total(values).astype(sums[n].dtype)

                    out.go(
                        (job, half, 3),
                        "y",
                        lambda peer: sums[n].at[peer["y"], :, x, rows, cols],
                        lambda step: later.at[step - 1, :, rows],
                    )

        def four(job, n, rows):
            for half, (cols, order) in halves(n):
                out.landed((job, half, 3))
                box = self.thirds[n][half]

                @pl.loop(0, levels)
                def _(zz):
                    values = [sums[n][y, zz, x, rows, cols]]
                    values += [box[k, zz, rows] for k in range(box.shape[0])]
                    sums[n][y, zz, x, rows, cols] = total(values).astype(sums[n].dtype)

            if n < self.full:
                out.go(
                    (job, 4),
                    "z",
                    lambda peer: sums[n].at[y, peer["z"], x, rows],
                    lambda step: self.fourths[n].at[step - 1, rows],
                )

        def five(job, n, rows):
            if n >= self.full:
                return
            out.landed((job, 4))
            values = [sums[n][y, z, x, rows]]
            values += [self.fourths[n][k, rows] for k in range(levels - 1)]
            results[n][rows] = total(values)

        def first(n):
            out.go(
                ("tail", n),
                "z",
                lambda peer: parts[n].at[peer["z"]],
                lambda step: self.fourths[n].at[step - 1],
            )

        def final(n):
            self.own[n].wait()
            out.landed(("tail", n))
            values = [sums[n][...]] + [self.fourths[n][k] for k in range(levels - 1)]
            results[n][...] = total(values)

        jobs = [(("scatter", at),) + job for at, job in enumerate(self.jobs)]
        tails = [n for n, p in enumerate(parts) if len(p.shape) == 3]
        for n in tails:
            first(n)
        for step in range(len(jobs) + 4):
            if step > 2 and tails:
                final(tails.pop(0))
            for stage, late in ((one, 0), (two, 1), (three, 2), (four, 3), (five, 4)):
                if 0 <= step - late < len(jobs):
                    stage(*jobs[step - late])
            feed()
        last = []
        for n, result in enumerate(results):
            copy = pltpu.make_async_copy(result, self.totals[n], self.own_sem[n])
            copy.start()
            last.append(copy)
        for copy in last:
            copy.wait()


def scatter_boxes(place, part, lean, held):
    lines, _, levels, across = place.grid()
    rows, cols = part.shape[-2:]
    final = [
        pltpu.VMEM((levels - 1, rows, cols), part.dtype),
        pltpu.VMEM((rows, cols), jnp.float32),
    ]
    if part.ndim == 3:
        return [pltpu.VMEM((rows, cols), part.dtype)] + final
    block = pltpu.VMEM((lines, levels, across, rows, cols), part.dtype)
    first, later = [], []
    for piece, order in halves_of(cols, lean):
        size = (rows, piece.stop - piece.start)
        steps = (lines - 1, across - 1) if order == "xy" else (across - 1, lines - 1)
        middle = (levels, across) if order == "xy" else (lines, levels)
        first.append(pltpu.VMEM((steps[0],) + middle + size, part.dtype))
        later.append(pltpu.VMEM((steps[1], levels) + size, part.dtype))
    return [block, block] + first + later + ([] if held else final)


def move_kernel(place, counts, lean, tails, held, *refs):
    refs = list(refs)
    swaps, gathers, scatters = counts
    whole = swaps + gathers + scatters
    ins, outs, rest = refs[:whole], refs[whole : 2 * whole], refs[2 * whole :]
    own_sem, send_sem, recv_sem = rest[-3:]
    staged = swaps > 0 and whole > swaps
    relays, boxes = rest[: swaps * staged], rest[swaps * staged : -3]
    spot = place.here()
    dp, me = place.device(spot)
    devices = place.levels * place.across
    sent, got = ins[:swaps], outs[:swaps]
    own = []
    for n in range(swaps):
        copy = pltpu.make_async_copy(sent[n].at[me], got[n].at[me], own_sem.at[n])
        copy.start()
        own.append(copy)
    cut = swaps + gathers
    gather = Gather(
        place, spot, lean, tails, ins[swaps:cut], outs[swaps:cut], [own_sem.at[n] for n in range(swaps, cut)]
    )
    scatter = Scatter(
        place, spot, lean, held, ins[cut:], outs[cut:], boxes, [own_sem.at[n] for n in range(cut, whole)]
    )
    place.greet(spot, swaps > 0 and not staged)
    out = Sender(place, spot, send_sem, recv_sem)
    levels, across = place.levels, place.across
    z, x = spot["z"], spot["x"]

    def straight(n):
        for step in range(1, devices):
            peer = lax.rem(me + step, devices)
            out.put("swap", (dp, peer), sent[n].at[peer], got[n].at[me])

    def along_x(n):
        for skip in range(1, across):
            peer = place.shift(spot, "x", skip)
            device = place.device(peer)
            out.put("swap", device, sent[n].at[device[1]], got[n].at[me])
            for step in range(1, levels):
                piece = place.device(place.shift(peer, "z", step))[1]
                out.put(
                    ("relay", n), device, sent[n].at[piece], relays[n].at[skip - 1, step - 1]
                )

    def along_z(n):
        for step in range(1, levels):
            device = place.device(place.shift(spot, "z", step))
            out.put("swap", device, sent[n].at[device[1]], got[n].at[me])

    def pass_on(n):
        out.landed(("relay", n))
        for skip in range(1, across):
            source = place.device(place.shift(spot, "x", across - skip))[1]
            for step in range(1, levels):
                device = place.device(place.shift(spot, "z", step))
                out.put("swap", device, relays[n].at[skip - 1, step - 1], got[n].at[source])

    if staged:
        pending = []
        for time in range(swaps + 2):
            acts = [(pass_on, time - 2), (along_x, time), (along_z, time + 1)]
            if time == 0:
                acts.insert(0, (along_z, 0))
            pending.append([(act, n) for act, n in acts if 0 <= n < swaps])
    else:
        pending = [[(straight, n)] for n in range(swaps)]

    def feed():
        for act, n in pending.pop(0) if pending else ():
            act(n)

    if gathers:
        gather.run(out, feed)
    if scatters:
        scatter.run(out, feed)
    while pending:
        feed()
    for copy in own:
        copy.wait()
    if swaps:
        out.landed("swap")
    out.finish()


def move(place, collective_id, swaps=(), gathers=(), scatters=(), tails=0, held=0):
    lean = len(swaps) > 0
    lines, cores, levels, across = place.grid()
    copies = len(swaps) * (2 * levels * across - across - 1)
    boxes = []
    if len(swaps) > 0 and len(gathers) + len(scatters) > 0:
        boxes += [pltpu.VMEM((across - 1, levels - 1) + a.shape[1:], a.dtype) for a in swaps]
    shapes = [jax.ShapeDtypeStruct(a.shape, a.dtype) for a in swaps]
    for n, shard in enumerate(gathers):
        rows, cols = shard.shape[-2:]
        if shard.ndim == 2:
            copies += 2 * (levels - 1)
        grid = place.grid()
        if n < len(gathers) - tails:
            count = len(halves_of(cols, lean)) * (across + lines + cores - 3)
            copies += len(chunks_of(rows)) * count
        else:
            grid = (levels,)
        shapes.append(jax.ShapeDtypeStruct(grid + (rows, cols), shard.dtype))
    for n, part in enumerate(scatters):
        rows, cols = part.shape[-2:]
        keeps = n >= len(scatters) - held
        count = 0 if keeps else levels - 1
        if part.ndim > 3:
            count += (cores - 1) + len(halves_of(cols, lean)) * (lines + across - 2)
            count *= len(chunks_of(rows))
        copies += count
        boxes += scatter_boxes(place, part, lean, keeps)
        shapes.append(
            jax.ShapeDtypeStruct((levels, rows, cols), part.dtype)
            if keeps
            else jax.ShapeDtypeStruct((rows, cols), jnp.float32)
        )

    def is_result(a):
        return a.dtype == jnp.float32 and a.shape[-1] > 128

    return pl.pallas_call(
        functools.partial(
            move_kernel, place, (len(swaps), len(gathers), len(scatters)), lean, tails, held
        ),
        out_shape=shapes,
        in_specs=[pl.BlockSpec(memory_space=pl.ANY)] * len(shapes),
        out_specs=[
            pl.BlockSpec(memory_space=pltpu.HBM if is_result(a) else pl.ANY)
            for a in shapes
        ],
        scratch_shapes=boxes
        + [
            pltpu.SemaphoreType.DMA((len(shapes),)),
            pltpu.SemaphoreType.DMA((copies,)),
            pltpu.SemaphoreType.DMA((copies,)),
        ],
        compiler_params=pltpu.CompilerParams(
            collective_id=collective_id,
            has_side_effects=True,
            vmem_limit_bytes=VMEM_BYTES,
        ),
        name=f"move_{collective_id}",
    )(*swaps, *gathers, *scatters)


def side_by_side(ref):
    return jnp.concatenate([ref[s] for s in range(ref.shape[0])], axis=1)


def dot_first(left, right):
    return lax.dot_general(
        left, right, (((0,), (0,)), ((), ())), preferred_element_type=jnp.float32
    )


def dot_last(left, right):
    return lax.dot_general(
        left, right, (((1,), (1,)), ((), ())), preferred_element_type=jnp.float32
    )


def attend_kernel(q_ref, k_ref, v_ref, o_ref, full_ref, sum_ref):
    tokens = q_ref.shape[-1]
    each = ATT_BLOCK // tokens
    keys, values = side_by_side(k_ref), side_by_side(v_ref)
    for block in range(q_ref.shape[0] // each):
        first = block * each
        limit = (block + 1) * ATT_BLOCK
        queries = jnp.concatenate([q_ref[first + s] for s in range(each)], axis=1)
        weights = jnp.exp(dot_first(keys[:, :limit], queries))
        sums = jnp.sum(weights, axis=0, keepdims=True)
        mixed = jnp.dot(
            values[:, :limit],
            weights.astype(jnp.bfloat16),
            preferred_element_type=jnp.float32,
        )
        mixed = mixed / sums
        sum_ref[0, 0, :, pl.ds(block * ATT_BLOCK, ATT_BLOCK)] = sums
        for s in range(each):
            piece = mixed[:, s * tokens : (s + 1) * tokens]
            full_ref[first + s] = piece
            o_ref[first + s] = piece.astype(jnp.bfloat16)


def attend_specs(devices, tokens):
    piece = pl.BlockSpec((devices, HEAD_DIM, tokens), lambda m, h: (0, h, m))
    sums = pl.BlockSpec((1, 1, 1, devices * tokens), lambda m, h: (m, h, 0, 0))
    return piece, sums


def attend(queries, keys, values, tokens):
    devices, rows, cols = queries.shape
    grid = (cols // tokens, rows // HEAD_DIM)
    piece, sums = attend_specs(devices, tokens)
    return pl.pallas_call(
        attend_kernel,
        grid=grid,
        out_shape=[
            jax.ShapeDtypeStruct(queries.shape, jnp.bfloat16),
            jax.ShapeDtypeStruct(queries.shape, jnp.float32),
            jax.ShapeDtypeStruct(grid + (1, devices * tokens), jnp.float32),
        ],
        in_specs=[piece] * 3,
        out_specs=[piece, piece, sums],
        compiler_params=pltpu.CompilerParams(vmem_limit_bytes=VMEM_BYTES),
        name="attend",
    )(queries, keys, values)


def slopes_kernel(
    q_ref, k_ref, v_ref, do_ref, full_ref, sum_ref, rate_ref, dq_ref, dk_ref, dv_ref
):
    tokens = q_ref.shape[-1]
    each = ATT_BLOCK // tokens
    keys, values = side_by_side(k_ref), side_by_side(v_ref)
    rate = rate_ref[...]
    key_total = value_total = None
    for block in reversed(range(q_ref.shape[0] // each)):
        first = block * each
        limit = (block + 1) * ATT_BLOCK

        def pick(ref):
            return jnp.concatenate([ref[first + s] for s in range(each)], axis=1)

        queries = pick(q_ref)
        slope = pick(do_ref).astype(jnp.float32)
        sums = sum_ref[0, 0, :, pl.ds(block * ATT_BLOCK, ATT_BLOCK)]
        scaled = (slope / sums).astype(jnp.bfloat16)
        centre = jnp.sum(slope * pick(full_ref), axis=0, keepdims=True) / sums
        weights = jnp.exp(dot_first(keys[:, :limit], queries))
        dots = dot_first(values[:, :limit], scaled)
        slopes = (weights * (dots - centre)).astype(jnp.bfloat16)
        weights = weights.astype(jnp.bfloat16)
        query_part = jnp.dot(keys[:, :limit], slopes, preferred_element_type=jnp.float32)
        query_part = (query_part * rate).astype(jnp.bfloat16)
        for s in range(each):
            dq_ref[first + s] = query_part[:, s * tokens : (s + 1) * tokens]
        key_part = dot_last(queries, slopes)
        value_part = dot_last(scaled, weights)
        if key_total is None:
            key_total, value_total = key_part, value_part
        else:
            key_total = jnp.concatenate(
                [key_total[:, :limit] + key_part, key_total[:, limit:]], axis=1
            )
            value_total = jnp.concatenate(
                [value_total[:, :limit] + value_part, value_total[:, limit:]], axis=1
            )
    for s in range(q_ref.shape[0]):
        cols = slice(s * tokens, (s + 1) * tokens)
        dk_ref[s] = key_total[:, cols].astype(jnp.bfloat16)
        dv_ref[s] = value_total[:, cols].astype(jnp.bfloat16)


def slopes(queries, keys, values, slope, full, sums, rate, tokens):
    devices, rows, cols = queries.shape
    grid = (cols // tokens, rows // HEAD_DIM)
    piece, sum_spec = attend_specs(devices, tokens)
    return pl.pallas_call(
        slopes_kernel,
        grid=grid,
        out_shape=[jax.ShapeDtypeStruct(queries.shape, jnp.bfloat16)] * 3,
        in_specs=[piece] * 5
        + [sum_spec, pl.BlockSpec((HEAD_DIM, 1), lambda m, h: (0, 0))],
        out_specs=[piece] * 3,
        compiler_params=pltpu.CompilerParams(vmem_limit_bytes=VMEM_BYTES),
        name="slopes",
    )(queries, keys, values, slope, full, sums, rate)


def rms_scale(values):
    return lax.rsqrt(jnp.mean(values * values, axis=-1, keepdims=True) + EPSILON)


def contract(spec, left, right):
    return jnp.einsum(spec, left, right, preferred_element_type=jnp.float32)


def on_device(place, devices, *args):
    inputs, cotangent = args[:2]
    (
        norm_one,
        query_mat,
        query_add,
        key_mat,
        value_mat,
        value_add,
        output_mat,
        output_add,
        norm_two,
        hidden_mat,
        hidden_add,
        project_mat,
        project_add,
    ) = args[2:15]
    depth = args[15].astype(jnp.float32)
    micro, tokens, seqs, width = inputs.shape
    rows = micro * tokens * seqs
    vectors = (norm_one, query_add, value_add, output_add, norm_two, hidden_add, project_add)
    share = norm_one.shape[0]
    small = jnp.pad(jnp.stack(vectors), ((0, 16 - len(vectors)), (0, 128 - share)))
    query_mat, small, key_mat, value_mat, output_mat, hidden_mat, project_mat = move(
        place,
        0,
        gathers=(query_mat, small, key_mat, value_mat, output_mat, hidden_mat, project_mat),
        tails=3,
    )
    small = small.reshape(-1, 16, 128)[:, : len(vectors), :share]
    small = small.transpose(1, 0, 2).reshape(len(vectors), width).astype(jnp.float32)
    gain_one, query_add, value_add, output_add, gain_two, hidden_add, project_add = small
    query_mat, key_mat, value_mat = (
        g.reshape(width, width) for g in (query_mat, key_mat, value_mat)
    )

    def to_rows(array):
        return array.transpose(0, 2, 1, 3).reshape(rows, width)

    def from_rows(array):
        return array.reshape(micro, seqs, tokens, width).transpose(0, 2, 1, 3)

    rate = SOFT_BASE / math.sqrt(HEAD_DIM) * jax.nn.softplus(depth)
    rate_full = jnp.tile(rate, HEADS)[:, None]
    xfloat = to_rows(inputs).astype(jnp.float32)
    inv_one = rms_scale(xfloat)
    normed = (xfloat * inv_one * gain_one).astype(jnp.bfloat16)
    query_pre = contract("df,rd->fr", query_mat, normed) + query_add[:, None]
    queries = (query_pre * rate_full).astype(jnp.bfloat16)
    keys = contract("df,rd->fr", key_mat, normed).astype(jnp.bfloat16)
    values = (contract("df,rd->fr", value_mat, normed) + value_add[:, None]).astype(jnp.bfloat16)

    def split(array):
        return array.reshape(devices, width // devices, rows)

    q_in, k_in, v_in, output_mat, hidden_mat, project_mat = move(
        place,
        1,
        (split(queries), split(keys), split(values)),
        (output_mat, hidden_mat, project_mat),
    )
    output_mat, hidden_mat, project_mat = (
        g.reshape(width, width) for g in (output_mat, hidden_mat, project_mat)
    )
    mixed, full, sums = attend(q_in, k_in, v_in, tokens)
    (mixed,) = move(place, 2, (mixed,))
    mixed = mixed.reshape(width, rows)
    residual = xfloat + (contract("fr,fd->rd", mixed, output_mat) + output_add)
    inv_two = rms_scale(residual)
    second = (residual * inv_two * gain_two).astype(jnp.bfloat16)
    hidden_pre = contract("rd,df->rf", second, hidden_mat) + hidden_add
    active = jax.nn.silu(hidden_pre).astype(jnp.bfloat16)
    result = residual + (contract("rf,fd->rd", active, project_mat) + project_add)
    result = from_rows(result.astype(jnp.bfloat16))

    upper = to_rows(cotangent)
    project_grad = contract("rf,rd->fd", active, upper)
    project_bias_grad = jnp.sum(upper.astype(jnp.float32), axis=0)
    active_grad = contract("rd,fd->rf", upper, project_mat)
    logistic = jax.nn.sigmoid(hidden_pre)
    hidden_grad = (active_grad * logistic * (1.0 + hidden_pre * (1.0 - logistic))).astype(
        jnp.bfloat16
    )
    hidden_mat_grad = contract("rd,rf->df", second, hidden_grad)
    hidden_bias_grad = jnp.sum(hidden_grad.astype(jnp.float32), axis=0)
    second_grad = contract("rf,df->rd", hidden_grad, hidden_mat)
    normal_two = residual * inv_two
    scaled_two = second_grad * gain_two
    norm_two_grad = jnp.sum(second_grad * normal_two, axis=0)
    residual_grad = upper.astype(jnp.float32) + inv_two * (
        scaled_two - normal_two * jnp.mean(scaled_two * normal_two, axis=-1, keepdims=True)
    )
    branch_grad = residual_grad.astype(jnp.bfloat16)
    output_mat_grad = contract("fr,rd->fd", mixed, branch_grad)
    output_bias_grad = jnp.sum(branch_grad.astype(jnp.float32), axis=0)
    mixed_grad = contract("fd,rd->fr", output_mat, branch_grad).astype(jnp.bfloat16)

    def as_parts(*grads):
        return tuple(
            g.astype(jnp.bfloat16).reshape(place.grid() + (share, width)) for g in grads
        )

    merged = share % 8 == 0
    (do_in,) = move(place, 3, (split(mixed_grad),))
    slopes_out = slopes(q_in, k_in, v_in, do_in, full, sums, rate[:, None], tokens)
    early = as_parts(output_mat_grad, hidden_mat_grad, project_grad) if merged else ()
    query_slope, key_grad, value_grad, *early = move(
        place, 4, slopes_out, (), early, held=2 if merged else 0
    )
    query_slope, key_grad, value_grad = (
        a.reshape(width, rows) for a in (query_slope, key_grad, value_grad)
    )
    query_float = query_slope.astype(jnp.float32)
    scale_part = jnp.sum(query_float / rate_full * query_pre, axis=1)
    scale_part = jnp.sum(scale_part.reshape(HEADS, HEAD_DIM), axis=0)
    query_mat_grad = contract("rd,fr->df", normed, query_slope)
    query_bias_grad = jnp.sum(query_float, axis=1)
    key_mat_grad = contract("rd,fr->df", normed, key_grad)
    value_mat_grad = contract("rd,fr->df", normed, value_grad)
    value_bias_grad = jnp.sum(value_grad.astype(jnp.float32), axis=1)
    normed_grad = (
        contract("fr,df->rd", query_slope, query_mat)
        + contract("fr,df->rd", key_grad, key_mat)
        + contract("fr,df->rd", value_grad, value_mat)
    )
    normal_one = xfloat * inv_one
    scaled_one = normed_grad * gain_one
    norm_one_grad = jnp.sum(normed_grad * normal_one, axis=0)
    source_grad = residual_grad + inv_one * (
        scaled_one - normal_one * jnp.mean(scaled_one * normal_one, axis=-1, keepdims=True)
    )
    source_grad = from_rows(source_grad.astype(jnp.bfloat16))

    vector_grads = jnp.stack(
        (
            norm_one_grad,
            query_bias_grad,
            value_bias_grad,
            output_bias_grad,
            norm_two_grad,
            hidden_bias_grad,
            project_bias_grad,
        )
    )
    vector_grads = vector_grads.reshape(7, -1, share).transpose(1, 0, 2)
    vector_grads = jnp.pad(vector_grads, ((0, 0), (0, 0), (0, 128 - share)))
    scale_row = jnp.pad(scale_part, (0, 128 - HEAD_DIM))
    scale_row = jnp.broadcast_to(scale_row, (vector_grads.shape[0], 1, 128))
    vector_grads = jnp.concatenate([vector_grads, scale_row], axis=1)
    vector_grads = vector_grads.reshape(place.grid() + (8, 128))
    late = as_parts(query_mat_grad, key_mat_grad, value_mat_grad)
    if merged:
        output_mat_grad, *early = early
        hidden_mat_grad, project_grad, *late, vector_sums = move(
            place, 5, scatters=(*early, *late, vector_grads)
        )
    else:
        (vector_sums,) = move(place, 5, scatters=(vector_grads,))
        early = as_parts(output_mat_grad, hidden_mat_grad, project_grad)
        early = [move(place, 6, scatters=(p,))[0] for p in early]
        output_mat_grad, hidden_mat_grad, project_grad = early
        late = [move(place, 6, scatters=(p,))[0] for p in late]
    query_mat_grad, key_mat_grad, value_mat_grad = late
    g_one, g_query, g_value, g_output, g_two, g_hidden, g_project = (
        vector_sums[n, :share] for n in range(7)
    )
    scale_summed = vector_sums[7, :HEAD_DIM]
    depth_grad = scale_summed * (SOFT_BASE / math.sqrt(HEAD_DIM)) * jax.nn.sigmoid(depth)
    return (
        result,
        source_grad,
        g_one,
        query_mat_grad,
        g_query,
        key_mat_grad,
        value_mat_grad,
        g_value,
        output_mat_grad,
        g_output,
        g_two,
        hidden_mat_grad,
        g_hidden,
        project_grad,
        g_project,
        depth_grad,
    )


def solution(mesh):
    both = ("dp", "seq")
    token, vector, matrix = P(None, "seq", "dp", None), P(both), P(both, None)
    weights = (
        vector,
        matrix,
        vector,
        matrix,
        matrix,
        vector,
        matrix,
        vector,
        vector,
        matrix,
        vector,
        matrix,
        vector,
    )
    specs = (token, token) + weights + (P(),)
    place = Place(mesh.shape["dp"], mesh.shape["seq"])
    return jax.shard_map(
        functools.partial(on_device, place, mesh.shape["seq"]),
        mesh=mesh,
        in_specs=specs,
        out_specs=specs,
        check_vma=False,
    )
```

```python
import functools
import itertools
import math

import jax
import jax.numpy as jnp
from jax import lax
from jax.experimental import pallas as pl
from jax.experimental.pallas import tpu as pltpu
from jax.sharding import PartitionSpec as P

HEADS = 16
HEAD_DIM = 80
ATT_BLOCK = 256
SOFT_BASE = 1.442695041
EPSILON = 1e-06
MESH = pl.DeviceIdType.MESH
VMEM_BYTES = 60 * 1024 * 1024


class Place:
    def __init__(self, dp, seq):
        self.cores = 2 if dp % 2 == 0 else 1
        self.lines = dp // self.cores
        self.levels = 4 if seq % 4 == 0 else seq
        self.across = seq // self.levels
        self.sizes = {
            "y": self.lines,
            "c": self.cores,
            "z": self.levels,
            "x": self.across,
        }

    def here(self):
        dp = lax.axis_index("dp")
        seq = lax.axis_index("seq")
        return {
            "y": dp // self.cores,
            "c": dp % self.cores,
            "z": seq // self.across,
            "x": seq % self.across,
        }

    def shift(self, spot, axis, step):
        moved = dict(spot)
        moved[axis] = lax.rem(spot[axis] + step, self.sizes[axis])
        return moved

    def device(self, spot):
        return (
            spot["y"] * self.cores + spot["c"],
            spot["z"] * self.across + spot["x"],
        )

    def grid(self):
        return (self.lines, self.cores, self.levels, self.across)

    def greet(self, spot, wide):
        barrier = pltpu.get_barrier_semaphore()
        dp, seq = self.device(spot)
        peers = [
            self.device(self.shift(spot, axis, step))
            for axis in ("yc" if wide else "zxyc")
            for step in range(1, self.sizes[axis])
        ]
        if wide:
            devices = self.levels * self.across
            peers += [(dp, lax.rem(seq + step, devices)) for step in range(1, devices)]
        for peer in peers:
            pl.semaphore_signal(barrier, inc=1, device_id=peer, device_id_type=MESH)
        pl.semaphore_wait(barrier, len(peers))


def halves_of(cols, lean):
    if lean and cols % 640 == 0:
        cut = cols * 4 // 5
    elif cols % 256 == 0:
        cut = cols // 2
    else:
        return ((slice(0, cols), "xy"),)
    return ((slice(0, cut), "xy"), (slice(cut, cols), "yx"))


def chunks_of(rows, first=0):
    if rows % 8 or rows < 32:
        return (slice(0, rows),)
    starts = [0] + list(range(first or 16, rows, 16))
    return tuple(slice(p, q) for p, q in zip(starts, starts[1:] + [rows]))


class Sender:
    def __init__(self, place, spot, send_sem, recv_sem):
        self.place = place
        self.spot = spot
        self.send_sem = send_sem
        self.recv_sem = recv_sem
        self.count = itertools.count()
        self.open = {}
        self.every = []

    def put(self, key, device, source, target, leaves=None, comes=None):
        at = next(self.count)
        copy = pltpu.make_async_remote_copy(
            src_ref=source,
            dst_ref=target,
            send_sem=self.send_sem.at[at],
            recv_sem=self.recv_sem.at[at],
            device_id=device,
            device_id_type=MESH,
        )
        self.guard(leaves, copy.start)
        self.open.setdefault(key, []).append((comes, copy))
        self.every.append((leaves, copy))

    def guard(self, when, act):
        if when is None:
            act()
        else:
            pl.when(when)(act)

    def go(self, key, axis, source, target):
        self.open[key] = []
        for step in range(1, self.place.sizes[axis]):
            peer = self.place.shift(self.spot, axis, step)
            self.put(key, self.place.device(peer), source(peer), target(step))

    def chain(self, key, turn, own, slot):
        levels, z = self.place.levels, self.spot["z"]
        self.open[key] = []

        def inside(at):
            return jnp.logical_and(at >= 0, at < levels)

        for way in (1, -1):
            shard, to, back = z - turn * way, z + way, z - (turn + 1) * way
            part = slot(lax.rem(shard + levels, levels))
            peer = dict(self.spot, z=lax.rem(to + levels, levels))
            self.put(
                key,
                self.place.device(peer),
                own if turn == 0 else part,
                part,
                jnp.logical_and(inside(shard), inside(to)),
                inside(back),
            )

    def landed(self, key):
        for comes, copy in self.open[key]:
            self.guard(comes, copy.wait_recv)

    def finish(self):
        for leaves, copy in self.every:
            self.guard(leaves, copy.wait_send)


class Gather:
    def __init__(self, place, spot, lean, tails, shards, wholes, own_sem):
        self.place, self.spot, self.lean, self.tails = place, spot, lean, tails
        self.shards, self.wholes = shards, wholes
        y, c, z, x = (spot[k] for k in "yczx")
        self.own = []
        for n, shard in enumerate(shards):
            if n >= len(shards) - tails:
                target = wholes[n].at[z]
            elif len(shard.shape) == 3:
                target = wholes[n].at[y, c, :, x]
            else:
                target = wholes[n].at[y, c, z, x]
            copy = pltpu.make_async_copy(shard, target, own_sem[n])
            copy.start()
            self.own.append(copy)

    def run(self, out, feed):
        shards, wholes = self.shards, self.wholes
        y, c, _, x = (self.spot[k] for k in "yczx")
        turns = self.place.levels - 1
        full = len(shards) - self.tails
        raw = [n for n, s in enumerate(shards) if len(s.shape) == 2]
        jobs = [(n, r) for n in range(full) for r in chunks_of(shards[n].shape[-2], 8)]
        filled = set()

        def halves(n):
            return enumerate(halves_of(shards[n].shape[-1], self.lean))

        def along(turn, n):
            def slot(level):
                return wholes[n].at[y, c, level, x] if n < full else wholes[n].at[level]

            if turn > 0:
                out.landed(("z", n, turn - 1))
            if turn < turns:
                out.chain(("z", n, turn), turn, shards[n], slot)

        def fill(n):
            if n not in filled:
                filled.add(n)
                self.own[n].wait()

        def two(job, n, rows):
            lined = len(shards[n].shape) == 3
            if not lined:
                fill(n)
            for half, (cols, order) in halves(n):
                part = wholes[n].at[y, c, :, x, rows, cols]
                source = shards[n].at[:, rows, cols] if lined else part
                out.go((job, half, 2), order[0], lambda peer: source, lambda step: part)

        def three(job, n, rows):
            fill(n)
            for half, (cols, order) in halves(n):
                out.landed((job, half, 2))
                if order == "xy":
                    part = wholes[n].at[y, c, :, :, rows, cols]
                else:
                    part = wholes[n].at[:, c, :, x, rows, cols]
                out.go((job, half, 3), order[1], lambda peer: part, lambda step: part)

        def four(job, n, rows):
            for half, (cols, order) in halves(n):
                out.landed((job, half, 3))
                part = wholes[n].at[:, c, :, :, rows, cols]
                out.go((job, half, 4), "c", lambda peer: part, lambda step: part)

        def five(job, n, rows):
            for half, _ in halves(n):
                out.landed((job, half, 4))

        steps = iter(range(len(jobs) + 3))

        def advance():
            step = next(steps, None)
            if step is not None:
                for stage, late in ((two, 0), (three, 1), (four, 2), (five, 3)):
                    if 0 <= step - late < len(jobs):
                        stage(("gather", step - late), *jobs[step - late])

        if raw:
            for time in range(len(raw) + turns):
                for turn in range(turns + 1):
                    if 0 <= time - turn < len(raw):
                        along(turn, raw[time - turn])
                done = time - turns
                if 0 <= done < full:
                    for _ in chunks_of(shards[raw[done]].shape[-2], 8):
                        advance()
        for _ in range(len(jobs) + 3):
            advance()
            feed()
        for n in range(len(shards)):
            fill(n)


def total(values):
    result = values[0].astype(jnp.float32)
    for value in values[1:]:
        result = result + value.astype(jnp.float32)
    return result


class Scatter:
    def __init__(self, place, spot, lean, held, parts, totals, boxes, own_sem):
        self.place, self.spot, self.lean = place, spot, lean
        self.parts, self.totals = parts, totals
        self.full = len(parts) - held
        self.jobs = [
            (n, r)
            for n, p in enumerate(parts)
            if len(p.shape) > 3
            for r in chunks_of(p.shape[-2])
        ]
        self.own_sem = own_sem
        self.sums, self.cores, self.seconds, self.thirds, self.fourths = [], [], [], [], []
        self.results, self.own = [], []
        for n, part in enumerate(parts):
            self.sums.append(boxes.pop(0))
            if len(part.shape) > 3:
                self.cores.append(boxes.pop(0))
                halves = halves_of(part.shape[-1], lean)
                self.seconds.append([boxes.pop(0) for _ in halves])
                self.thirds.append([boxes.pop(0) for _ in halves])
                mine = part.at[:, spot["c"]]
            else:
                for boxed in (self.cores, self.seconds, self.thirds):
                    boxed.append(None)
                mine = part.at[spot["z"]]
            if n < self.full:
                self.fourths.append(boxes.pop(0))
                self.results.append(boxes.pop(0))
            else:
                self.fourths.append(None)
                self.results.append(self.sums[n].at[spot["y"], :, spot["x"]])
            copy = pltpu.make_async_copy(mine, self.sums[n], own_sem[n])
            copy.start()
            self.own.append(copy)

    def run(self, out, feed):
        place, parts, sums = self.place, self.parts, self.sums
        cores, results = self.cores, self.results
        y, c, z, x = (self.spot[k] for k in "yczx")
        lines, _, levels, across = place.grid()
        filled = set()

        def halves(n):
            return enumerate(halves_of(parts[n].shape[-1], self.lean))

        def one(job, n, rows):
            out.go(
                (job, 1),
                "c",
                lambda peer: parts[n].at[:, peer["c"], :, :, rows],
                lambda step: cores[n].at[:, :, :, rows],
            )

        def two(job, n, rows):
            if n not in filled:
                filled.add(n)
                self.own[n].wait()
            out.landed((job, 1))
            if place.cores > 1:

                @pl.loop(0, lines * levels * across)
                def _(at):
                    where = (at // (levels * across), (at // across) % levels, at % across)
                    sums[n][where + (rows,)] = total(
                        [sums[n][where + (rows,)], cores[n][where + (rows,)]]
                    ).astype(sums[n].dtype)

            for half, (cols, order) in halves(n):
                box = self.seconds[n][half]
                if order == "xy":
                    out.go(
                        (job, half, 2),
                        "y",
                        lambda peer: sums[n].at[peer["y"], :, :, rows, cols],
                        lambda step: box.at[step - 1, :, :, rows],
                    )
                else:
                    out.go(
                        (job, half, 2),
                        "x",
                        lambda peer: sums[n].at[:, :, peer["x"], rows, cols],
                        lambda step: box.at[step - 1, :, :, rows],
                    )

        def three(job, n, rows):
            for half, (cols, order) in halves(n):
                out.landed((job, half, 2))
                box, later = self.seconds[n][half], self.thirds[n][half]
                if order == "xy":

                    @pl.loop(0, levels * across)
                    def _(at):
                        zz, xx = at // across, at % across
                        values = [sums[n][y, zz, xx, rows, cols]]
                        values += [box[k, zz, xx, rows] for k in range(lines - 1)]
                        sums[n][y, zz, xx, rows, cols] = total(values).astype(sums[n].dtype)

                    out.go(
                        (job, half, 3),
                        "x",
                        lambda peer: sums[n].at[y, :, peer["x"], rows, cols],
                        lambda step: later.at[step - 1, :, rows],
                    )
                else:

                    @pl.loop(0, lines * levels)
                    def _(at):
                        yy, zz = at // levels, at % levels
                        values = [sums[n][yy, zz, x, rows, cols]]
                        values += [box[k, yy, zz, rows] for k in range(across - 1)]
                        sums[n][yy, zz, x, rows, cols] = total(values).astype(sums[n].dtype)

                    out.go(
                        (job, half, 3),
                        "y",
                        lambda peer: sums[n].at[peer["y"], :, x, rows, cols],
                        lambda step: later.at[step - 1, :, rows],
                    )

        def four(job, n, rows):
            for half, (cols, order) in halves(n):
                out.landed((job, half, 3))
                box = self.thirds[n][half]

                @pl.loop(0, levels)
                def _(zz):
                    values = [sums[n][y, zz, x, rows, cols]]
                    values += [box[k, zz, rows] for k in range(box.shape[0])]
                    sums[n][y, zz, x, rows, cols] = total(values).astype(sums[n].dtype)

            if n < self.full:
                out.go(
                    (job, 4),
                    "z",
                    lambda peer: sums[n].at[y, peer["z"], x, rows],
                    lambda step: self.fourths[n].at[step - 1, rows],
                )

        def five(job, n, rows):
            if n >= self.full:
                return
            out.landed((job, 4))
            values = [sums[n][y, z, x, rows]]
            values += [self.fourths[n][k, rows] for k in range(levels - 1)]
            results[n][rows] = total(values)

        def first(n):
            out.go(
                ("tail", n),
                "z",
                lambda peer: parts[n].at[peer["z"]],
                lambda step: self.fourths[n].at[step - 1],
            )

        def final(n):
            self.own[n].wait()
            out.landed(("tail", n))
            values = [sums[n][...]] + [self.fourths[n][k] for k in range(levels - 1)]
            results[n][...] = total(values)

        jobs = [(("scatter", at),) + job for at, job in enumerate(self.jobs)]
        tails = [n for n, p in enumerate(parts) if len(p.shape) == 3]
        for n in tails:
            first(n)
        for step in range(len(jobs) + 4):
            if step > 2 and tails:
                final(tails.pop(0))
            for stage, late in ((one, 0), (two, 1), (three, 2), (four, 3), (five, 4)):
                if 0 <= step - late < len(jobs):
                    stage(*jobs[step - late])
            feed()
        last = []
        for n, result in enumerate(results):
            copy = pltpu.make_async_copy(result, self.totals[n], self.own_sem[n])
            copy.start()
            last.append(copy)
        for copy in last:
            copy.wait()


def scatter_boxes(place, part, lean, held):
    lines, _, levels, across = place.grid()
    rows, cols = part.shape[-2:]
    final = [
        pltpu.VMEM((levels - 1, rows, cols), part.dtype),
        pltpu.VMEM((rows, cols), jnp.float32),
    ]
    if part.ndim == 3:
        return [pltpu.VMEM((rows, cols), part.dtype)] + final
    block = pltpu.VMEM((lines, levels, across, rows, cols), part.dtype)
    first, later = [], []
    for piece, order in halves_of(cols, lean):
        size = (rows, piece.stop - piece.start)
        steps = (lines - 1, across - 1) if order == "xy" else (across - 1, lines - 1)
        middle = (levels, across) if order == "xy" else (lines, levels)
        first.append(pltpu.VMEM((steps[0],) + middle + size, part.dtype))
        later.append(pltpu.VMEM((steps[1], levels) + size, part.dtype))
    return [block, block] + first + later + ([] if held else final)


def move_kernel(place, counts, lean, tails, held, *refs):
    refs = list(refs)
    swaps, gathers, scatters = counts
    whole = swaps + gathers + scatters
    ins, outs, rest = refs[:whole], refs[whole : 2 * whole], refs[2 * whole :]
    own_sem, send_sem, recv_sem = rest[-3:]
    staged = swaps > 0 and whole > swaps
    relays, boxes = rest[: swaps * staged], rest[swaps * staged : -3]
    spot = place.here()
    dp, me = place.device(spot)
    devices = place.levels * place.across
    sent, got = ins[:swaps], outs[:swaps]
    own = []
    for n in range(swaps):
        copy = pltpu.make_async_copy(sent[n].at[me], got[n].at[me], own_sem.at[n])
        copy.start()
        own.append(copy)
    cut = swaps + gathers
    gather = Gather(
        place, spot, lean, tails, ins[swaps:cut], outs[swaps:cut], [own_sem.at[n] for n in range(swaps, cut)]
    )
    scatter = Scatter(
        place, spot, lean, held, ins[cut:], outs[cut:], boxes, [own_sem.at[n] for n in range(cut, whole)]
    )
    place.greet(spot, swaps > 0 and not staged)
    out = Sender(place, spot, send_sem, recv_sem)
    levels, across = place.levels, place.across
    z, x = spot["z"], spot["x"]

    def straight(n):
        for step in range(1, devices):
            peer = lax.rem(me + step, devices)
            out.put("swap", (dp, peer), sent[n].at[peer], got[n].at[me])

    def along_x(n):
        for skip in range(1, across):
            peer = place.shift(spot, "x", skip)
            device = place.device(peer)
            out.put("swap", device, sent[n].at[device[1]], got[n].at[me])
            for step in range(1, levels):
                piece = place.device(place.shift(peer, "z", step))[1]
                out.put(
                    ("relay", n), device, sent[n].at[piece], relays[n].at[skip - 1, step - 1]
                )

    def along_z(n):
        for step in range(1, levels):
            device = place.device(place.shift(spot, "z", step))
            out.put("swap", device, sent[n].at[device[1]], got[n].at[me])

    def pass_on(n):
        out.landed(("relay", n))
        for skip in range(1, across):
            source = place.device(place.shift(spot, "x", across - skip))[1]
            for step in range(1, levels):
                device = place.device(place.shift(spot, "z", step))
                out.put("swap", device, relays[n].at[skip - 1, step - 1], got[n].at[source])

    if staged:
        apart = 3 if gathers else 1
        pending = [[] for _ in range(apart * (swaps - 1) + 3)]
        for n in range(swaps):
            pending[0 if gathers else max(n - 1, 0)].append((along_z, n))
        for n in range(swaps):
            pending[apart * n].append((along_x, n))
            pending[apart * n + 2].append((pass_on, n))
    else:
        pending = [[(straight, n)] for n in range(swaps)]

    def feed():
        for act, n in pending.pop(0) if pending else ():
            act(n)

    if gathers:
        gather.run(out, feed)
    if scatters:
        scatter.run(out, feed)
    while pending:
        feed()
    for copy in own:
        copy.wait()
    if swaps:
        out.landed("swap")
    out.finish()


def move(place, collective_id, swaps=(), gathers=(), scatters=(), tails=0, held=0):
    lean = len(swaps) > 0
    lines, cores, levels, across = place.grid()
    copies = len(swaps) * (2 * levels * across - across - 1)
    boxes = []
    if len(swaps) > 0 and len(gathers) + len(scatters) > 0:
        boxes += [pltpu.VMEM((across - 1, levels - 1) + a.shape[1:], a.dtype) for a in swaps]
    shapes = [jax.ShapeDtypeStruct(a.shape, a.dtype) for a in swaps]
    for n, shard in enumerate(gathers):
        rows, cols = shard.shape[-2:]
        if shard.ndim == 2:
            copies += 2 * (levels - 1)
        grid = place.grid()
        if n < len(gathers) - tails:
            count = len(halves_of(cols, lean)) * (across + lines + cores - 3)
            copies += len(chunks_of(rows, 8)) * count
        else:
            grid = (levels,)
        shapes.append(jax.ShapeDtypeStruct(grid + (rows, cols), shard.dtype))
    for n, part in enumerate(scatters):
        rows, cols = part.shape[-2:]
        keeps = n >= len(scatters) - held
        count = 0 if keeps else levels - 1
        if part.ndim > 3:
            count += (cores - 1) + len(halves_of(cols, lean)) * (lines + across - 2)
            count *= len(chunks_of(rows))
        copies += count
        boxes += scatter_boxes(place, part, lean, keeps)
        shapes.append(
            jax.ShapeDtypeStruct((levels, rows, cols), part.dtype)
            if keeps
            else jax.ShapeDtypeStruct((rows, cols), jnp.float32)
        )

    def is_result(a):
        return a.dtype == jnp.float32 and a.shape[-1] > 128

    return pl.pallas_call(
        functools.partial(
            move_kernel, place, (len(swaps), len(gathers), len(scatters)), lean, tails, held
        ),
        out_shape=shapes,
        in_specs=[pl.BlockSpec(memory_space=pl.ANY)] * len(shapes),
        out_specs=[
            pl.BlockSpec(memory_space=pltpu.HBM if is_result(a) else pl.ANY)
            for a in shapes
        ],
        scratch_shapes=boxes
        + [
            pltpu.SemaphoreType.DMA((len(shapes),)),
            pltpu.SemaphoreType.DMA((copies,)),
            pltpu.SemaphoreType.DMA((copies,)),
        ],
        compiler_params=pltpu.CompilerParams(
            collective_id=collective_id,
            has_side_effects=True,
            vmem_limit_bytes=VMEM_BYTES,
        ),
        name=f"move_{collective_id}",
    )(*swaps, *gathers, *scatters)


def side_by_side(ref):
    return jnp.concatenate([ref[s] for s in range(ref.shape[0])], axis=1)


def dot_first(left, right):
    return lax.dot_general(
        left, right, (((0,), (0,)), ((), ())), preferred_element_type=jnp.float32
    )


def dot_last(left, right):
    return lax.dot_general(
        left, right, (((1,), (1,)), ((), ())), preferred_element_type=jnp.float32
    )


def attend_kernel(q_ref, k_ref, v_ref, o_ref, full_ref, sum_ref):
    tokens = q_ref.shape[-1]
    each = ATT_BLOCK // tokens
    keys, values = side_by_side(k_ref), side_by_side(v_ref)
    for block in range(q_ref.shape[0] // each):
        first = block * each
        limit = (block + 1) * ATT_BLOCK
        queries = jnp.concatenate([q_ref[first + s] for s in range(each)], axis=1)
        weights = jnp.exp(dot_first(keys[:, :limit], queries))
        sums = jnp.sum(weights, axis=0, keepdims=True)
        mixed = jnp.dot(
            values[:, :limit],
            weights.astype(jnp.bfloat16),
            preferred_element_type=jnp.float32,
        )
        mixed = mixed / sums
        sum_ref[0, 0, :, pl.ds(block * ATT_BLOCK, ATT_BLOCK)] = sums
        for s in range(each):
            piece = mixed[:, s * tokens : (s + 1) * tokens]
            full_ref[first + s] = piece
            o_ref[first + s] = piece.astype(jnp.bfloat16)


def attend_specs(devices, tokens):
    piece = pl.BlockSpec((devices, HEAD_DIM, tokens), lambda m, h: (0, h, m))
    sums = pl.BlockSpec((1, 1, 1, devices * tokens), lambda m, h: (m, h, 0, 0))
    return piece, sums


def attend(queries, keys, values, tokens):
    devices, rows, cols = queries.shape
    grid = (cols // tokens, rows // HEAD_DIM)
    piece, sums = attend_specs(devices, tokens)
    return pl.pallas_call(
        attend_kernel,
        grid=grid,
        out_shape=[
            jax.ShapeDtypeStruct(queries.shape, jnp.bfloat16),
            jax.ShapeDtypeStruct(queries.shape, jnp.float32),
            jax.ShapeDtypeStruct(grid + (1, devices * tokens), jnp.float32),
        ],
        in_specs=[piece] * 3,
        out_specs=[piece, piece, sums],
        compiler_params=pltpu.CompilerParams(vmem_limit_bytes=VMEM_BYTES),
        name="attend",
    )(queries, keys, values)


def slopes_kernel(
    q_ref, k_ref, v_ref, do_ref, full_ref, sum_ref, rate_ref, dq_ref, dk_ref, dv_ref
):
    tokens = q_ref.shape[-1]
    each = ATT_BLOCK // tokens
    keys, values = side_by_side(k_ref), side_by_side(v_ref)
    rate = rate_ref[...]
    key_total = value_total = None
    for block in reversed(range(q_ref.shape[0] // each)):
        first = block * each
        limit = (block + 1) * ATT_BLOCK

        def pick(ref):
            return jnp.concatenate([ref[first + s] for s in range(each)], axis=1)

        queries = pick(q_ref)
        slope = pick(do_ref).astype(jnp.float32)
        sums = sum_ref[0, 0, :, pl.ds(block * ATT_BLOCK, ATT_BLOCK)]
        scaled = (slope / sums).astype(jnp.bfloat16)
        centre = jnp.sum(slope * pick(full_ref), axis=0, keepdims=True) / sums
        weights = jnp.exp(dot_first(keys[:, :limit], queries))
        dots = dot_first(values[:, :limit], scaled)
        slopes = (weights * (dots - centre)).astype(jnp.bfloat16)
        weights = weights.astype(jnp.bfloat16)
        query_part = jnp.dot(keys[:, :limit], slopes, preferred_element_type=jnp.float32)
        query_part = (query_part * rate).astype(jnp.bfloat16)
        for s in range(each):
            dq_ref[first + s] = query_part[:, s * tokens : (s + 1) * tokens]
        key_part = dot_last(queries, slopes)
        value_part = dot_last(scaled, weights)
        if key_total is None:
            key_total, value_total = key_part, value_part
        else:
            key_total = jnp.concatenate(
                [key_total[:, :limit] + key_part, key_total[:, limit:]], axis=1
            )
            value_total = jnp.concatenate(
                [value_total[:, :limit] + value_part, value_total[:, limit:]], axis=1
            )
    for s in range(q_ref.shape[0]):
        cols = slice(s * tokens, (s + 1) * tokens)
        dk_ref[s] = key_total[:, cols].astype(jnp.bfloat16)
        dv_ref[s] = value_total[:, cols].astype(jnp.bfloat16)


def slopes(queries, keys, values, slope, full, sums, rate, tokens):
    devices, rows, cols = queries.shape
    grid = (cols // tokens, rows // HEAD_DIM)
    piece, sum_spec = attend_specs(devices, tokens)
    return pl.pallas_call(
        slopes_kernel,
        grid=grid,
        out_shape=[jax.ShapeDtypeStruct(queries.shape, jnp.bfloat16)] * 3,
        in_specs=[piece] * 5
        + [sum_spec, pl.BlockSpec((HEAD_DIM, 1), lambda m, h: (0, 0))],
        out_specs=[piece] * 3,
        compiler_params=pltpu.CompilerParams(vmem_limit_bytes=VMEM_BYTES),
        name="slopes",
    )(queries, keys, values, slope, full, sums, rate)


def rms_scale(values):
    return lax.rsqrt(jnp.mean(values * values, axis=-1, keepdims=True) + EPSILON)


def contract(spec, left, right):
    return jnp.einsum(spec, left, right, preferred_element_type=jnp.float32)


def on_device(place, devices, *args):
    inputs, cotangent = args[:2]
    (
        norm_one,
        query_mat,
        query_add,
        key_mat,
        value_mat,
        value_add,
        output_mat,
        output_add,
        norm_two,
        hidden_mat,
        hidden_add,
        project_mat,
        project_add,
    ) = args[2:15]
    depth = args[15].astype(jnp.float32)
    micro, tokens, seqs, width = inputs.shape
    rows = micro * tokens * seqs
    vectors = (norm_one, query_add, value_add, output_add, norm_two, hidden_add, project_add)
    share = norm_one.shape[0]
    small = jnp.pad(jnp.stack(vectors), ((0, 16 - len(vectors)), (0, 128 - share)))
    query_mat, small, key_mat, value_mat, output_mat, hidden_mat, project_mat = move(
        place,
        0,
        gathers=(query_mat, small, key_mat, value_mat, output_mat, hidden_mat, project_mat),
        tails=3,
    )
    small = small.reshape(-1, 16, 128)[:, : len(vectors), :share]
    small = small.transpose(1, 0, 2).reshape(len(vectors), width).astype(jnp.float32)
    gain_one, query_add, value_add, output_add, gain_two, hidden_add, project_add = small
    query_mat, key_mat, value_mat = (
        g.reshape(width, width) for g in (query_mat, key_mat, value_mat)
    )

    def to_rows(array):
        return array.transpose(0, 2, 1, 3).reshape(rows, width)

    def from_rows(array):
        return array.reshape(micro, seqs, tokens, width).transpose(0, 2, 1, 3)

    rate = SOFT_BASE / math.sqrt(HEAD_DIM) * jax.nn.softplus(depth)
    rate_full = jnp.tile(rate, HEADS)[:, None]
    xfloat = to_rows(inputs).astype(jnp.float32)
    inv_one = rms_scale(xfloat)
    normed = (xfloat * inv_one * gain_one).astype(jnp.bfloat16)
    query_pre = contract("df,rd->fr", query_mat, normed) + query_add[:, None]
    queries = (query_pre * rate_full).astype(jnp.bfloat16)
    keys = contract("df,rd->fr", key_mat, normed).astype(jnp.bfloat16)
    values = (contract("df,rd->fr", value_mat, normed) + value_add[:, None]).astype(jnp.bfloat16)

    def split(array):
        return array.reshape(devices, width // devices, rows)

    q_in, k_in, v_in, output_mat, hidden_mat, project_mat = move(
        place,
        1,
        (split(queries), split(keys), split(values)),
        (output_mat, hidden_mat, project_mat),
    )
    output_mat, hidden_mat, project_mat = (
        g.reshape(width, width) for g in (output_mat, hidden_mat, project_mat)
    )
    mixed, full, sums = attend(q_in, k_in, v_in, tokens)
    (mixed,) = move(place, 2, (mixed,))
    mixed = mixed.reshape(width, rows)
    residual = xfloat + (contract("fr,fd->rd", mixed, output_mat) + output_add)
    inv_two = rms_scale(residual)
    second = (residual * inv_two * gain_two).astype(jnp.bfloat16)
    hidden_pre = contract("rd,df->rf", second, hidden_mat) + hidden_add
    active = jax.nn.silu(hidden_pre).astype(jnp.bfloat16)
    result = residual + (contract("rf,fd->rd", active, project_mat) + project_add)
    result = from_rows(result.astype(jnp.bfloat16))

    upper = to_rows(cotangent)
    project_grad = contract("rf,rd->fd", active, upper)
    project_bias_grad = jnp.sum(upper.astype(jnp.float32), axis=0)
    active_grad = contract("rd,fd->rf", upper, project_mat)
    logistic = jax.nn.sigmoid(hidden_pre)
    hidden_grad = (active_grad * logistic * (1.0 + hidden_pre * (1.0 - logistic))).astype(
        jnp.bfloat16
    )
    hidden_mat_grad = contract("rd,rf->df", second, hidden_grad)
    hidden_bias_grad = jnp.sum(hidden_grad.astype(jnp.float32), axis=0)
    second_grad = contract("rf,df->rd", hidden_grad, hidden_mat)
    normal_two = residual * inv_two
    scaled_two = second_grad * gain_two
    norm_two_grad = jnp.sum(second_grad * normal_two, axis=0)
    residual_grad = upper.astype(jnp.float32) + inv_two * (
        scaled_two - normal_two * jnp.mean(scaled_two * normal_two, axis=-1, keepdims=True)
    )
    branch_grad = residual_grad.astype(jnp.bfloat16)
    output_mat_grad = contract("fr,rd->fd", mixed, branch_grad)
    output_bias_grad = jnp.sum(branch_grad.astype(jnp.float32), axis=0)
    mixed_grad = contract("fd,rd->fr", output_mat, branch_grad).astype(jnp.bfloat16)

    def as_parts(*grads):
        return tuple(
            g.astype(jnp.bfloat16).reshape(place.grid() + (share, width)) for g in grads
        )

    merged = share % 8 == 0
    (do_in,) = move(place, 3, (split(mixed_grad),))
    slopes_out = slopes(q_in, k_in, v_in, do_in, full, sums, rate[:, None], tokens)
    early = as_parts(output_mat_grad, hidden_mat_grad, project_grad) if merged else ()
    query_slope, key_grad, value_grad, *early = move(
        place, 4, slopes_out, (), early, held=2 if merged else 0
    )
    query_slope, key_grad, value_grad = (
        a.reshape(width, rows) for a in (query_slope, key_grad, value_grad)
    )
    query_float = query_slope.astype(jnp.float32)
    scale_part = jnp.sum(query_float / rate_full * query_pre, axis=1)
    scale_part = jnp.sum(scale_part.reshape(HEADS, HEAD_DIM), axis=0)
    query_mat_grad = contract("rd,fr->df", normed, query_slope)
    query_bias_grad = jnp.sum(query_float, axis=1)
    key_mat_grad = contract("rd,fr->df", normed, key_grad)
    value_mat_grad = contract("rd,fr->df", normed, value_grad)
    value_bias_grad = jnp.sum(value_grad.astype(jnp.float32), axis=1)
    normed_grad = (
        contract("fr,df->rd", query_slope, query_mat)
        + contract("fr,df->rd", key_grad, key_mat)
        + contract("fr,df->rd", value_grad, value_mat)
    )
    normal_one = xfloat * inv_one
    scaled_one = normed_grad * gain_one
    norm_one_grad = jnp.sum(normed_grad * normal_one, axis=0)
    source_grad = residual_grad + inv_one * (
        scaled_one - normal_one * jnp.mean(scaled_one * normal_one, axis=-1, keepdims=True)
    )
    source_grad = from_rows(source_grad.astype(jnp.bfloat16))

    vector_grads = jnp.stack(
        (
            norm_one_grad,
            query_bias_grad,
            value_bias_grad,
            output_bias_grad,
            norm_two_grad,
            hidden_bias_grad,
            project_bias_grad,
        )
    )
    vector_grads = vector_grads.reshape(7, -1, share).transpose(1, 0, 2)
    vector_grads = jnp.pad(vector_grads, ((0, 0), (0, 0), (0, 128 - share)))
    scale_row = jnp.pad(scale_part, (0, 128 - HEAD_DIM))
    scale_row = jnp.broadcast_to(scale_row, (vector_grads.shape[0], 1, 128))
    vector_grads = jnp.concatenate([vector_grads, scale_row], axis=1)
    vector_grads = vector_grads.reshape(place.grid() + (8, 128))
    late = as_parts(query_mat_grad, key_mat_grad, value_mat_grad)
    if merged:
        output_mat_grad, *early = early
        hidden_mat_grad, project_grad, *late, vector_sums = move(
            place, 5, scatters=(*early, *late, vector_grads)
        )
    else:
        (vector_sums,) = move(place, 5, scatters=(vector_grads,))
        early = as_parts(output_mat_grad, hidden_mat_grad, project_grad)
        early = [move(place, 6, scatters=(p,))[0] for p in early]
        output_mat_grad, hidden_mat_grad, project_grad = early
        late = [move(place, 6, scatters=(p,))[0] for p in late]
    query_mat_grad, key_mat_grad, value_mat_grad = late
    g_one, g_query, g_value, g_output, g_two, g_hidden, g_project = (
        vector_sums[n, :share] for n in range(7)
    )
    scale_summed = vector_sums[7, :HEAD_DIM]
    depth_grad = scale_summed * (SOFT_BASE / math.sqrt(HEAD_DIM)) * jax.nn.sigmoid(depth)
    return (
        result,
        source_grad,
        g_one,
        query_mat_grad,
        g_query,
        key_mat_grad,
        value_mat_grad,
        g_value,
        output_mat_grad,
        g_output,
        g_two,
        hidden_mat_grad,
        g_hidden,
        project_grad,
        g_project,
        depth_grad,
    )


def solution(mesh):
    both = ("dp", "seq")
    token, vector, matrix = P(None, "seq", "dp", None), P(both), P(both, None)
    weights = (
        vector,
        matrix,
        vector,
        matrix,
        matrix,
        vector,
        matrix,
        vector,
        vector,
        matrix,
        vector,
        matrix,
        vector,
    )
    specs = (token, token) + weights + (P(),)
    place = Place(mesh.shape["dp"], mesh.shape["seq"])
    return jax.shard_map(
        functools.partial(on_device, place, mesh.shape["seq"]),
        mesh=mesh,
        in_specs=specs,
        out_specs=specs,
        check_vma=False,
    )
```

```python
import functools
import itertools
import math

import jax
import jax.numpy as jnp
from jax import lax
from jax.experimental import pallas as pl
from jax.experimental.pallas import tpu as pltpu
from jax.sharding import PartitionSpec as P

HEADS = 16
HEAD_DIM = 80
ATT_BLOCK = 256
SOFT_BASE = 1.442695041
EPSILON = 1e-06
MESH = pl.DeviceIdType.MESH
VMEM_BYTES = 60 * 1024 * 1024
LAG = 2


class Place:
    def __init__(self, dp, seq):
        self.cores = 2 if dp % 2 == 0 else 1
        self.lines = dp // self.cores
        self.levels = 4 if seq % 4 == 0 else seq
        self.across = seq // self.levels
        self.sizes = {
            "y": self.lines,
            "c": self.cores,
            "z": self.levels,
            "x": self.across,
        }

    def here(self):
        dp = lax.axis_index("dp")
        seq = lax.axis_index("seq")
        return {
            "y": dp // self.cores,
            "c": dp % self.cores,
            "z": seq // self.across,
            "x": seq % self.across,
        }

    def shift(self, spot, axis, step):
        moved = dict(spot)
        moved[axis] = lax.rem(spot[axis] + step, self.sizes[axis])
        return moved

    def device(self, spot):
        return (
            spot["y"] * self.cores + spot["c"],
            spot["z"] * self.across + spot["x"],
        )

    def grid(self):
        return (self.lines, self.cores, self.levels, self.across)

    def greet(self, spot, wide):
        barrier = pltpu.get_barrier_semaphore()
        dp, seq = self.device(spot)
        peers = [
            self.device(self.shift(spot, axis, step))
            for axis in ("yc" if wide else "zxyc")
            for step in range(1, self.sizes[axis])
        ]
        if wide:
            devices = self.levels * self.across
            peers += [(dp, lax.rem(seq + step, devices)) for step in range(1, devices)]
        for peer in peers:
            pl.semaphore_signal(barrier, inc=1, device_id=peer, device_id_type=MESH)
        pl.semaphore_wait(barrier, len(peers))


def halves_of(cols, lean):
    if lean and cols % 640 == 0:
        cut = cols * 4 // 5
    elif cols % 256 == 0:
        cut = cols // 2
    else:
        return ((slice(0, cols), "xy"),)
    return ((slice(0, cut), "xy"), (slice(cut, cols), "yx"))


def chunks_of(rows):
    if rows % 8 == 0 and rows >= 32:
        cut = rows // 32 * 16
        return (slice(0, cut), slice(cut, rows))
    return (slice(0, rows),)


class Sender:
    def __init__(self, place, spot, send_sem, recv_sem):
        self.place = place
        self.spot = spot
        self.send_sem = send_sem
        self.recv_sem = recv_sem
        self.count = itertools.count()
        self.open = {}
        self.every = []

    def put(self, key, device, source, target, leaves=None, comes=None):
        at = next(self.count)
        copy = pltpu.make_async_remote_copy(
            src_ref=source,
            dst_ref=target,
            send_sem=self.send_sem.at[at],
            recv_sem=self.recv_sem.at[at],
            device_id=device,
            device_id_type=MESH,
        )
        self.guard(leaves, copy.start)
        self.open.setdefault(key, []).append((comes, copy))
        self.every.append((leaves, copy))

    def guard(self, when, act):
        if when is None:
            act()
        else:
            pl.when(when)(act)

    def go(self, key, axis, source, target):
        self.open[key] = []
        for step in range(1, self.place.sizes[axis]):
            peer = self.place.shift(self.spot, axis, step)
            self.put(key, self.place.device(peer), source(peer), target(step))

    def chain(self, key, turn, own, slot):
        levels, z = self.place.levels, self.spot["z"]
        self.open[key] = []

        def inside(at):
            return jnp.logical_and(at >= 0, at < levels)

        for way in (1, -1):
            shard, to, back = z - turn * way, z + way, z - (turn + 1) * way
            part = slot(lax.rem(shard + levels, levels))
            peer = dict(self.spot, z=lax.rem(to + levels, levels))
            self.put(
                key,
                self.place.device(peer),
                own if turn == 0 else part,
                part,
                jnp.logical_and(inside(shard), inside(to)),
                inside(back),
            )

    def landed(self, key):
        for comes, copy in self.open[key]:
            self.guard(comes, copy.wait_recv)

    def finish(self):
        for leaves, copy in self.every:
            self.guard(leaves, copy.wait_send)


class Gather:
    def __init__(self, place, spot, lean, tails, shards, wholes, own_sem):
        self.place, self.spot, self.lean, self.tails = place, spot, lean, tails
        self.shards, self.wholes = shards, wholes
        y, c, z, x = (spot[k] for k in "yczx")
        self.own = []
        for n, shard in enumerate(shards):
            if n >= len(shards) - tails:
                target = wholes[n].at[z]
            elif len(shard.shape) == 3:
                target = wholes[n].at[y, c, :, x]
            else:
                target = wholes[n].at[y, c, z, x]
            copy = pltpu.make_async_copy(shard, target, own_sem[n])
            copy.start()
            self.own.append(copy)

    def run(self, out, feed):
        shards, wholes = self.shards, self.wholes
        y, c, _, x = (self.spot[k] for k in "yczx")
        turns = self.place.levels - 1
        full = len(shards) - self.tails
        raw = [n for n, s in enumerate(shards) if len(s.shape) == 2]
        jobs = [(n, r) for n in range(full) for r in chunks_of(shards[n].shape[-2])]
        filled = set()

        def halves(n):
            return enumerate(halves_of(shards[n].shape[-1], self.lean))

        def along(turn, n):
            def slot(level):
                return wholes[n].at[y, c, level, x] if n < full else wholes[n].at[level]

            if turn > 0:
                out.landed(("z", n, turn - 1))
            if turn < turns:
                out.chain(("z", n, turn), turn, shards[n], slot)

        def fill(n):
            if n not in filled:
                filled.add(n)
                self.own[n].wait()

        def two(job, n, rows):
            lined = len(shards[n].shape) == 3
            if not lined:
                fill(n)
            for half, (cols, order) in halves(n):
                part = wholes[n].at[y, c, :, x, rows, cols]
                source = shards[n].at[:, rows, cols] if lined else part
                out.go((job, half, 2), order[0], lambda peer: source, lambda step: part)

        def three(job, n, rows):
            fill(n)
            for half, (cols, order) in halves(n):
                out.landed((job, half, 2))
                if order == "xy":
                    part = wholes[n].at[y, c, :, :, rows, cols]
                else:
                    part = wholes[n].at[:, c, :, x, rows, cols]
                out.go((job, half, 3), order[1], lambda peer: part, lambda step: part)

        def four(job, n, rows):
            for half, (cols, order) in halves(n):
                out.landed((job, half, 3))
                part = wholes[n].at[:, c, :, :, rows, cols]
                out.go((job, half, 4), "c", lambda peer: part, lambda step: part)

        def five(job, n, rows):
            for half, _ in halves(n):
                out.landed((job, half, 4))

        steps = iter(range(len(jobs) + 3 * LAG))

        def advance():
            step = next(steps, None)
            if step is not None:
                for stage, late in ((two, 0), (three, LAG), (four, 2 * LAG), (five, 3 * LAG)):
                    if 0 <= step - late < len(jobs):
                        stage(("gather", step - late), *jobs[step - late])

        if raw:
            for time in range(len(raw) + turns):
                for turn in range(turns + 1):
                    if 0 <= time - turn < len(raw):
                        along(turn, raw[time - turn])
                done = time - turns
                if 0 <= done < full:
                    for _ in chunks_of(shards[raw[done]].shape[-2]):
                        advance()
        for _ in range(len(jobs) + 3 * LAG):
            advance()
            feed()
        for n in range(len(shards)):
            fill(n)


def total(values):
    result = values[0].astype(jnp.float32)
    for value in values[1:]:
        result = result + value.astype(jnp.float32)
    return result


class Scatter:
    def __init__(self, place, spot, lean, held, parts, totals, boxes, own_sem):
        self.place, self.spot, self.lean = place, spot, lean
        self.parts, self.totals = parts, totals
        self.full = len(parts) - held
        self.jobs = [
            (n, r)
            for n, p in enumerate(parts)
            if len(p.shape) > 3
            for r in chunks_of(p.shape[-2])
        ]
        self.own_sem = own_sem
        self.sums, self.cores, self.seconds, self.thirds, self.fourths = [], [], [], [], []
        self.results, self.own = [], []
        for n, part in enumerate(parts):
            self.sums.append(boxes.pop(0))
            if len(part.shape) > 3:
                self.cores.append(boxes.pop(0))
                halves = halves_of(part.shape[-1], lean)
                self.seconds.append([boxes.pop(0) for _ in halves])
                self.thirds.append([boxes.pop(0) for _ in halves])
                mine = part.at[:, spot["c"]]
            else:
                for boxed in (self.cores, self.seconds, self.thirds):
                    boxed.append(None)
                mine = part.at[spot["z"]]
            if n < self.full:
                self.fourths.append(boxes.pop(0))
                self.results.append(boxes.pop(0))
            else:
                self.fourths.append(None)
                self.results.append(self.sums[n].at[spot["y"], :, spot["x"]])
            copy = pltpu.make_async_copy(mine, self.sums[n], own_sem[n])
            copy.start()
            self.own.append(copy)

    def run(self, out, feed):
        place, parts, sums = self.place, self.parts, self.sums
        cores, results = self.cores, self.results
        y, c, z, x = (self.spot[k] for k in "yczx")
        lines, _, levels, across = place.grid()
        filled = set()

        def halves(n):
            return enumerate(halves_of(parts[n].shape[-1], self.lean))

        def one(job, n, rows):
            out.go(
                (job, 1),
                "c",
                lambda peer: parts[n].at[:, peer["c"], :, :, rows],
                lambda step: cores[n].at[:, :, :, rows],
            )

        def two(job, n, rows):
            if n not in filled:
                filled.add(n)
                self.own[n].wait()
            out.landed((job, 1))
            if place.cores > 1:

                @pl.loop(0, lines * levels * across)
                def _(at):
                    where = (at // (levels * across), (at // across) % levels, at % across)
                    sums[n][where + (rows,)] = total(
                        [sums[n][where + (rows,)], cores[n][where + (rows,)]]
                    ).astype(sums[n].dtype)

            for half, (cols, order) in halves(n):
                box = self.seconds[n][half]
                if order == "xy":
                    out.go(
                        (job, half, 2),
                        "y",
                        lambda peer: sums[n].at[peer["y"], :, :, rows, cols],
                        lambda step: box.at[step - 1, :, :, rows],
                    )
                else:
                    out.go(
                        (job, half, 2),
                        "x",
                        lambda peer: sums[n].at[:, :, peer["x"], rows, cols],
                        lambda step: box.at[step - 1, :, :, rows],
                    )

        def three(job, n, rows):
            for half, (cols, order) in halves(n):
                out.landed((job, half, 2))
                box, later = self.seconds[n][half], self.thirds[n][half]
                if order == "xy":

                    @pl.loop(0, levels * across)
                    def _(at):
                        zz, xx = at // across, at % across
                        values = [sums[n][y, zz, xx, rows, cols]]
                        values += [box[k, zz, xx, rows] for k in range(lines - 1)]
                        sums[n][y, zz, xx, rows, cols] = total(values).astype(sums[n].dtype)

                    out.go(
                        (job, half, 3),
                        "x",
                        lambda peer: sums[n].at[y, :, peer["x"], rows, cols],
                        lambda step: later.at[step - 1, :, rows],
                    )
                else:

                    @pl.loop(0, lines * levels)
                    def _(at):
                        yy, zz = at // levels, at % levels
                        values = [sums[n][yy, zz, x, rows, cols]]
                        values += [box[k, yy, zz, rows] for k in range(across - 1)]
                        sums[n][yy, zz, x, rows, cols] = total(values).astype(sums[n].dtype)

                    out.go(
                        (job, half, 3),
                        "y",
                        lambda peer: sums[n].at[peer["y"], :, x, rows, cols],
                        lambda step: later.at[step - 1, :, rows],
                    )

        def four(job, n, rows):
            for half, (cols, order) in halves(n):
                out.landed((job, half, 3))
                box = self.thirds[n][half]

                @pl.loop(0, levels)
                def _(zz):
                    values = [sums[n][y, zz, x, rows, cols]]
                    values += [box[k, zz, rows] for k in range(box.shape[0])]
                    sums[n][y, zz, x, rows, cols] = total(values).astype(sums[n].dtype)

            if n < self.full:
                out.go(
                    (job, 4),
                    "z",
                    lambda peer: sums[n].at[y, peer["z"], x, rows],
                    lambda step: self.fourths[n].at[step - 1, rows],
                )

        def five(job, n, rows):
            if n >= self.full:
                return
            out.landed((job, 4))
            values = [sums[n][y, z, x, rows]]
            values += [self.fourths[n][k, rows] for k in range(levels - 1)]
            results[n][rows] = total(values)

        def first(n):
            out.go(
                ("tail", n),
                "z",
                lambda peer: parts[n].at[peer["z"]],
                lambda step: self.fourths[n].at[step - 1],
            )

        def final(n):
            self.own[n].wait()
            out.landed(("tail", n))
            values = [sums[n][...]] + [self.fourths[n][k] for k in range(levels - 1)]
            results[n][...] = total(values)

        jobs = [(("scatter", at),) + job for at, job in enumerate(self.jobs)]
        tails = [n for n, p in enumerate(parts) if len(p.shape) == 3]
        for n in tails:
            first(n)
        for step in range(len(jobs) + 4 * LAG):
            if step > 2 and tails:
                final(tails.pop(0))
            for turn, stage in enumerate((one, two, three, four, five)):
                late = turn * LAG
                if 0 <= step - late < len(jobs):
                    stage(*jobs[step - late])
            feed()
        last = []
        for n, result in enumerate(results):
            copy = pltpu.make_async_copy(result, self.totals[n], self.own_sem[n])
            copy.start()
            last.append(copy)
        for copy in last:
            copy.wait()


def scatter_boxes(place, part, lean, held):
    lines, _, levels, across = place.grid()
    rows, cols = part.shape[-2:]
    final = [
        pltpu.VMEM((levels - 1, rows, cols), part.dtype),
        pltpu.VMEM((rows, cols), jnp.float32),
    ]
    if part.ndim == 3:
        return [pltpu.VMEM((rows, cols), part.dtype)] + final
    block = pltpu.VMEM((lines, levels, across, rows, cols), part.dtype)
    first, later = [], []
    for piece, order in halves_of(cols, lean):
        size = (rows, piece.stop - piece.start)
        steps = (lines - 1, across - 1) if order == "xy" else (across - 1, lines - 1)
        middle = (levels, across) if order == "xy" else (lines, levels)
        first.append(pltpu.VMEM((steps[0],) + middle + size, part.dtype))
        later.append(pltpu.VMEM((steps[1], levels) + size, part.dtype))
    return [block, block] + first + later + ([] if held else final)


def move_kernel(place, counts, lean, tails, held, *refs):
    refs = list(refs)
    swaps, gathers, scatters = counts
    whole = swaps + gathers + scatters
    ins, outs, rest = refs[:whole], refs[whole : 2 * whole], refs[2 * whole :]
    own_sem, send_sem, recv_sem = rest[-3:]
    staged = swaps > 0 and whole > swaps
    relays, boxes = rest[: swaps * staged], rest[swaps * staged : -3]
    spot = place.here()
    dp, me = place.device(spot)
    devices = place.levels * place.across
    sent, got = ins[:swaps], outs[:swaps]
    own = []
    for n in range(swaps):
        copy = pltpu.make_async_copy(sent[n].at[me], got[n].at[me], own_sem.at[n])
        copy.start()
        own.append(copy)
    cut = swaps + gathers
    gather = Gather(
        place, spot, lean, tails, ins[swaps:cut], outs[swaps:cut], [own_sem.at[n] for n in range(swaps, cut)]
    )
    scatter = Scatter(
        place, spot, lean, held, ins[cut:], outs[cut:], boxes, [own_sem.at[n] for n in range(cut, whole)]
    )
    place.greet(spot, swaps > 0 and not staged)
    out = Sender(place, spot, send_sem, recv_sem)
    levels, across = place.levels, place.across
    z, x = spot["z"], spot["x"]

    def straight(n):
        for step in range(1, devices):
            peer = lax.rem(me + step, devices)
            out.put("swap", (dp, peer), sent[n].at[peer], got[n].at[me])

    def along_x(n):
        for skip in range(1, across):
            peer = place.shift(spot, "x", skip)
            device = place.device(peer)
            out.put("swap", device, sent[n].at[device[1]], got[n].at[me])
            for step in range(1, levels):
                piece = place.device(place.shift(peer, "z", step))[1]
                out.put(
                    ("relay", n), device, sent[n].at[piece], relays[n].at[skip - 1, step - 1]
                )

    def along_z(n):
        for step in range(1, levels):
            device = place.device(place.shift(spot, "z", step))
            out.put("swap", device, sent[n].at[device[1]], got[n].at[me])

    def pass_on(n):
        out.landed(("relay", n))
        for skip in range(1, across):
            source = place.device(place.shift(spot, "x", across - skip))[1]
            for step in range(1, levels):
                device = place.device(place.shift(spot, "z", step))
                out.put("swap", device, relays[n].at[skip - 1, step - 1], got[n].at[source])

    if staged:
        apart = 2 if gathers else 1
        pending = [[] for _ in range(apart * (swaps - 1) + LAG + 2)]
        for n in range(swaps):
            pending[0 if gathers else max(n - 1, 0)].append((along_z, n))
        for n in range(swaps):
            pending[apart * n].append((along_x, n))
            pending[apart * n + LAG + 1].append((pass_on, n))
    else:
        pending = [[(straight, n)] for n in range(swaps)]

    def feed():
        for act, n in pending.pop(0) if pending else ():
            act(n)

    if gathers:
        gather.run(out, feed)
    if scatters:
        scatter.run(out, feed)
    while pending:
        feed()
    for copy in own:
        copy.wait()
    if swaps:
        out.landed("swap")
    out.finish()


def move(place, collective_id, swaps=(), gathers=(), scatters=(), tails=0, held=0):
    lean = len(swaps) > 0
    lines, cores, levels, across = place.grid()
    copies = len(swaps) * (2 * levels * across - across - 1)
    boxes = []
    if len(swaps) > 0 and len(gathers) + len(scatters) > 0:
        boxes += [pltpu.VMEM((across - 1, levels - 1) + a.shape[1:], a.dtype) for a in swaps]
    shapes = [jax.ShapeDtypeStruct(a.shape, a.dtype) for a in swaps]
    for n, shard in enumerate(gathers):
        rows, cols = shard.shape[-2:]
        if shard.ndim == 2:
            copies += 2 * (levels - 1)
        grid = place.grid()
        if n < len(gathers) - tails:
            count = len(halves_of(cols, lean)) * (across + lines + cores - 3)
            copies += len(chunks_of(rows)) * count
        else:
            grid = (levels,)
        shapes.append(jax.ShapeDtypeStruct(grid + (rows, cols), shard.dtype))
    for n, part in enumerate(scatters):
        rows, cols = part.shape[-2:]
        keeps = n >= len(scatters) - held
        count = 0 if keeps else levels - 1
        if part.ndim > 3:
            count += (cores - 1) + len(halves_of(cols, lean)) * (lines + across - 2)
            count *= len(chunks_of(rows))
        copies += count
        boxes += scatter_boxes(place, part, lean, keeps)
        shapes.append(
            jax.ShapeDtypeStruct((levels, rows, cols), part.dtype)
            if keeps
            else jax.ShapeDtypeStruct((rows, cols), jnp.float32)
        )

    def is_result(a):
        return a.dtype == jnp.float32 and a.shape[-1] > 128

    return pl.pallas_call(
        functools.partial(
            move_kernel, place, (len(swaps), len(gathers), len(scatters)), lean, tails, held
        ),
        out_shape=shapes,
        in_specs=[pl.BlockSpec(memory_space=pl.ANY)] * len(shapes),
        out_specs=[
            pl.BlockSpec(memory_space=pltpu.HBM if is_result(a) else pl.ANY)
            for a in shapes
        ],
        scratch_shapes=boxes
        + [
            pltpu.SemaphoreType.DMA((len(shapes),)),
            pltpu.SemaphoreType.DMA((copies,)),
            pltpu.SemaphoreType.DMA((copies,)),
        ],
        compiler_params=pltpu.CompilerParams(
            collective_id=collective_id,
            has_side_effects=True,
            vmem_limit_bytes=VMEM_BYTES,
        ),
        name=f"move_{collective_id}",
    )(*swaps, *gathers, *scatters)


def side_by_side(ref):
    return jnp.concatenate([ref[s] for s in range(ref.shape[0])], axis=1)


def dot_first(left, right):
    return lax.dot_general(
        left, right, (((0,), (0,)), ((), ())), preferred_element_type=jnp.float32
    )


def dot_last(left, right):
    return lax.dot_general(
        left, right, (((1,), (1,)), ((), ())), preferred_element_type=jnp.float32
    )


def attend_kernel(q_ref, k_ref, v_ref, o_ref, full_ref, sum_ref):
    tokens = q_ref.shape[-1]
    each = ATT_BLOCK // tokens
    keys, values = side_by_side(k_ref), side_by_side(v_ref)
    for block in range(q_ref.shape[0] // each):
        first = block * each
        limit = (block + 1) * ATT_BLOCK
        queries = jnp.concatenate([q_ref[first + s] for s in range(each)], axis=1)
        weights = jnp.exp(dot_first(keys[:, :limit], queries))
        sums = jnp.sum(weights, axis=0, keepdims=True)
        mixed = jnp.dot(
            values[:, :limit],
            weights.astype(jnp.bfloat16),
            preferred_element_type=jnp.float32,
        )
        mixed = mixed / sums
        sum_ref[0, 0, :, pl.ds(block * ATT_BLOCK, ATT_BLOCK)] = sums
        for s in range(each):
            piece = mixed[:, s * tokens : (s + 1) * tokens]
            full_ref[first + s] = piece
            o_ref[first + s] = piece.astype(jnp.bfloat16)


def attend_specs(devices, tokens):
    piece = pl.BlockSpec((devices, HEAD_DIM, tokens), lambda m, h: (0, h, m))
    sums = pl.BlockSpec((1, 1, 1, devices * tokens), lambda m, h: (m, h, 0, 0))
    return piece, sums


def attend(queries, keys, values, tokens):
    devices, rows, cols = queries.shape
    grid = (cols // tokens, rows // HEAD_DIM)
    piece, sums = attend_specs(devices, tokens)
    return pl.pallas_call(
        attend_kernel,
        grid=grid,
        out_shape=[
            jax.ShapeDtypeStruct(queries.shape, jnp.bfloat16),
            jax.ShapeDtypeStruct(queries.shape, jnp.float32),
            jax.ShapeDtypeStruct(grid + (1, devices * tokens), jnp.float32),
        ],
        in_specs=[piece] * 3,
        out_specs=[piece, piece, sums],
        compiler_params=pltpu.CompilerParams(vmem_limit_bytes=VMEM_BYTES),
        name="attend",
    )(queries, keys, values)


def slopes_kernel(
    q_ref, k_ref, v_ref, do_ref, full_ref, sum_ref, rate_ref, dq_ref, dk_ref, dv_ref
):
    tokens = q_ref.shape[-1]
    each = ATT_BLOCK // tokens
    keys, values = side_by_side(k_ref), side_by_side(v_ref)
    rate = rate_ref[...]
    key_total = value_total = None
    for block in reversed(range(q_ref.shape[0] // each)):
        first = block * each
        limit = (block + 1) * ATT_BLOCK

        def pick(ref):
            return jnp.concatenate([ref[first + s] for s in range(each)], axis=1)

        queries = pick(q_ref)
        slope = pick(do_ref).astype(jnp.float32)
        sums = sum_ref[0, 0, :, pl.ds(block * ATT_BLOCK, ATT_BLOCK)]
        scaled = (slope / sums).astype(jnp.bfloat16)
        centre = jnp.sum(slope * pick(full_ref), axis=0, keepdims=True) / sums
        weights = jnp.exp(dot_first(keys[:, :limit], queries))
        dots = dot_first(values[:, :limit], scaled)
        slopes = (weights * (dots - centre)).astype(jnp.bfloat16)
        weights = weights.astype(jnp.bfloat16)
        query_part = jnp.dot(keys[:, :limit], slopes, preferred_element_type=jnp.float32)
        query_part = (query_part * rate).astype(jnp.bfloat16)
        for s in range(each):
            dq_ref[first + s] = query_part[:, s * tokens : (s + 1) * tokens]
        key_part = dot_last(queries, slopes)
        value_part = dot_last(scaled, weights)
        if key_total is None:
            key_total, value_total = key_part, value_part
        else:
            key_total = jnp.concatenate(
                [key_total[:, :limit] + key_part, key_total[:, limit:]], axis=1
            )
            value_total = jnp.concatenate(
                [value_total[:, :limit] + value_part, value_total[:, limit:]], axis=1
            )
    for s in range(q_ref.shape[0]):
        cols = slice(s * tokens, (s + 1) * tokens)
        dk_ref[s] = key_total[:, cols].astype(jnp.bfloat16)
        dv_ref[s] = value_total[:, cols].astype(jnp.bfloat16)


def slopes(queries, keys, values, slope, full, sums, rate, tokens):
    devices, rows, cols = queries.shape
    grid = (cols // tokens, rows // HEAD_DIM)
    piece, sum_spec = attend_specs(devices, tokens)
    return pl.pallas_call(
        slopes_kernel,
        grid=grid,
        out_shape=[jax.ShapeDtypeStruct(queries.shape, jnp.bfloat16)] * 3,
        in_specs=[piece] * 5
        + [sum_spec, pl.BlockSpec((HEAD_DIM, 1), lambda m, h: (0, 0))],
        out_specs=[piece] * 3,
        compiler_params=pltpu.CompilerParams(vmem_limit_bytes=VMEM_BYTES),
        name="slopes",
    )(queries, keys, values, slope, full, sums, rate)


def rms_scale(values):
    return lax.rsqrt(jnp.mean(values * values, axis=-1, keepdims=True) + EPSILON)


def contract(spec, left, right):
    return jnp.einsum(spec, left, right, preferred_element_type=jnp.float32)


def on_device(place, devices, *args):
    inputs, cotangent = args[:2]
    (
        norm_one,
        query_mat,
        query_add,
        key_mat,
        value_mat,
        value_add,
        output_mat,
        output_add,
        norm_two,
        hidden_mat,
        hidden_add,
        project_mat,
        project_add,
    ) = args[2:15]
    depth = args[15].astype(jnp.float32)
    micro, tokens, seqs, width = inputs.shape
    rows = micro * tokens * seqs
    vectors = (norm_one, query_add, value_add, output_add, norm_two, hidden_add, project_add)
    share = norm_one.shape[0]
    small = jnp.pad(jnp.stack(vectors), ((0, 16 - len(vectors)), (0, 128 - share)))
    query_mat, small, key_mat, value_mat, output_mat, hidden_mat, project_mat = move(
        place,
        0,
        gathers=(query_mat, small, key_mat, value_mat, output_mat, hidden_mat, project_mat),
        tails=3,
    )
    small = small.reshape(-1, 16, 128)[:, : len(vectors), :share]
    small = small.transpose(1, 0, 2).reshape(len(vectors), width).astype(jnp.float32)
    gain_one, query_add, value_add, output_add, gain_two, hidden_add, project_add = small
    query_mat, key_mat, value_mat = (
        g.reshape(width, width) for g in (query_mat, key_mat, value_mat)
    )

    def to_rows(array):
        return array.transpose(0, 2, 1, 3).reshape(rows, width)

    def from_rows(array):
        return array.reshape(micro, seqs, tokens, width).transpose(0, 2, 1, 3)

    rate = SOFT_BASE / math.sqrt(HEAD_DIM) * jax.nn.softplus(depth)
    rate_full = jnp.tile(rate, HEADS)[:, None]
    xfloat = to_rows(inputs).astype(jnp.float32)
    inv_one = rms_scale(xfloat)
    normed = (xfloat * inv_one * gain_one).astype(jnp.bfloat16)
    query_pre = contract("df,rd->fr", query_mat, normed) + query_add[:, None]
    queries = (query_pre * rate_full).astype(jnp.bfloat16)
    keys = contract("df,rd->fr", key_mat, normed).astype(jnp.bfloat16)
    values = (contract("df,rd->fr", value_mat, normed) + value_add[:, None]).astype(jnp.bfloat16)

    def split(array):
        return array.reshape(devices, width // devices, rows)

    q_in, k_in, v_in, output_mat, hidden_mat, project_mat = move(
        place,
        1,
        (split(queries), split(keys), split(values)),
        (output_mat, hidden_mat, project_mat),
    )
    output_mat, hidden_mat, project_mat = (
        g.reshape(width, width) for g in (output_mat, hidden_mat, project_mat)
    )
    mixed, full, sums = attend(q_in, k_in, v_in, tokens)
    (mixed,) = move(place, 2, (mixed,))
    mixed = mixed.reshape(width, rows)
    residual = xfloat + (contract("fr,fd->rd", mixed, output_mat) + output_add)
    inv_two = rms_scale(residual)
    second = (residual * inv_two * gain_two).astype(jnp.bfloat16)
    hidden_pre = contract("rd,df->rf", second, hidden_mat) + hidden_add
    active = jax.nn.silu(hidden_pre).astype(jnp.bfloat16)
    result = residual + (contract("rf,fd->rd", active, project_mat) + project_add)
    result = from_rows(result.astype(jnp.bfloat16))

    upper = to_rows(cotangent)
    project_grad = contract("rf,rd->fd", active, upper)
    project_bias_grad = jnp.sum(upper.astype(jnp.float32), axis=0)
    active_grad = contract("rd,fd->rf", upper, project_mat)
    logistic = jax.nn.sigmoid(hidden_pre)
    hidden_grad = (active_grad * logistic * (1.0 + hidden_pre * (1.0 - logistic))).astype(
        jnp.bfloat16
    )
    hidden_mat_grad = contract("rd,rf->df", second, hidden_grad)
    hidden_bias_grad = jnp.sum(hidden_grad.astype(jnp.float32), axis=0)
    second_grad = contract("rf,df->rd", hidden_grad, hidden_mat)
    normal_two = residual * inv_two
    scaled_two = second_grad * gain_two
    norm_two_grad = jnp.sum(second_grad * normal_two, axis=0)
    residual_grad = upper.astype(jnp.float32) + inv_two * (
        scaled_two - normal_two * jnp.mean(scaled_two * normal_two, axis=-1, keepdims=True)
    )
    branch_grad = residual_grad.astype(jnp.bfloat16)
    output_mat_grad = contract("fr,rd->fd", mixed, branch_grad)
    output_bias_grad = jnp.sum(branch_grad.astype(jnp.float32), axis=0)
    mixed_grad = contract("fd,rd->fr", output_mat, branch_grad).astype(jnp.bfloat16)

    def as_parts(*grads):
        return tuple(
            g.astype(jnp.bfloat16).reshape(place.grid() + (share, width)) for g in grads
        )

    merged = share % 8 == 0
    (do_in,) = move(place, 3, (split(mixed_grad),))
    slopes_out = slopes(q_in, k_in, v_in, do_in, full, sums, rate[:, None], tokens)
    early = as_parts(output_mat_grad, hidden_mat_grad, project_grad) if merged else ()
    query_slope, key_grad, value_grad, *early = move(
        place, 4, slopes_out, (), early, held=2 if merged else 0
    )
    query_slope, key_grad, value_grad = (
        a.reshape(width, rows) for a in (query_slope, key_grad, value_grad)
    )
    query_float = query_slope.astype(jnp.float32)
    scale_part = jnp.sum(query_float / rate_full * query_pre, axis=1)
    scale_part = jnp.sum(scale_part.reshape(HEADS, HEAD_DIM), axis=0)
    query_mat_grad = contract("rd,fr->df", normed, query_slope)
    query_bias_grad = jnp.sum(query_float, axis=1)
    key_mat_grad = contract("rd,fr->df", normed, key_grad)
    value_mat_grad = contract("rd,fr->df", normed, value_grad)
    value_bias_grad = jnp.sum(value_grad.astype(jnp.float32), axis=1)
    normed_grad = (
        contract("fr,df->rd", query_slope, query_mat)
        + contract("fr,df->rd", key_grad, key_mat)
        + contract("fr,df->rd", value_grad, value_mat)
    )
    normal_one = xfloat * inv_one
    scaled_one = normed_grad * gain_one
    norm_one_grad = jnp.sum(normed_grad * normal_one, axis=0)
    source_grad = residual_grad + inv_one * (
        scaled_one - normal_one * jnp.mean(scaled_one * normal_one, axis=-1, keepdims=True)
    )
    source_grad = from_rows(source_grad.astype(jnp.bfloat16))

    vector_grads = jnp.stack(
        (
            norm_one_grad,
            query_bias_grad,
            value_bias_grad,
            output_bias_grad,
            norm_two_grad,
            hidden_bias_grad,
            project_bias_grad,
        )
    )
    vector_grads = vector_grads.reshape(7, -1, share).transpose(1, 0, 2)
    vector_grads = jnp.pad(vector_grads, ((0, 0), (0, 0), (0, 128 - share)))
    scale_row = jnp.pad(scale_part, (0, 128 - HEAD_DIM))
    scale_row = jnp.broadcast_to(scale_row, (vector_grads.shape[0], 1, 128))
    vector_grads = jnp.concatenate([vector_grads, scale_row], axis=1)
    vector_grads = vector_grads.reshape(place.grid() + (8, 128))
    late = as_parts(query_mat_grad, key_mat_grad, value_mat_grad)
    if merged:
        output_mat_grad, *early = early
        hidden_mat_grad, project_grad, *late, vector_sums = move(
            place, 5, scatters=(*early, *late, vector_grads)
        )
    else:
        (vector_sums,) = move(place, 5, scatters=(vector_grads,))
        early = as_parts(output_mat_grad, hidden_mat_grad, project_grad)
        early = [move(place, 6, scatters=(p,))[0] for p in early]
        output_mat_grad, hidden_mat_grad, project_grad = early
        late = [move(place, 6, scatters=(p,))[0] for p in late]
    query_mat_grad, key_mat_grad, value_mat_grad = late
    g_one, g_query, g_value, g_output, g_two, g_hidden, g_project = (
        vector_sums[n, :share] for n in range(7)
    )
    scale_summed = vector_sums[7, :HEAD_DIM]
    depth_grad = scale_summed * (SOFT_BASE / math.sqrt(HEAD_DIM)) * jax.nn.sigmoid(depth)
    return (
        result,
        source_grad,
        g_one,
        query_mat_grad,
        g_query,
        key_mat_grad,
        value_mat_grad,
        g_value,
        output_mat_grad,
        g_output,
        g_two,
        hidden_mat_grad,
        g_hidden,
        project_grad,
        g_project,
        depth_grad,
    )


def solution(mesh):
    both = ("dp", "seq")
    token, vector, matrix = P(None, "seq", "dp", None), P(both), P(both, None)
    weights = (
        vector,
        matrix,
        vector,
        matrix,
        matrix,
        vector,
        matrix,
        vector,
        vector,
        matrix,
        vector,
        matrix,
        vector,
    )
    specs = (token, token) + weights + (P(),)
    place = Place(mesh.shape["dp"], mesh.shape["seq"])
    return jax.shard_map(
        functools.partial(on_device, place, mesh.shape["seq"]),
        mesh=mesh,
        in_specs=specs,
        out_specs=specs,
        check_vma=False,
    )
```

```python
import functools
import itertools
import math

import jax
import jax.numpy as jnp
from jax import lax
from jax.experimental import pallas as pl
from jax.experimental.pallas import tpu as pltpu
from jax.sharding import PartitionSpec as P

HEADS = 16
HEAD_DIM = 80
ATT_BLOCK = 256
SOFT_BASE = 1.442695041
EPSILON = 1e-06
MESH = pl.DeviceIdType.MESH
VMEM_BYTES = 60 * 1024 * 1024
LAG = 2


class Place:
    def __init__(self, dp, seq):
        self.cores = 2 if dp % 2 == 0 else 1
        self.lines = dp // self.cores
        self.levels = 4 if seq % 4 == 0 else seq
        self.across = seq // self.levels
        self.sizes = {
            "y": self.lines,
            "c": self.cores,
            "z": self.levels,
            "x": self.across,
        }

    def here(self):
        dp = lax.axis_index("dp")
        seq = lax.axis_index("seq")
        return {
            "y": dp // self.cores,
            "c": dp % self.cores,
            "z": seq // self.across,
            "x": seq % self.across,
        }

    def shift(self, spot, axis, step):
        moved = dict(spot)
        moved[axis] = lax.rem(spot[axis] + step, self.sizes[axis])
        return moved

    def device(self, spot):
        return (
            spot["y"] * self.cores + spot["c"],
            spot["z"] * self.across + spot["x"],
        )

    def grid(self):
        return (self.lines, self.cores, self.levels, self.across)

    def greet(self, spot, wide):
        barrier = pltpu.get_barrier_semaphore()
        dp, seq = self.device(spot)
        peers = [
            self.device(self.shift(spot, axis, step))
            for axis in ("yc" if wide else "zxyc")
            for step in range(1, self.sizes[axis])
        ]
        if wide:
            devices = self.levels * self.across
            peers += [(dp, lax.rem(seq + step, devices)) for step in range(1, devices)]
        for peer in peers:
            pl.semaphore_signal(barrier, inc=1, device_id=peer, device_id_type=MESH)
        pl.semaphore_wait(barrier, len(peers))


def halves_of(cols, lean):
    if lean and cols % 640 == 0:
        cut = cols * 4 // 5
    elif cols % 256 == 0:
        cut = cols // 2
    else:
        return ((slice(0, cols), "xy"),)
    return ((slice(0, cut), "xy"), (slice(cut, cols), "yx"))


def chunks_of(rows, short_last=False):
    if rows % 8 == 0 and rows >= 32:
        cut = rows // 32 * 16
        if short_last:
            cut = rows - cut
        return (slice(0, cut), slice(cut, rows))
    return (slice(0, rows),)


class Sender:
    def __init__(self, place, spot, send_sem, recv_sem):
        self.place = place
        self.spot = spot
        self.send_sem = send_sem
        self.recv_sem = recv_sem
        self.count = itertools.count()
        self.open = {}
        self.every = []

    def put(self, key, device, source, target, leaves=None, comes=None):
        at = next(self.count)
        copy = pltpu.make_async_remote_copy(
            src_ref=source,
            dst_ref=target,
            send_sem=self.send_sem.at[at],
            recv_sem=self.recv_sem.at[at],
            device_id=device,
            device_id_type=MESH,
        )
        self.guard(leaves, copy.start)
        self.open.setdefault(key, []).append((comes, copy))
        self.every.append((leaves, copy))

    def guard(self, when, act):
        if when is None:
            act()
        else:
            pl.when(when)(act)

    def go(self, key, axis, source, target):
        self.open[key] = []
        for step in range(1, self.place.sizes[axis]):
            peer = self.place.shift(self.spot, axis, step)
            self.put(key, self.place.device(peer), source(peer), target(step))

    def chain(self, key, turn, own, slot):
        levels, z = self.place.levels, self.spot["z"]
        self.open[key] = []

        def inside(at):
            return jnp.logical_and(at >= 0, at < levels)

        for way in (1, -1):
            shard, to, back = z - turn * way, z + way, z - (turn + 1) * way
            part = slot(lax.rem(shard + levels, levels))
            peer = dict(self.spot, z=lax.rem(to + levels, levels))
            self.put(
                key,
                self.place.device(peer),
                own if turn == 0 else part,
                part,
                jnp.logical_and(inside(shard), inside(to)),
                inside(back),
            )

    def landed(self, key):
        for comes, copy in self.open[key]:
            self.guard(comes, copy.wait_recv)

    def finish(self):
        for leaves, copy in self.every:
            self.guard(leaves, copy.wait_send)


class Gather:
    def __init__(self, place, spot, lean, tails, shards, wholes, own_sem):
        self.place, self.spot, self.lean, self.tails = place, spot, lean, tails
        self.shards, self.wholes = shards, wholes
        y, c, z, x = (spot[k] for k in "yczx")
        self.own = []
        for n, shard in enumerate(shards):
            if n >= len(shards) - tails:
                target = wholes[n].at[z]
            elif len(shard.shape) == 3:
                target = wholes[n].at[y, c, :, x]
            else:
                target = wholes[n].at[y, c, z, x]
            copy = pltpu.make_async_copy(shard, target, own_sem[n])
            copy.start()
            self.own.append(copy)

    def run(self, out, feed):
        shards, wholes = self.shards, self.wholes
        y, c, _, x = (self.spot[k] for k in "yczx")
        turns = self.place.levels - 1
        full = len(shards) - self.tails
        raw = [n for n, s in enumerate(shards) if len(s.shape) == 2]
        jobs = [(n, r) for n in range(full) for r in chunks_of(shards[n].shape[-2], True)]
        filled = set()

        def halves(n):
            return enumerate(halves_of(shards[n].shape[-1], self.lean))

        def along(turn, n):
            def slot(level):
                return wholes[n].at[y, c, level, x] if n < full else wholes[n].at[level]

            if turn > 0:
                out.landed(("z", n, turn - 1))
            if turn < turns:
                out.chain(("z", n, turn), turn, shards[n], slot)

        def fill(n):
            if n not in filled:
                filled.add(n)
                self.own[n].wait()

        def two(job, n, rows):
            lined = len(shards[n].shape) == 3
            if not lined:
                fill(n)
            for half, (cols, order) in halves(n):
                part = wholes[n].at[y, c, :, x, rows, cols]
                source = shards[n].at[:, rows, cols] if lined else part
                out.go((job, half, 2), order[0], lambda peer: source, lambda step: part)

        def three(job, n, rows):
            fill(n)
            for half, (cols, order) in halves(n):
                out.landed((job, half, 2))
                if order == "xy":
                    part = wholes[n].at[y, c, :, :, rows, cols]
                else:
                    part = wholes[n].at[:, c, :, x, rows, cols]
                out.go((job, half, 3), order[1], lambda peer: part, lambda step: part)

        def four(job, n, rows):
            for half, (cols, order) in halves(n):
                out.landed((job, half, 3))
                part = wholes[n].at[:, c, :, :, rows, cols]
                out.go((job, half, 4), "c", lambda peer: part, lambda step: part)

        def five(job, n, rows):
            for half, _ in halves(n):
                out.landed((job, half, 4))

        steps = iter(range(len(jobs) + 3 * LAG))

        def advance():
            step = next(steps, None)
            if step is not None:
                for stage, late in ((two, 0), (three, LAG), (four, 2 * LAG), (five, 3 * LAG)):
                    if 0 <= step - late < len(jobs):
                        stage(("gather", step - late), *jobs[step - late])

        if raw:
            for time in range(len(raw) + turns):
                for turn in range(turns + 1):
                    if 0 <= time - turn < len(raw):
                        along(turn, raw[time - turn])
                done = time - turns
                if 0 <= done < full:
                    for _ in chunks_of(shards[raw[done]].shape[-2]):
                        advance()
        for _ in range(len(jobs) + 3 * LAG):
            advance()
            feed()
        for n in range(len(shards)):
            fill(n)


def total(values):
    result = values[0].astype(jnp.float32)
    for value in values[1:]:
        result = result + value.astype(jnp.float32)
    return result


class Scatter:
    def __init__(self, place, spot, lean, held, parts, totals, boxes, own_sem):
        self.place, self.spot, self.lean = place, spot, lean
        self.parts, self.totals = parts, totals
        self.full = len(parts) - held
        self.jobs = [
            (n, r)
            for n, p in enumerate(parts)
            if len(p.shape) > 3
            for r in chunks_of(p.shape[-2])
        ]
        self.own_sem = own_sem
        self.sums, self.cores, self.seconds, self.thirds, self.fourths = [], [], [], [], []
        self.results, self.own = [], []
        for n, part in enumerate(parts):
            self.sums.append(boxes.pop(0))
            if len(part.shape) > 3:
                self.cores.append(boxes.pop(0))
                halves = halves_of(part.shape[-1], lean)
                self.seconds.append([boxes.pop(0) for _ in halves])
                self.thirds.append([boxes.pop(0) for _ in halves])
                mine = part.at[:, spot["c"]]
            else:
                for boxed in (self.cores, self.seconds, self.thirds):
                    boxed.append(None)
                mine = part.at[spot["z"]]
            if n < self.full:
                self.fourths.append(boxes.pop(0))
                self.results.append(boxes.pop(0))
            else:
                self.fourths.append(None)
                self.results.append(self.sums[n].at[spot["y"], :, spot["x"]])
            copy = pltpu.make_async_copy(mine, self.sums[n], own_sem[n])
            copy.start()
            self.own.append(copy)

    def run(self, out, feed):
        place, parts, sums = self.place, self.parts, self.sums
        cores, results = self.cores, self.results
        y, c, z, x = (self.spot[k] for k in "yczx")
        lines, _, levels, across = place.grid()
        filled = set()

        def halves(n):
            return enumerate(halves_of(parts[n].shape[-1], self.lean))

        def one(job, n, rows):
            out.go(
                (job, 1),
                "c",
                lambda peer: parts[n].at[:, peer["c"], :, :, rows],
                lambda step: cores[n].at[:, :, :, rows],
            )

        def two(job, n, rows):
            if n not in filled:
                filled.add(n)
                self.own[n].wait()
            out.landed((job, 1))
            if place.cores > 1:

                @pl.loop(0, lines * levels * across)
                def _(at):
                    where = (at // (levels * across), (at // across) % levels, at % across)
                    sums[n][where + (rows,)] = total(
                        [sums[n][where + (rows,)], cores[n][where + (rows,)]]
                    ).astype(sums[n].dtype)

            for half, (cols, order) in halves(n):
                box = self.seconds[n][half]
                if order == "xy":
                    out.go(
                        (job, half, 2),
                        "y",
                        lambda peer: sums[n].at[peer["y"], :, :, rows, cols],
                        lambda step: box.at[step - 1, :, :, rows],
                    )
                else:
                    out.go(
                        (job, half, 2),
                        "x",
                        lambda peer: sums[n].at[:, :, peer["x"], rows, cols],
                        lambda step: box.at[step - 1, :, :, rows],
                    )

        def three(job, n, rows):
            for half, (cols, order) in halves(n):
                out.landed((job, half, 2))
                box, later = self.seconds[n][half], self.thirds[n][half]
                if order == "xy":

                    @pl.loop(0, levels * across)
                    def _(at):
                        zz, xx = at // across, at % across
                        values = [sums[n][y, zz, xx, rows, cols]]
                        values += [box[k, zz, xx, rows] for k in range(lines - 1)]
                        sums[n][y, zz, xx, rows, cols] = total(values).astype(sums[n].dtype)

                    out.go(
                        (job, half, 3),
                        "x",
                        lambda peer: sums[n].at[y, :, peer["x"], rows, cols],
                        lambda step: later.at[step - 1, :, rows],
                    )
                else:

                    @pl.loop(0, lines * levels)
                    def _(at):
                        yy, zz = at // levels, at % levels
                        values = [sums[n][yy, zz, x, rows, cols]]
                        values += [box[k, yy, zz, rows] for k in range(across - 1)]
                        sums[n][yy, zz, x, rows, cols] = total(values).astype(sums[n].dtype)

                    out.go(
                        (job, half, 3),
                        "y",
                        lambda peer: sums[n].at[peer["y"], :, x, rows, cols],
                        lambda step: later.at[step - 1, :, rows],
                    )

        def four(job, n, rows):
            for half, (cols, order) in halves(n):
                out.landed((job, half, 3))
                box = self.thirds[n][half]

                @pl.loop(0, levels)
                def _(zz):
                    values = [sums[n][y, zz, x, rows, cols]]
                    values += [box[k, zz, rows] for k in range(box.shape[0])]
                    sums[n][y, zz, x, rows, cols] = total(values).astype(sums[n].dtype)

            if n < self.full:
                out.go(
                    (job, 4),
                    "z",
                    lambda peer: sums[n].at[y, peer["z"], x, rows],
                    lambda step: self.fourths[n].at[step - 1, rows],
                )

        def five(job, n, rows):
            if n >= self.full:
                return
            out.landed((job, 4))
            values = [sums[n][y, z, x, rows]]
            values += [self.fourths[n][k, rows] for k in range(levels - 1)]
            results[n][rows] = total(values)

        def first(n):
            out.go(
                ("tail", n),
                "z",
                lambda peer: parts[n].at[peer["z"]],
                lambda step: self.fourths[n].at[step - 1],
            )

        def final(n):
            self.own[n].wait()
            out.landed(("tail", n))
            values = [sums[n][...]] + [self.fourths[n][k] for k in range(levels - 1)]
            results[n][...] = total(values)

        jobs = [(("scatter", at),) + job for at, job in enumerate(self.jobs)]
        tails = [n for n, p in enumerate(parts) if len(p.shape) == 3]
        for n in tails:
            first(n)
        lag = LAG if self.lean else 1
        for step in range(len(jobs) + 4 * lag):
            if step > 2 and tails:
                final(tails.pop(0))
            for turn, stage in enumerate((one, two, three, four, five)):
                late = turn * lag
                if 0 <= step - late < len(jobs):
                    stage(*jobs[step - late])
            feed()
        last = []
        for n, result in enumerate(results):
            copy = pltpu.make_async_copy(result, self.totals[n], self.own_sem[n])
            copy.start()
            last.append(copy)
        for copy in last:
            copy.wait()


def scatter_boxes(place, part, lean, held):
    lines, _, levels, across = place.grid()
    rows, cols = part.shape[-2:]
    final = [
        pltpu.VMEM((levels - 1, rows, cols), part.dtype),
        pltpu.VMEM((rows, cols), jnp.float32),
    ]
    if part.ndim == 3:
        return [pltpu.VMEM((rows, cols), part.dtype)] + final
    block = pltpu.VMEM((lines, levels, across, rows, cols), part.dtype)
    first, later = [], []
    for piece, order in halves_of(cols, lean):
        size = (rows, piece.stop - piece.start)
        steps = (lines - 1, across - 1) if order == "xy" else (across - 1, lines - 1)
        middle = (levels, across) if order == "xy" else (lines, levels)
        first.append(pltpu.VMEM((steps[0],) + middle + size, part.dtype))
        later.append(pltpu.VMEM((steps[1], levels) + size, part.dtype))
    return [block, block] + first + later + ([] if held else final)


def move_kernel(place, counts, lean, tails, held, *refs):
    refs = list(refs)
    swaps, gathers, scatters = counts
    whole = swaps + gathers + scatters
    ins, outs, rest = refs[:whole], refs[whole : 2 * whole], refs[2 * whole :]
    own_sem, send_sem, recv_sem = rest[-3:]
    staged = swaps > 0 and whole > swaps
    relays, boxes = rest[: swaps * staged], rest[swaps * staged : -3]
    spot = place.here()
    dp, me = place.device(spot)
    devices = place.levels * place.across
    sent, got = ins[:swaps], outs[:swaps]
    own = []
    for n in range(swaps):
        copy = pltpu.make_async_copy(sent[n].at[me], got[n].at[me], own_sem.at[n])
        copy.start()
        own.append(copy)
    cut = swaps + gathers
    gather = Gather(
        place, spot, lean, tails, ins[swaps:cut], outs[swaps:cut], [own_sem.at[n] for n in range(swaps, cut)]
    )
    scatter = Scatter(
        place, spot, lean, held, ins[cut:], outs[cut:], boxes, [own_sem.at[n] for n in range(cut, whole)]
    )
    place.greet(spot, swaps > 0 and not staged)
    out = Sender(place, spot, send_sem, recv_sem)
    levels, across = place.levels, place.across
    z, x = spot["z"], spot["x"]

    def straight(n):
        for step in range(1, devices):
            peer = lax.rem(me + step, devices)
            out.put("swap", (dp, peer), sent[n].at[peer], got[n].at[me])

    def along_x(n):
        for skip in range(1, across):
            peer = place.shift(spot, "x", skip)
            device = place.device(peer)
            out.put("swap", device, sent[n].at[device[1]], got[n].at[me])
            for step in range(1, levels):
                piece = place.device(place.shift(peer, "z", step))[1]
                out.put(
                    ("relay", n), device, sent[n].at[piece], relays[n].at[skip - 1, step - 1]
                )

    def along_z(n):
        for step in range(1, levels):
            device = place.device(place.shift(spot, "z", step))
            out.put("swap", device, sent[n].at[device[1]], got[n].at[me])

    def pass_on(n):
        out.landed(("relay", n))
        for skip in range(1, across):
            source = place.device(place.shift(spot, "x", across - skip))[1]
            for step in range(1, levels):
                device = place.device(place.shift(spot, "z", step))
                out.put("swap", device, relays[n].at[skip - 1, step - 1], got[n].at[source])

    if staged:
        apart = 2 if gathers else 1
        pending = [[] for _ in range(apart * (swaps - 1) + LAG + 2)]
        for n in range(swaps):
            pending[0 if gathers else max(n - 1, 0)].append((along_z, n))
        for n in range(swaps):
            pending[apart * n].append((along_x, n))
            pending[apart * n + LAG + 1].append((pass_on, n))
    else:
        pending = [[(straight, n)] for n in range(swaps)]

    def feed():
        for act, n in pending.pop(0) if pending else ():
            act(n)

    if gathers:
        gather.run(out, feed)
    if scatters:
        scatter.run(out, feed)
    while pending:
        feed()
    for copy in own:
        copy.wait()
    if swaps:
        out.landed("swap")
    out.finish()


def move(place, collective_id, swaps=(), gathers=(), scatters=(), tails=0, held=0):
    lean = len(swaps) > 0
    lines, cores, levels, across = place.grid()
    copies = len(swaps) * (2 * levels * across - across - 1)
    boxes = []
    if len(swaps) > 0 and len(gathers) + len(scatters) > 0:
        boxes += [pltpu.VMEM((across - 1, levels - 1) + a.shape[1:], a.dtype) for a in swaps]
    shapes = [jax.ShapeDtypeStruct(a.shape, a.dtype) for a in swaps]
    for n, shard in enumerate(gathers):
        rows, cols = shard.shape[-2:]
        if shard.ndim == 2:
            copies += 2 * (levels - 1)
        grid = place.grid()
        if n < len(gathers) - tails:
            count = len(halves_of(cols, lean)) * (across + lines + cores - 3)
            copies += len(chunks_of(rows)) * count
        else:
            grid = (levels,)
        shapes.append(jax.ShapeDtypeStruct(grid + (rows, cols), shard.dtype))
    for n, part in enumerate(scatters):
        rows, cols = part.shape[-2:]
        keeps = n >= len(scatters) - held
        count = 0 if keeps else levels - 1
        if part.ndim > 3:
            count += (cores - 1) + len(halves_of(cols, lean)) * (lines + across - 2)
            count *= len(chunks_of(rows))
        copies += count
        boxes += scatter_boxes(place, part, lean, keeps)
        shapes.append(
            jax.ShapeDtypeStruct((levels, rows, cols), part.dtype)
            if keeps
            else jax.ShapeDtypeStruct((rows, cols), jnp.float32)
        )

    def is_result(a):
        return a.dtype == jnp.float32 and a.shape[-1] > 128

    return pl.pallas_call(
        functools.partial(
            move_kernel, place, (len(swaps), len(gathers), len(scatters)), lean, tails, held
        ),
        out_shape=shapes,
        in_specs=[pl.BlockSpec(memory_space=pl.ANY)] * len(shapes),
        out_specs=[
            pl.BlockSpec(memory_space=pltpu.HBM if is_result(a) else pl.ANY)
            for a in shapes
        ],
        scratch_shapes=boxes
        + [
            pltpu.SemaphoreType.DMA((len(shapes),)),
            pltpu.SemaphoreType.DMA((copies,)),
            pltpu.SemaphoreType.DMA((copies,)),
        ],
        compiler_params=pltpu.CompilerParams(
            collective_id=collective_id,
            has_side_effects=True,
            vmem_limit_bytes=VMEM_BYTES,
        ),
        name=f"move_{collective_id}",
    )(*swaps, *gathers, *scatters)


def side_by_side(ref):
    return jnp.concatenate([ref[s] for s in range(ref.shape[0])], axis=1)


def dot_first(left, right):
    return lax.dot_general(
        left, right, (((0,), (0,)), ((), ())), preferred_element_type=jnp.float32
    )


def dot_last(left, right):
    return lax.dot_general(
        left, right, (((1,), (1,)), ((), ())), preferred_element_type=jnp.float32
    )


def attend_kernel(q_ref, k_ref, v_ref, o_ref, full_ref, sum_ref):
    tokens = q_ref.shape[-1]
    each = ATT_BLOCK // tokens
    keys, values = side_by_side(k_ref), side_by_side(v_ref)
    for block in range(q_ref.shape[0] // each):
        first = block * each
        limit = (block + 1) * ATT_BLOCK
        queries = jnp.concatenate([q_ref[first + s] for s in range(each)], axis=1)
        weights = jnp.exp(dot_first(keys[:, :limit], queries))
        sums = jnp.sum(weights, axis=0, keepdims=True)
        mixed = jnp.dot(
            values[:, :limit],
            weights.astype(jnp.bfloat16),
            preferred_element_type=jnp.float32,
        )
        mixed = mixed / sums
        sum_ref[0, 0, :, pl.ds(block * ATT_BLOCK, ATT_BLOCK)] = sums
        for s in range(each):
            piece = mixed[:, s * tokens : (s + 1) * tokens]
            full_ref[first + s] = piece
            o_ref[first + s] = piece.astype(jnp.bfloat16)


def attend_specs(devices, tokens):
    piece = pl.BlockSpec((devices, HEAD_DIM, tokens), lambda m, h: (0, h, m))
    sums = pl.BlockSpec((1, 1, 1, devices * tokens), lambda m, h: (m, h, 0, 0))
    return piece, sums


def attend(queries, keys, values, tokens):
    devices, rows, cols = queries.shape
    grid = (cols // tokens, rows // HEAD_DIM)
    piece, sums = attend_specs(devices, tokens)
    return pl.pallas_call(
        attend_kernel,
        grid=grid,
        out_shape=[
            jax.ShapeDtypeStruct(queries.shape, jnp.bfloat16),
            jax.ShapeDtypeStruct(queries.shape, jnp.float32),
            jax.ShapeDtypeStruct(grid + (1, devices * tokens), jnp.float32),
        ],
        in_specs=[piece] * 3,
        out_specs=[piece, piece, sums],
        compiler_params=pltpu.CompilerParams(vmem_limit_bytes=VMEM_BYTES),
        name="attend",
    )(queries, keys, values)


def slopes_kernel(
    q_ref, k_ref, v_ref, do_ref, full_ref, sum_ref, rate_ref, dq_ref, dk_ref, dv_ref
):
    tokens = q_ref.shape[-1]
    each = ATT_BLOCK // tokens
    keys, values = side_by_side(k_ref), side_by_side(v_ref)
    rate = rate_ref[...]
    key_total = value_total = None
    for block in reversed(range(q_ref.shape[0] // each)):
        first = block * each
        limit = (block + 1) * ATT_BLOCK

        def pick(ref):
            return jnp.concatenate([ref[first + s] for s in range(each)], axis=1)

        queries = pick(q_ref)
        slope = pick(do_ref).astype(jnp.float32)
        sums = sum_ref[0, 0, :, pl.ds(block * ATT_BLOCK, ATT_BLOCK)]
        scaled = (slope / sums).astype(jnp.bfloat16)
        centre = jnp.sum(slope * pick(full_ref), axis=0, keepdims=True) / sums
        weights = jnp.exp(dot_first(keys[:, :limit], queries))
        dots = dot_first(values[:, :limit], scaled)
        slopes = (weights * (dots - centre)).astype(jnp.bfloat16)
        weights = weights.astype(jnp.bfloat16)
        query_part = jnp.dot(keys[:, :limit], slopes, preferred_element_type=jnp.float32)
        query_part = (query_part * rate).astype(jnp.bfloat16)
        for s in range(each):
            dq_ref[first + s] = query_part[:, s * tokens : (s + 1) * tokens]
        key_part = dot_last(queries, slopes)
        value_part = dot_last(scaled, weights)
        if key_total is None:
            key_total, value_total = key_part, value_part
        else:
            key_total = jnp.concatenate(
                [key_total[:, :limit] + key_part, key_total[:, limit:]], axis=1
            )
            value_total = jnp.concatenate(
                [value_total[:, :limit] + value_part, value_total[:, limit:]], axis=1
            )
    for s in range(q_ref.shape[0]):
        cols = slice(s * tokens, (s + 1) * tokens)
        dk_ref[s] = key_total[:, cols].astype(jnp.bfloat16)
        dv_ref[s] = value_total[:, cols].astype(jnp.bfloat16)


def slopes(queries, keys, values, slope, full, sums, rate, tokens):
    devices, rows, cols = queries.shape
    grid = (cols // tokens, rows // HEAD_DIM)
    piece, sum_spec = attend_specs(devices, tokens)
    return pl.pallas_call(
        slopes_kernel,
        grid=grid,
        out_shape=[jax.ShapeDtypeStruct(queries.shape, jnp.bfloat16)] * 3,
        in_specs=[piece] * 5
        + [sum_spec, pl.BlockSpec((HEAD_DIM, 1), lambda m, h: (0, 0))],
        out_specs=[piece] * 3,
        compiler_params=pltpu.CompilerParams(vmem_limit_bytes=VMEM_BYTES),
        name="slopes",
    )(queries, keys, values, slope, full, sums, rate)


def rms_scale(values):
    return lax.rsqrt(jnp.mean(values * values, axis=-1, keepdims=True) + EPSILON)


def contract(spec, left, right):
    return jnp.einsum(spec, left, right, preferred_element_type=jnp.float32)


def on_device(place, devices, *args):
    inputs, cotangent = args[:2]
    (
        norm_one,
        query_mat,
        query_add,
        key_mat,
        value_mat,
        value_add,
        output_mat,
        output_add,
        norm_two,
        hidden_mat,
        hidden_add,
        project_mat,
        project_add,
    ) = args[2:15]
    depth = args[15].astype(jnp.float32)
    micro, tokens, seqs, width = inputs.shape
    rows = micro * tokens * seqs
    vectors = (norm_one, query_add, value_add, output_add, norm_two, hidden_add, project_add)
    share = norm_one.shape[0]
    small = jnp.pad(jnp.stack(vectors), ((0, 16 - len(vectors)), (0, 128 - share)))
    query_mat, small, key_mat, value_mat, output_mat, hidden_mat, project_mat = move(
        place,
        0,
        gathers=(query_mat, small, key_mat, value_mat, output_mat, hidden_mat, project_mat),
        tails=3,
    )
    small = small.reshape(-1, 16, 128)[:, : len(vectors), :share]
    small = small.transpose(1, 0, 2).reshape(len(vectors), width).astype(jnp.float32)
    gain_one, query_add, value_add, output_add, gain_two, hidden_add, project_add = small
    query_mat, key_mat, value_mat = (
        g.reshape(width, width) for g in (query_mat, key_mat, value_mat)
    )

    def to_rows(array):
        return array.transpose(0, 2, 1, 3).reshape(rows, width)

    def from_rows(array):
        return array.reshape(micro, seqs, tokens, width).transpose(0, 2, 1, 3)

    rate = SOFT_BASE / math.sqrt(HEAD_DIM) * jax.nn.softplus(depth)
    rate_full = jnp.tile(rate, HEADS)[:, None]
    xfloat = to_rows(inputs).astype(jnp.float32)
    inv_one = rms_scale(xfloat)
    normed = (xfloat * inv_one * gain_one).astype(jnp.bfloat16)
    query_pre = contract("df,rd->fr", query_mat, normed) + query_add[:, None]
    queries = (query_pre * rate_full).astype(jnp.bfloat16)
    keys = contract("df,rd->fr", key_mat, normed).astype(jnp.bfloat16)
    values = (contract("df,rd->fr", value_mat, normed) + value_add[:, None]).astype(jnp.bfloat16)

    def split(array):
        return array.reshape(devices, width // devices, rows)

    q_in, k_in, v_in, output_mat, hidden_mat, project_mat = move(
        place,
        1,
        (split(queries), split(keys), split(values)),
        (output_mat, hidden_mat, project_mat),
    )
    output_mat, hidden_mat, project_mat = (
        g.reshape(width, width) for g in (output_mat, hidden_mat, project_mat)
    )
    mixed, full, sums = attend(q_in, k_in, v_in, tokens)
    (mixed,) = move(place, 2, (mixed,))
    mixed = mixed.reshape(width, rows)
    residual = xfloat + (contract("fr,fd->rd", mixed, output_mat) + output_add)
    inv_two = rms_scale(residual)
    second = (residual * inv_two * gain_two).astype(jnp.bfloat16)
    hidden_pre = contract("rd,df->rf", second, hidden_mat) + hidden_add
    active = jax.nn.silu(hidden_pre).astype(jnp.bfloat16)
    result = residual + (contract("rf,fd->rd", active, project_mat) + project_add)
    result = from_rows(result.astype(jnp.bfloat16))

    upper = to_rows(cotangent)
    project_grad = contract("rf,rd->fd", active, upper)
    project_bias_grad = jnp.sum(upper.astype(jnp.float32), axis=0)
    active_grad = contract("rd,fd->rf", upper, project_mat)
    logistic = jax.nn.sigmoid(hidden_pre)
    hidden_grad = (active_grad * logistic * (1.0 + hidden_pre * (1.0 - logistic))).astype(
        jnp.bfloat16
    )
    hidden_mat_grad = contract("rd,rf->df", second, hidden_grad)
    hidden_bias_grad = jnp.sum(hidden_grad.astype(jnp.float32), axis=0)
    second_grad = contract("rf,df->rd", hidden_grad, hidden_mat)
    normal_two = residual * inv_two
    scaled_two = second_grad * gain_two
    norm_two_grad = jnp.sum(second_grad * normal_two, axis=0)
    residual_grad = upper.astype(jnp.float32) + inv_two * (
        scaled_two - normal_two * jnp.mean(scaled_two * normal_two, axis=-1, keepdims=True)
    )
    branch_grad = residual_grad.astype(jnp.bfloat16)
    output_mat_grad = contract("fr,rd->fd", mixed, branch_grad)
    output_bias_grad = jnp.sum(branch_grad.astype(jnp.float32), axis=0)
    mixed_grad = contract("fd,rd->fr", output_mat, branch_grad).astype(jnp.bfloat16)

    def as_parts(*grads):
        return tuple(
            g.astype(jnp.bfloat16).reshape(place.grid() + (share, width)) for g in grads
        )

    merged = share % 8 == 0
    (do_in,) = move(place, 3, (split(mixed_grad),))
    slopes_out = slopes(q_in, k_in, v_in, do_in, full, sums, rate[:, None], tokens)
    early = as_parts(output_mat_grad, hidden_mat_grad, project_grad) if merged else ()
    query_slope, key_grad, value_grad, *early = move(
        place, 4, slopes_out, (), early, held=2 if merged else 0
    )
    query_slope, key_grad, value_grad = (
        a.reshape(width, rows) for a in (query_slope, key_grad, value_grad)
    )
    query_float = query_slope.astype(jnp.float32)
    scale_part = jnp.sum(query_float / rate_full * query_pre, axis=1)
    scale_part = jnp.sum(scale_part.reshape(HEADS, HEAD_DIM), axis=0)
    query_mat_grad = contract("rd,fr->df", normed, query_slope)
    query_bias_grad = jnp.sum(query_float, axis=1)
    key_mat_grad = contract("rd,fr->df", normed, key_grad)
    value_mat_grad = contract("rd,fr->df", normed, value_grad)
    value_bias_grad = jnp.sum(value_grad.astype(jnp.float32), axis=1)
    normed_grad = (
        contract("fr,df->rd", query_slope, query_mat)
        + contract("fr,df->rd", key_grad, key_mat)
        + contract("fr,df->rd", value_grad, value_mat)
    )
    normal_one = xfloat * inv_one
    scaled_one = normed_grad * gain_one
    norm_one_grad = jnp.sum(normed_grad * normal_one, axis=0)
    source_grad = residual_grad + inv_one * (
        scaled_one - normal_one * jnp.mean(scaled_one * normal_one, axis=-1, keepdims=True)
    )
    source_grad = from_rows(source_grad.astype(jnp.bfloat16))

    vector_grads = jnp.stack(
        (
            norm_one_grad,
            query_bias_grad,
            value_bias_grad,
            output_bias_grad,
            norm_two_grad,
            hidden_bias_grad,
            project_bias_grad,
        )
    )
    vector_grads = vector_grads.reshape(7, -1, share).transpose(1, 0, 2)
    vector_grads = jnp.pad(vector_grads, ((0, 0), (0, 0), (0, 128 - share)))
    scale_row = jnp.pad(scale_part, (0, 128 - HEAD_DIM))
    scale_row = jnp.broadcast_to(scale_row, (vector_grads.shape[0], 1, 128))
    vector_grads = jnp.concatenate([vector_grads, scale_row], axis=1)
    vector_grads = vector_grads.reshape(place.grid() + (8, 128))
    late = as_parts(query_mat_grad, key_mat_grad, value_mat_grad)
    if merged:
        output_mat_grad, *early = early
        hidden_mat_grad, project_grad, *late, vector_sums = move(
            place, 5, scatters=(*early, *late, vector_grads)
        )
    else:
        (vector_sums,) = move(place, 5, scatters=(vector_grads,))
        early = as_parts(output_mat_grad, hidden_mat_grad, project_grad)
        early = [move(place, 6, scatters=(p,))[0] for p in early]
        output_mat_grad, hidden_mat_grad, project_grad = early
        late = [move(place, 6, scatters=(p,))[0] for p in late]
    query_mat_grad, key_mat_grad, value_mat_grad = late
    g_one, g_query, g_value, g_output, g_two, g_hidden, g_project = (
        vector_sums[n, :share] for n in range(7)
    )
    scale_summed = vector_sums[7, :HEAD_DIM]
    depth_grad = scale_summed * (SOFT_BASE / math.sqrt(HEAD_DIM)) * jax.nn.sigmoid(depth)
    return (
        result,
        source_grad,
        g_one,
        query_mat_grad,
        g_query,
        key_mat_grad,
        value_mat_grad,
        g_value,
        output_mat_grad,
        g_output,
        g_two,
        hidden_mat_grad,
        g_hidden,
        project_grad,
        g_project,
        depth_grad,
    )


def solution(mesh):
    both = ("dp", "seq")
    token, vector, matrix = P(None, "seq", "dp", None), P(both), P(both, None)
    weights = (
        vector,
        matrix,
        vector,
        matrix,
        matrix,
        vector,
        matrix,
        vector,
        vector,
        matrix,
        vector,
        matrix,
        vector,
    )
    specs = (token, token) + weights + (P(),)
    place = Place(mesh.shape["dp"], mesh.shape["seq"])
    return jax.shard_map(
        functools.partial(on_device, place, mesh.shape["seq"]),
        mesh=mesh,
        in_specs=specs,
        out_specs=specs,
        check_vma=False,
    )
```

```python
import functools
import itertools
import math

import jax
import jax.numpy as jnp
from jax import lax
from jax.experimental import pallas as pl
from jax.experimental.pallas import tpu as pltpu
from jax.sharding import PartitionSpec as P

HEADS = 16
HEAD_DIM = 80
ATT_BLOCK = 256
SOFT_BASE = 1.442695041
EPSILON = 1e-06
MESH = pl.DeviceIdType.MESH
VMEM_BYTES = 60 * 1024 * 1024
LAG = 2


class Place:
    def __init__(self, dp, seq):
        self.cores = 2 if dp % 2 == 0 else 1
        self.lines = dp // self.cores
        self.levels = 4 if seq % 4 == 0 else seq
        self.across = seq // self.levels
        self.sizes = {
            "y": self.lines,
            "c": self.cores,
            "z": self.levels,
            "x": self.across,
        }

    def here(self):
        dp = lax.axis_index("dp")
        seq = lax.axis_index("seq")
        return {
            "y": dp // self.cores,
            "c": dp % self.cores,
            "z": seq // self.across,
            "x": seq % self.across,
        }

    def shift(self, spot, axis, step):
        moved = dict(spot)
        moved[axis] = lax.rem(spot[axis] + step, self.sizes[axis])
        return moved

    def device(self, spot):
        return (
            spot["y"] * self.cores + spot["c"],
            spot["z"] * self.across + spot["x"],
        )

    def grid(self):
        return (self.lines, self.cores, self.levels, self.across)

    def greet(self, spot, wide):
        barrier = pltpu.get_barrier_semaphore()
        dp, seq = self.device(spot)
        peers = [
            self.device(self.shift(spot, axis, step))
            for axis in ("yc" if wide else "zxyc")
            for step in range(1, self.sizes[axis])
        ]
        if wide:
            devices = self.levels * self.across
            peers += [(dp, lax.rem(seq + step, devices)) for step in range(1, devices)]
        for peer in peers:
            pl.semaphore_signal(barrier, inc=1, device_id=peer, device_id_type=MESH)
        pl.semaphore_wait(barrier, len(peers))


def halves_of(cols, lean):
    if lean and cols % 640 == 0:
        cut = cols * 4 // 5
    elif cols % 256 == 0:
        cut = cols // 2
    else:
        return ((slice(0, cols), "xy"),)
    return ((slice(0, cut), "xy"), (slice(cut, cols), "yx"))


def chunks_of(rows, short_last=False):
    if rows % 8 == 0 and rows >= 32:
        cut = rows // 32 * 16
        if short_last:
            cut = rows - cut
        return (slice(0, cut), slice(cut, rows))
    return (slice(0, rows),)


class Sender:
    def __init__(self, place, spot, send_sem, recv_sem):
        self.place = place
        self.spot = spot
        self.send_sem = send_sem
        self.recv_sem = recv_sem
        self.count = itertools.count()
        self.open = {}
        self.every = []

    def put(self, key, device, source, target, leaves=None, comes=None):
        at = next(self.count)
        copy = pltpu.make_async_remote_copy(
            src_ref=source,
            dst_ref=target,
            send_sem=self.send_sem.at[at],
            recv_sem=self.recv_sem.at[at],
            device_id=device,
            device_id_type=MESH,
        )
        self.guard(leaves, copy.start)
        self.open.setdefault(key, []).append((comes, copy))
        self.every.append((leaves, copy))

    def guard(self, when, act):
        if when is None:
            act()
        else:
            pl.when(when)(act)

    def go(self, key, axis, source, target):
        self.open[key] = []
        for step in range(1, self.place.sizes[axis]):
            peer = self.place.shift(self.spot, axis, step)
            self.put(key, self.place.device(peer), source(peer), target(step))

    def chain(self, key, turn, own, slot):
        levels, z = self.place.levels, self.spot["z"]
        self.open[key] = []

        def inside(at):
            return jnp.logical_and(at >= 0, at < levels)

        for way in (1, -1):
            shard, to, back = z - turn * way, z + way, z - (turn + 1) * way
            part = slot(lax.rem(shard + levels, levels))
            peer = dict(self.spot, z=lax.rem(to + levels, levels))
            self.put(
                key,
                self.place.device(peer),
                own if turn == 0 else part,
                part,
                jnp.logical_and(inside(shard), inside(to)),
                inside(back),
            )

    def landed(self, key):
        for comes, copy in self.open[key]:
            self.guard(comes, copy.wait_recv)

    def finish(self):
        for leaves, copy in self.every:
            self.guard(leaves, copy.wait_send)


class Gather:
    def __init__(self, place, spot, lean, tails, shards, wholes, own_sem):
        self.place, self.spot, self.lean, self.tails = place, spot, lean, tails
        self.shards, self.wholes = shards, wholes
        y, c, z, x = (spot[k] for k in "yczx")
        self.own = []
        for n, shard in enumerate(shards):
            if n >= len(shards) - tails:
                target = wholes[n].at[z]
            elif len(shard.shape) == 3:
                target = wholes[n].at[y, c, :, x]
            else:
                target = wholes[n].at[y, c, z, x]
            copy = pltpu.make_async_copy(shard, target, own_sem[n])
            copy.start()
            self.own.append(copy)

    def run(self, out, feed):
        shards, wholes = self.shards, self.wholes
        y, c, _, x = (self.spot[k] for k in "yczx")
        turns = self.place.levels - 1
        full = len(shards) - self.tails
        raw = [n for n, s in enumerate(shards) if len(s.shape) == 2]
        jobs = [(n, r) for n in range(full) for r in chunks_of(shards[n].shape[-2], True)]
        filled = set()

        def halves(n):
            return enumerate(halves_of(shards[n].shape[-1], self.lean))

        def along(turn, n):
            def slot(level):
                return wholes[n].at[y, c, level, x] if n < full else wholes[n].at[level]

            if turn > 0:
                out.landed(("z", n, turn - 1))
            if turn < turns:
                out.chain(("z", n, turn), turn, shards[n], slot)

        def fill(n):
            if n not in filled:
                filled.add(n)
                self.own[n].wait()

        def two(job, n, rows):
            lined = len(shards[n].shape) == 3
            if not lined:
                fill(n)
            for half, (cols, order) in halves(n):
                part = wholes[n].at[y, c, :, x, rows, cols]
                source = shards[n].at[:, rows, cols] if lined else part
                out.go((job, half, 2), order[0], lambda peer: source, lambda step: part)

        def three(job, n, rows):
            fill(n)
            for half, (cols, order) in halves(n):
                out.landed((job, half, 2))
                if order == "xy":
                    part = wholes[n].at[y, c, :, :, rows, cols]
                else:
                    part = wholes[n].at[:, c, :, x, rows, cols]
                out.go((job, half, 3), order[1], lambda peer: part, lambda step: part)

        def four(job, n, rows):
            for half, (cols, order) in halves(n):
                out.landed((job, half, 3))
                part = wholes[n].at[:, c, :, :, rows, cols]
                out.go((job, half, 4), "c", lambda peer: part, lambda step: part)

        def five(job, n, rows):
            for half, _ in halves(n):
                out.landed((job, half, 4))

        steps = iter(range(len(jobs) + 3 * LAG))

        def advance():
            step = next(steps, None)
            if step is not None:
                for stage, late in ((two, 0), (three, LAG), (four, 2 * LAG), (five, 3 * LAG)):
                    if 0 <= step - late < len(jobs):
                        stage(("gather", step - late), *jobs[step - late])

        if raw:
            for time in range(len(raw) + turns):
                for turn in range(turns + 1):
                    if 0 <= time - turn < len(raw):
                        along(turn, raw[time - turn])
                done = time - turns
                if 0 <= done < full:
                    for _ in chunks_of(shards[raw[done]].shape[-2]):
                        advance()
        for _ in range(len(jobs) + 3 * LAG):
            advance()
            feed()
        for n in range(len(shards)):
            fill(n)


def total(values):
    result = values[0].astype(jnp.float32)
    for value in values[1:]:
        result = result + value.astype(jnp.float32)
    return result


class Scatter:
    def __init__(self, place, spot, lean, held, parts, totals, boxes, own_sem):
        self.place, self.spot, self.lean = place, spot, lean
        self.parts, self.totals = parts, totals
        self.full = len(parts) - held
        self.jobs = [
            (n, r)
            for n, p in enumerate(parts)
            if len(p.shape) > 3
            for r in chunks_of(p.shape[-2])
        ]
        self.own_sem = own_sem
        self.sums, self.cores, self.seconds, self.thirds, self.fourths = [], [], [], [], []
        self.results, self.own = [], []
        for n, part in enumerate(parts):
            self.sums.append(boxes.pop(0))
            if len(part.shape) > 3:
                self.cores.append(boxes.pop(0))
                halves = halves_of(part.shape[-1], lean)
                self.seconds.append([boxes.pop(0) for _ in halves])
                self.thirds.append([boxes.pop(0) for _ in halves])
                mine = part.at[:, spot["c"]]
            else:
                for boxed in (self.cores, self.seconds, self.thirds):
                    boxed.append(None)
                mine = part.at[spot["z"]]
            if n < self.full:
                self.fourths.append(boxes.pop(0))
                self.results.append(boxes.pop(0))
            else:
                self.fourths.append(None)
                self.results.append(self.sums[n].at[spot["y"], :, spot["x"]])
            copy = pltpu.make_async_copy(mine, self.sums[n], own_sem[n])
            copy.start()
            self.own.append(copy)

    def run(self, out, feed):
        place, parts, sums = self.place, self.parts, self.sums
        cores, results = self.cores, self.results
        y, c, z, x = (self.spot[k] for k in "yczx")
        lines, _, levels, across = place.grid()
        filled = set()

        def halves(n):
            return enumerate(halves_of(parts[n].shape[-1], self.lean))

        def one(job, n, rows):
            out.go(
                (job, 1),
                "c",
                lambda peer: parts[n].at[:, peer["c"], :, :, rows],
                lambda step: cores[n].at[:, :, :, rows],
            )

        def two(job, n, rows):
            if n not in filled:
                filled.add(n)
                self.own[n].wait()
            out.landed((job, 1))
            if place.cores > 1:

                @pl.loop(0, lines * levels * across)
                def _(at):
                    where = (at // (levels * across), (at // across) % levels, at % across)
                    sums[n][where + (rows,)] = total(
                        [sums[n][where + (rows,)], cores[n][where + (rows,)]]
                    ).astype(sums[n].dtype)

            for half, (cols, order) in halves(n):
                box = self.seconds[n][half]
                if order == "xy":
                    out.go(
                        (job, half, 2),
                        "y",
                        lambda peer: sums[n].at[peer["y"], :, :, rows, cols],
                        lambda step: box.at[step - 1, :, :, rows],
                    )
                else:
                    out.go(
                        (job, half, 2),
                        "x",
                        lambda peer: sums[n].at[:, :, peer["x"], rows, cols],
                        lambda step: box.at[step - 1, :, :, rows],
                    )

        def three(job, n, rows):
            for half, (cols, order) in halves(n):
                out.landed((job, half, 2))
                box, later = self.seconds[n][half], self.thirds[n][half]
                if order == "xy":

                    @pl.loop(0, levels * across)
                    def _(at):
                        zz, xx = at // across, at % across
                        values = [sums[n][y, zz, xx, rows, cols]]
                        values += [box[k, zz, xx, rows] for k in range(lines - 1)]
                        sums[n][y, zz, xx, rows, cols] = total(values).astype(sums[n].dtype)

                    out.go(
                        (job, half, 3),
                        "x",
                        lambda peer: sums[n].at[y, :, peer["x"], rows, cols],
                        lambda step: later.at[step - 1, :, rows],
                    )
                else:

                    @pl.loop(0, lines * levels)
                    def _(at):
                        yy, zz = at // levels, at % levels
                        values = [sums[n][yy, zz, x, rows, cols]]
                        values += [box[k, yy, zz, rows] for k in range(across - 1)]
                        sums[n][yy, zz, x, rows, cols] = total(values).astype(sums[n].dtype)

                    out.go(
                        (job, half, 3),
                        "y",
                        lambda peer: sums[n].at[peer["y"], :, x, rows, cols],
                        lambda step: later.at[step - 1, :, rows],
                    )

        def four(job, n, rows):
            for half, (cols, order) in halves(n):
                out.landed((job, half, 3))
                box = self.thirds[n][half]

                @pl.loop(0, levels)
                def _(zz):
                    values = [sums[n][y, zz, x, rows, cols]]
                    values += [box[k, zz, rows] for k in range(box.shape[0])]
                    sums[n][y, zz, x, rows, cols] = total(values).astype(sums[n].dtype)

            if n < self.full:
                out.go(
                    (job, 4),
                    "z",
                    lambda peer: sums[n].at[y, peer["z"], x, rows],
                    lambda step: self.fourths[n].at[step - 1, rows],
                )

        def five(job, n, rows):
            if n >= self.full:
                return
            out.landed((job, 4))
            values = [sums[n][y, z, x, rows]]
            values += [self.fourths[n][k, rows] for k in range(levels - 1)]
            results[n][rows] = total(values)

        def first(n):
            out.go(
                ("tail", n),
                "z",
                lambda peer: parts[n].at[peer["z"]],
                lambda step: self.fourths[n].at[step - 1],
            )

        def final(n):
            self.own[n].wait()
            out.landed(("tail", n))
            values = [sums[n][...]] + [self.fourths[n][k] for k in range(levels - 1)]
            results[n][...] = total(values)

        jobs = [(("scatter", at),) + job for at, job in enumerate(self.jobs)]
        tails = [n for n, p in enumerate(parts) if len(p.shape) == 3]
        for n in tails:
            first(n)
        lag = LAG if self.lean else 1
        for step in range(len(jobs) + 4 * lag):
            if step > 2 and tails:
                final(tails.pop(0))
            for turn, stage in enumerate((one, two, three, four, five)):
                late = turn * lag
                if 0 <= step - late < len(jobs):
                    stage(*jobs[step - late])
            feed()
        last = []
        for n, result in enumerate(results):
            copy = pltpu.make_async_copy(result, self.totals[n], self.own_sem[n])
            copy.start()
            last.append(copy)
        for copy in last:
            copy.wait()


def scatter_boxes(place, part, lean, held):
    lines, _, levels, across = place.grid()
    rows, cols = part.shape[-2:]
    final = [
        pltpu.VMEM((levels - 1, rows, cols), part.dtype),
        pltpu.VMEM((rows, cols), jnp.float32),
    ]
    if part.ndim == 3:
        return [pltpu.VMEM((rows, cols), part.dtype)] + final
    block = pltpu.VMEM((lines, levels, across, rows, cols), part.dtype)
    first, later = [], []
    for piece, order in halves_of(cols, lean):
        size = (rows, piece.stop - piece.start)
        steps = (lines - 1, across - 1) if order == "xy" else (across - 1, lines - 1)
        middle = (levels, across) if order == "xy" else (lines, levels)
        first.append(pltpu.VMEM((steps[0],) + middle + size, part.dtype))
        later.append(pltpu.VMEM((steps[1], levels) + size, part.dtype))
    return [block, block] + first + later + ([] if held else final)


def move_kernel(place, counts, lean, tails, held, *refs):
    refs = list(refs)
    swaps, gathers, scatters = counts
    whole = swaps + gathers + scatters
    ins, outs, rest = refs[:whole], refs[whole : 2 * whole], refs[2 * whole :]
    own_sem, send_sem, recv_sem = rest[-3:]
    staged = swaps > 0 and whole > swaps
    relays, boxes = rest[: swaps * staged], rest[swaps * staged : -3]
    spot = place.here()
    dp, me = place.device(spot)
    devices = place.levels * place.across
    sent, got = ins[:swaps], outs[:swaps]
    own = []
    for n in range(swaps):
        copy = pltpu.make_async_copy(sent[n].at[me], got[n].at[me], own_sem.at[n])
        copy.start()
        own.append(copy)
    cut = swaps + gathers
    gather = Gather(
        place, spot, lean, tails, ins[swaps:cut], outs[swaps:cut], [own_sem.at[n] for n in range(swaps, cut)]
    )
    scatter = Scatter(
        place, spot, lean, held, ins[cut:], outs[cut:], boxes, [own_sem.at[n] for n in range(cut, whole)]
    )
    place.greet(spot, swaps > 0 and not staged)
    out = Sender(place, spot, send_sem, recv_sem)
    levels, across = place.levels, place.across
    z, x = spot["z"], spot["x"]

    def straight(n):
        for step in range(1, devices):
            peer = lax.rem(me + step, devices)
            out.put("swap", (dp, peer), sent[n].at[peer], got[n].at[me])

    def along_x(n):
        for skip in range(1, across):
            peer = place.shift(spot, "x", skip)
            device = place.device(peer)
            out.put("swap", device, sent[n].at[device[1]], got[n].at[me])
            for step in range(1, levels):
                piece = place.device(place.shift(peer, "z", step))[1]
                out.put(
                    ("relay", n), device, sent[n].at[piece], relays[n].at[skip - 1, step - 1]
                )

    def along_z(n):
        for step in range(1, levels):
            device = place.device(place.shift(spot, "z", step))
            out.put("swap", device, sent[n].at[device[1]], got[n].at[me])

    def pass_on(n):
        out.landed(("relay", n))
        for skip in range(1, across):
            source = place.device(place.shift(spot, "x", across - skip))[1]
            for step in range(1, levels):
                device = place.device(place.shift(spot, "z", step))
                out.put("swap", device, relays[n].at[skip - 1, step - 1], got[n].at[source])

    if staged:
        apart = 2 if gathers else 1
        pending = [[] for _ in range(apart * (swaps - 1) + LAG + 2)]
        for n in range(swaps):
            pending[0 if gathers else max(n - 1, 0)].append((along_z, n))
        for n in range(swaps):
            pending[apart * n].append((along_x, n))
            pending[apart * n + LAG + 1].append((pass_on, n))
    else:
        pending = [[(straight, n)] for n in range(swaps)]

    def feed():
        for act, n in pending.pop(0) if pending else ():
            act(n)

    if gathers:
        gather.run(out, feed)
    if scatters:
        scatter.run(out, feed)
    while pending:
        feed()
    for copy in own:
        copy.wait()
    if swaps:
        out.landed("swap")
    out.finish()


def move(place, collective_id, swaps=(), gathers=(), scatters=(), tails=0, held=0):
    lean = len(swaps) > 0
    lines, cores, levels, across = place.grid()
    copies = len(swaps) * (2 * levels * across - across - 1)
    boxes = []
    if len(swaps) > 0 and len(gathers) + len(scatters) > 0:
        boxes += [pltpu.VMEM((across - 1, levels - 1) + a.shape[1:], a.dtype) for a in swaps]
    shapes = [jax.ShapeDtypeStruct(a.shape, a.dtype) for a in swaps]
    for n, shard in enumerate(gathers):
        rows, cols = shard.shape[-2:]
        if shard.ndim == 2:
            copies += 2 * (levels - 1)
        grid = place.grid()
        if n < len(gathers) - tails:
            count = len(halves_of(cols, lean)) * (across + lines + cores - 3)
            copies += len(chunks_of(rows)) * count
        else:
            grid = (levels,)
        shapes.append(jax.ShapeDtypeStruct(grid + (rows, cols), shard.dtype))
    for n, part in enumerate(scatters):
        rows, cols = part.shape[-2:]
        keeps = n >= len(scatters) - held
        count = 0 if keeps else levels - 1
        if part.ndim > 3:
            count += (cores - 1) + len(halves_of(cols, lean)) * (lines + across - 2)
            count *= len(chunks_of(rows))
        copies += count
        boxes += scatter_boxes(place, part, lean, keeps)
        shapes.append(
            jax.ShapeDtypeStruct((levels, rows, cols), part.dtype)
            if keeps
            else jax.ShapeDtypeStruct((rows, cols), jnp.float32)
        )

    def is_result(a):
        return a.dtype == jnp.float32 and a.shape[-1] > 128

    return pl.pallas_call(
        functools.partial(
            move_kernel, place, (len(swaps), len(gathers), len(scatters)), lean, tails, held
        ),
        out_shape=shapes,
        in_specs=[pl.BlockSpec(memory_space=pl.ANY)] * len(shapes),
        out_specs=[
            pl.BlockSpec(memory_space=pltpu.HBM if is_result(a) else pl.ANY)
            for a in shapes
        ],
        scratch_shapes=boxes
        + [
            pltpu.SemaphoreType.DMA((len(shapes),)),
            pltpu.SemaphoreType.DMA((copies,)),
            pltpu.SemaphoreType.DMA((copies,)),
        ],
        compiler_params=pltpu.CompilerParams(
            collective_id=collective_id,
            has_side_effects=True,
            vmem_limit_bytes=VMEM_BYTES,
        ),
        name=f"move_{collective_id}",
    )(*swaps, *gathers, *scatters)


def side_by_side(ref):
    return jnp.concatenate([ref[s] for s in range(ref.shape[0])], axis=1)


def dot_first(left, right):
    return lax.dot_general(
        left, right, (((0,), (0,)), ((), ())), preferred_element_type=jnp.float32
    )


def dot_last(left, right):
    return lax.dot_general(
        left, right, (((1,), (1,)), ((), ())), preferred_element_type=jnp.float32
    )


def attend_kernel(q_ref, k_ref, v_ref, o_ref, full_ref, sum_ref):
    tokens = q_ref.shape[-1]
    each = ATT_BLOCK // tokens
    keys, values = side_by_side(k_ref), side_by_side(v_ref)
    for block in range(q_ref.shape[0] // each):
        first = block * each
        limit = (block + 1) * ATT_BLOCK
        queries = jnp.concatenate([q_ref[first + s] for s in range(each)], axis=1)
        weights = jnp.exp(dot_first(keys[:, :limit], queries))
        sums = jnp.sum(weights, axis=0, keepdims=True)
        mixed = jnp.dot(
            values[:, :limit],
            weights.astype(jnp.bfloat16),
            preferred_element_type=jnp.float32,
        )
        mixed = mixed / sums
        sum_ref[0, 0, :, pl.ds(block * ATT_BLOCK, ATT_BLOCK)] = sums
        for s in range(each):
            piece = mixed[:, s * tokens : (s + 1) * tokens]
            full_ref[first + s] = piece
            o_ref[first + s] = piece.astype(jnp.bfloat16)


def attend_specs(devices, tokens):
    piece = pl.BlockSpec((devices, HEAD_DIM, tokens), lambda m, h: (0, h, m))
    sums = pl.BlockSpec((1, 1, 1, devices * tokens), lambda m, h: (m, h, 0, 0))
    return piece, sums


def attend(queries, keys, values, tokens):
    devices, rows, cols = queries.shape
    grid = (cols // tokens, rows // HEAD_DIM)
    piece, sums = attend_specs(devices, tokens)
    return pl.pallas_call(
        attend_kernel,
        grid=grid,
        out_shape=[
            jax.ShapeDtypeStruct(queries.shape, jnp.bfloat16),
            jax.ShapeDtypeStruct(queries.shape, jnp.float32),
            jax.ShapeDtypeStruct(grid + (1, devices * tokens), jnp.float32),
        ],
        in_specs=[piece] * 3,
        out_specs=[piece, piece, sums],
        compiler_params=pltpu.CompilerParams(vmem_limit_bytes=VMEM_BYTES),
        name="attend",
    )(queries, keys, values)


def slopes_kernel(
    q_ref, k_ref, v_ref, do_ref, full_ref, sum_ref, rate_ref, dq_ref, dk_ref, dv_ref
):
    tokens = q_ref.shape[-1]
    each = ATT_BLOCK // tokens
    keys, values = side_by_side(k_ref), side_by_side(v_ref)
    rate = rate_ref[...]
    key_total = value_total = None
    for block in reversed(range(q_ref.shape[0] // each)):
        first = block * each
        limit = (block + 1) * ATT_BLOCK

        def pick(ref):
            return jnp.concatenate([ref[first + s] for s in range(each)], axis=1)

        queries = pick(q_ref)
        slope = pick(do_ref).astype(jnp.float32)
        sums = sum_ref[0, 0, :, pl.ds(block * ATT_BLOCK, ATT_BLOCK)]
        scaled = (slope / sums).astype(jnp.bfloat16)
        centre = jnp.sum(slope * pick(full_ref), axis=0, keepdims=True) / sums
        weights = jnp.exp(dot_first(keys[:, :limit], queries))
        dots = dot_first(values[:, :limit], scaled)
        slopes = (weights * (dots - centre)).astype(jnp.bfloat16)
        weights = weights.astype(jnp.bfloat16)
        query_part = jnp.dot(keys[:, :limit], slopes, preferred_element_type=jnp.float32)
        query_part = (query_part * rate).astype(jnp.bfloat16)
        for s in range(each):
            dq_ref[first + s] = query_part[:, s * tokens : (s + 1) * tokens]
        key_part = dot_last(queries, slopes)
        value_part = dot_last(scaled, weights)
        if key_total is None:
            key_total, value_total = key_part, value_part
        else:
            key_total = jnp.concatenate(
                [key_total[:, :limit] + key_part, key_total[:, limit:]], axis=1
            )
            value_total = jnp.concatenate(
                [value_total[:, :limit] + value_part, value_total[:, limit:]], axis=1
            )
    for s in range(q_ref.shape[0]):
        cols = slice(s * tokens, (s + 1) * tokens)
        dk_ref[s] = key_total[:, cols].astype(jnp.bfloat16)
        dv_ref[s] = value_total[:, cols].astype(jnp.bfloat16)


def slopes(queries, keys, values, slope, full, sums, rate, tokens):
    devices, rows, cols = queries.shape
    grid = (cols // tokens, rows // HEAD_DIM)
    piece, sum_spec = attend_specs(devices, tokens)
    return pl.pallas_call(
        slopes_kernel,
        grid=grid,
        out_shape=[jax.ShapeDtypeStruct(queries.shape, jnp.bfloat16)] * 3,
        in_specs=[piece] * 5
        + [sum_spec, pl.BlockSpec((HEAD_DIM, 1), lambda m, h: (0, 0))],
        out_specs=[piece] * 3,
        compiler_params=pltpu.CompilerParams(vmem_limit_bytes=VMEM_BYTES),
        name="slopes",
    )(queries, keys, values, slope, full, sums, rate)


def rms_scale(values):
    return lax.rsqrt(jnp.mean(values * values, axis=-1, keepdims=True) + EPSILON)


def contract(spec, left, right):
    return jnp.einsum(spec, left, right, preferred_element_type=jnp.float32)


def on_device(place, devices, *args):
    inputs, cotangent = args[:2]
    (
        norm_one,
        query_mat,
        query_add,
        key_mat,
        value_mat,
        value_add,
        output_mat,
        output_add,
        norm_two,
        hidden_mat,
        hidden_add,
        project_mat,
        project_add,
    ) = args[2:15]
    depth = args[15].astype(jnp.float32)
    micro, tokens, seqs, width = inputs.shape
    rows = micro * tokens * seqs
    vectors = (norm_one, query_add, value_add, output_add, norm_two, hidden_add, project_add)
    share = norm_one.shape[0]
    small = jnp.pad(jnp.stack(vectors), ((0, 16 - len(vectors)), (0, 128 - share)))
    query_mat, small, key_mat, value_mat, output_mat, hidden_mat, project_mat = move(
        place,
        0,
        gathers=(query_mat, small, key_mat, value_mat, output_mat, hidden_mat, project_mat),
        tails=3,
    )
    small = small.reshape(-1, 16, 128)[:, : len(vectors), :share]
    small = small.transpose(1, 0, 2).reshape(len(vectors), width).astype(jnp.float32)
    gain_one, query_add, value_add, output_add, gain_two, hidden_add, project_add = small
    query_mat, key_mat, value_mat = (
        g.reshape(width, width) for g in (query_mat, key_mat, value_mat)
    )

    def to_rows(array):
        return array.transpose(0, 2, 1, 3).reshape(rows, width)

    def from_rows(array):
        return array.reshape(micro, seqs, tokens, width).transpose(0, 2, 1, 3)

    rate = SOFT_BASE / math.sqrt(HEAD_DIM) * jax.nn.softplus(depth)
    rate_full = jnp.tile(rate, HEADS)[:, None]
    xfloat = to_rows(inputs).astype(jnp.float32)
    inv_one = rms_scale(xfloat)
    normed = (xfloat * inv_one * gain_one).astype(jnp.bfloat16)
    query_pre = contract("df,rd->fr", query_mat, normed) + query_add[:, None]
    queries = (query_pre * rate_full).astype(jnp.bfloat16)
    keys = contract("df,rd->fr", key_mat, normed).astype(jnp.bfloat16)
    values = (contract("df,rd->fr", value_mat, normed) + value_add[:, None]).astype(jnp.bfloat16)

    def split(array):
        return array.reshape(devices, width // devices, rows)

    q_in, k_in, v_in, output_mat, hidden_mat, project_mat = move(
        place,
        1,
        (split(queries), split(keys), split(values)),
        (output_mat, hidden_mat, project_mat),
    )
    output_mat, hidden_mat, project_mat = (
        g.reshape(width, width) for g in (output_mat, hidden_mat, project_mat)
    )
    mixed, full, sums = attend(q_in, k_in, v_in, tokens)
    (mixed,) = move(place, 2, (mixed,))
    mixed = mixed.reshape(width, rows)
    residual = xfloat + (contract("fr,fd->rd", mixed, output_mat) + output_add)
    inv_two = rms_scale(residual)
    second = (residual * inv_two * gain_two).astype(jnp.bfloat16)
    hidden_pre = contract("rd,df->rf", second, hidden_mat) + hidden_add
    active = jax.nn.silu(hidden_pre).astype(jnp.bfloat16)
    result = residual + (contract("rf,fd->rd", active, project_mat) + project_add)
    result = from_rows(result.astype(jnp.bfloat16))

    upper = to_rows(cotangent)
    project_grad = contract("rf,rd->fd", active, upper)
    project_bias_grad = jnp.sum(upper.astype(jnp.float32), axis=0)
    active_grad = contract("rd,fd->rf", upper, project_mat)
    logistic = jax.nn.sigmoid(hidden_pre)
    hidden_grad = (active_grad * logistic * (1.0 + hidden_pre * (1.0 - logistic))).astype(
        jnp.bfloat16
    )
    hidden_mat_grad = contract("rd,rf->df", second, hidden_grad)
    hidden_bias_grad = jnp.sum(hidden_grad.astype(jnp.float32), axis=0)
    second_grad = contract("rf,df->rd", hidden_grad, hidden_mat)
    normal_two = residual * inv_two
    scaled_two = second_grad * gain_two
    norm_two_grad = jnp.sum(second_grad * normal_two, axis=0)
    residual_grad = upper.astype(jnp.float32) + inv_two * (
        scaled_two - normal_two * jnp.mean(scaled_two * normal_two, axis=-1, keepdims=True)
    )
    branch_grad = residual_grad.astype(jnp.bfloat16)
    output_mat_grad = contract("fr,rd->fd", mixed, branch_grad)
    output_bias_grad = jnp.sum(branch_grad.astype(jnp.float32), axis=0)
    mixed_grad = contract("fd,rd->fr", output_mat, branch_grad).astype(jnp.bfloat16)

    def as_parts(*grads):
        return tuple(
            g.astype(jnp.bfloat16).reshape(place.grid() + (share, width)) for g in grads
        )

    merged = share % 8 == 0
    (do_in,) = move(place, 3, (split(mixed_grad),))
    slopes_out = slopes(q_in, k_in, v_in, do_in, full, sums, rate[:, None], tokens)
    early = as_parts(output_mat_grad, hidden_mat_grad, project_grad) if merged else ()
    query_slope, key_grad, value_grad, *early = move(
        place, 4, slopes_out, (), early, held=2 if merged else 0
    )
    query_slope, key_grad, value_grad = (
        a.reshape(width, rows) for a in (query_slope, key_grad, value_grad)
    )
    query_float = query_slope.astype(jnp.float32)
    scale_part = jnp.sum(query_float / rate_full * query_pre, axis=1)
    scale_part = jnp.sum(scale_part.reshape(HEADS, HEAD_DIM), axis=0)
    query_mat_grad = contract("rd,fr->df", normed, query_slope)
    query_bias_grad = jnp.sum(query_float, axis=1)
    key_mat_grad = contract("rd,fr->df", normed, key_grad)
    value_mat_grad = contract("rd,fr->df", normed, value_grad)
    value_bias_grad = jnp.sum(value_grad.astype(jnp.float32), axis=1)
    normed_grad = (
        contract("fr,df->rd", query_slope, query_mat)
        + contract("fr,df->rd", key_grad, key_mat)
        + contract("fr,df->rd", value_grad, value_mat)
    )
    normal_one = xfloat * inv_one
    scaled_one = normed_grad * gain_one
    norm_one_grad = jnp.sum(normed_grad * normal_one, axis=0)
    source_grad = residual_grad + inv_one * (
        scaled_one - normal_one * jnp.mean(scaled_one * normal_one, axis=-1, keepdims=True)
    )
    source_grad = from_rows(source_grad.astype(jnp.bfloat16))

    vector_grads = jnp.stack(
        (
            norm_one_grad,
            query_bias_grad,
            value_bias_grad,
            output_bias_grad,
            norm_two_grad,
            hidden_bias_grad,
            project_bias_grad,
        )
    )
    vector_grads = vector_grads.reshape(7, -1, share).transpose(1, 0, 2)
    vector_grads = jnp.pad(vector_grads, ((0, 0), (0, 0), (0, 128 - share)))
    scale_row = jnp.pad(scale_part, (0, 128 - HEAD_DIM))
    scale_row = jnp.broadcast_to(scale_row, (vector_grads.shape[0], 1, 128))
    vector_grads = jnp.concatenate([vector_grads, scale_row], axis=1)
    vector_grads = vector_grads.reshape(place.grid() + (8, 128))
    late = as_parts(query_mat_grad, key_mat_grad, value_mat_grad)
    if merged:
        output_mat_grad, *early = early
        hidden_mat_grad, project_grad, vector_sums, *late = move(
            place, 5, scatters=(*early, vector_grads, *late)
        )
    else:
        (vector_sums,) = move(place, 5, scatters=(vector_grads,))
        early = as_parts(output_mat_grad, hidden_mat_grad, project_grad)
        early = [move(place, 6, scatters=(p,))[0] for p in early]
        output_mat_grad, hidden_mat_grad, project_grad = early
        late = [move(place, 6, scatters=(p,))[0] for p in late]
    query_mat_grad, key_mat_grad, value_mat_grad = late
    g_one, g_query, g_value, g_output, g_two, g_hidden, g_project = (
        vector_sums[n, :share] for n in range(7)
    )
    scale_summed = vector_sums[7, :HEAD_DIM]
    depth_grad = scale_summed * (SOFT_BASE / math.sqrt(HEAD_DIM)) * jax.nn.sigmoid(depth)
    return (
        result,
        source_grad,
        g_one,
        query_mat_grad,
        g_query,
        key_mat_grad,
        value_mat_grad,
        g_value,
        output_mat_grad,
        g_output,
        g_two,
        hidden_mat_grad,
        g_hidden,
        project_grad,
        g_project,
        depth_grad,
    )


def solution(mesh):
    both = ("dp", "seq")
    token, vector, matrix = P(None, "seq", "dp", None), P(both), P(both, None)
    weights = (
        vector,
        matrix,
        vector,
        matrix,
        matrix,
        vector,
        matrix,
        vector,
        vector,
        matrix,
        vector,
        matrix,
        vector,
    )
    specs = (token, token) + weights + (P(),)
    place = Place(mesh.shape["dp"], mesh.shape["seq"])
    return jax.shard_map(
        functools.partial(on_device, place, mesh.shape["seq"]),
        mesh=mesh,
        in_specs=specs,
        out_specs=specs,
        check_vma=False,
    )
```

```python
import functools
import itertools
import math

import jax
import jax.numpy as jnp
from jax import lax
from jax.experimental import pallas as pl
from jax.experimental.pallas import tpu as pltpu
from jax.sharding import PartitionSpec as P

HEADS = 16
HEAD_DIM = 80
ATT_BLOCK = 256
SOFT_BASE = 1.442695041
EPSILON = 1e-06
MESH = pl.DeviceIdType.MESH
VMEM_BYTES = 60 * 1024 * 1024
LAG = 2


class Place:
    def __init__(self, dp, seq):
        self.cores = 2 if dp % 2 == 0 else 1
        self.lines = dp // self.cores
        self.levels = 4 if seq % 4 == 0 else seq
        self.across = seq // self.levels
        self.sizes = {
            "y": self.lines,
            "c": self.cores,
            "z": self.levels,
            "x": self.across,
        }

    def here(self):
        dp = lax.axis_index("dp")
        seq = lax.axis_index("seq")
        return {
            "y": dp // self.cores,
            "c": dp % self.cores,
            "z": seq // self.across,
            "x": seq % self.across,
        }

    def shift(self, spot, axis, step):
        moved = dict(spot)
        moved[axis] = lax.rem(spot[axis] + step, self.sizes[axis])
        return moved

    def device(self, spot):
        return (
            spot["y"] * self.cores + spot["c"],
            spot["z"] * self.across + spot["x"],
        )

    def grid(self):
        return (self.lines, self.cores, self.levels, self.across)

    def greet(self, spot, wide):
        barrier = pltpu.get_barrier_semaphore()
        dp, seq = self.device(spot)
        peers = [
            self.device(self.shift(spot, axis, step))
            for axis in ("yc" if wide else "zxyc")
            for step in range(1, self.sizes[axis])
        ]
        if wide:
            devices = self.levels * self.across
            peers += [(dp, lax.rem(seq + step, devices)) for step in range(1, devices)]
        for peer in peers:
            pl.semaphore_signal(barrier, inc=1, device_id=peer, device_id_type=MESH)
        pl.semaphore_wait(barrier, len(peers))


def halves_of(cols, lean):
    if lean and cols % 640 == 0:
        cut = cols * 4 // 5
    elif cols % 256 == 0:
        cut = cols // 2
    else:
        return ((slice(0, cols), "xy"),)
    return ((slice(0, cut), "xy"), (slice(cut, cols), "yx"))


def chunks_of(rows, short_last=False):
    if rows % 8 == 0 and rows >= 32:
        cut = rows // 32 * 16
        if short_last:
            cut = rows - cut
        return (slice(0, cut), slice(cut, rows))
    return (slice(0, rows),)


class Sender:
    def __init__(self, place, spot, send_sem, recv_sem):
        self.place = place
        self.spot = spot
        self.send_sem = send_sem
        self.recv_sem = recv_sem
        self.count = itertools.count()
        self.open = {}
        self.every = []

    def put(self, key, device, source, target, leaves=None, comes=None):
        at = next(self.count)
        copy = pltpu.make_async_remote_copy(
            src_ref=source,
            dst_ref=target,
            send_sem=self.send_sem.at[at],
            recv_sem=self.recv_sem.at[at],
            device_id=device,
            device_id_type=MESH,
        )
        self.guard(leaves, copy.start)
        self.open.setdefault(key, []).append((comes, copy))
        self.every.append((leaves, copy))

    def guard(self, when, act):
        if when is None:
            act()
        else:
            pl.when(when)(act)

    def go(self, key, axis, source, target):
        self.open[key] = []
        for step in range(1, self.place.sizes[axis]):
            peer = self.place.shift(self.spot, axis, step)
            self.put(key, self.place.device(peer), source(peer), target(step))

    def chain(self, key, turn, own, slot):
        levels, z = self.place.levels, self.spot["z"]
        self.open[key] = []

        def inside(at):
            return jnp.logical_and(at >= 0, at < levels)

        for way in (1, -1):
            shard, to, back = z - turn * way, z + way, z - (turn + 1) * way
            part = slot(lax.rem(shard + levels, levels))
            peer = dict(self.spot, z=lax.rem(to + levels, levels))
            self.put(
                key,
                self.place.device(peer),
                own if turn == 0 else part,
                part,
                jnp.logical_and(inside(shard), inside(to)),
                inside(back),
            )

    def landed(self, key):
        for comes, copy in self.open[key]:
            self.guard(comes, copy.wait_recv)

    def finish(self):
        for leaves, copy in self.every:
            self.guard(leaves, copy.wait_send)


class Gather:
    def __init__(self, place, spot, lean, tails, shards, wholes, own_sem):
        self.place, self.spot, self.lean, self.tails = place, spot, lean, tails
        self.shards, self.wholes = shards, wholes
        y, c, z, x = (spot[k] for k in "yczx")
        self.own = []
        for n, shard in enumerate(shards):
            if n >= len(shards) - tails:
                target = wholes[n].at[z]
            elif len(shard.shape) == 3:
                target = wholes[n].at[y, c, :, x]
            else:
                target = wholes[n].at[y, c, z, x]
            copy = pltpu.make_async_copy(shard, target, own_sem[n])
            copy.start()
            self.own.append(copy)

    def run(self, out, feed):
        shards, wholes = self.shards, self.wholes
        y, c, _, x = (self.spot[k] for k in "yczx")
        turns = self.place.levels - 1
        full = len(shards) - self.tails
        raw = [n for n, s in enumerate(shards) if len(s.shape) == 2]
        jobs = [(n, r) for n in range(full) for r in chunks_of(shards[n].shape[-2], True)]
        filled = set()

        def halves(n):
            return enumerate(halves_of(shards[n].shape[-1], self.lean))

        def along(turn, n):
            def slot(level):
                return wholes[n].at[y, c, level, x] if n < full else wholes[n].at[level]

            if turn > 0:
                out.landed(("z", n, turn - 1))
            if turn < turns:
                out.chain(("z", n, turn), turn, shards[n], slot)

        def fill(n):
            if n not in filled:
                filled.add(n)
                self.own[n].wait()

        def two(job, n, rows):
            lined = len(shards[n].shape) == 3
            if not lined:
                fill(n)
            for half, (cols, order) in halves(n):
                part = wholes[n].at[y, c, :, x, rows, cols]
                source = shards[n].at[:, rows, cols] if lined else part
                out.go((job, half, 2), order[0], lambda peer: source, lambda step: part)

        def three(job, n, rows):
            fill(n)
            for half, (cols, order) in halves(n):
                out.landed((job, half, 2))
                if order == "xy":
                    part = wholes[n].at[y, c, :, :, rows, cols]
                else:
                    part = wholes[n].at[:, c, :, x, rows, cols]
                out.go((job, half, 3), order[1], lambda peer: part, lambda step: part)

        def four(job, n, rows):
            for half, (cols, order) in halves(n):
                out.landed((job, half, 3))
                part = wholes[n].at[:, c, :, :, rows, cols]
                out.go((job, half, 4), "c", lambda peer: part, lambda step: part)

        def five(job, n, rows):
            for half, _ in halves(n):
                out.landed((job, half, 4))

        steps = iter(range(len(jobs) + 3 * LAG))

        def advance():
            step = next(steps, None)
            if step is not None:
                for stage, late in ((two, 0), (three, LAG), (four, 2 * LAG), (five, 3 * LAG)):
                    if 0 <= step - late < len(jobs):
                        stage(("gather", step - late), *jobs[step - late])

        if raw:
            for time in range(len(raw) + turns):
                for turn in range(turns + 1):
                    if 0 <= time - turn < len(raw):
                        along(turn, raw[time - turn])
                done = time - turns
                if 0 <= done < full:
                    for _ in chunks_of(shards[raw[done]].shape[-2]):
                        advance()
        for _ in range(len(jobs) + 3 * LAG):
            advance()
            feed()
        for n in range(len(shards)):
            fill(n)


def total(values):
    result = values[0].astype(jnp.float32)
    for value in values[1:]:
        result = result + value.astype(jnp.float32)
    return result


class Scatter:
    def __init__(self, place, spot, lean, held, parts, totals, boxes, own_sem):
        self.place, self.spot, self.lean = place, spot, lean
        self.parts, self.totals = parts, totals
        self.full = len(parts) - held
        self.jobs = [
            (n, r)
            for n, p in enumerate(parts)
            if len(p.shape) > 3
            for r in chunks_of(p.shape[-2])
        ]
        self.own_sem = own_sem
        self.sums, self.cores, self.seconds, self.thirds, self.fourths = [], [], [], [], []
        self.results, self.own = [], []
        for n, part in enumerate(parts):
            self.sums.append(boxes.pop(0))
            if len(part.shape) > 3:
                self.cores.append(boxes.pop(0))
                halves = halves_of(part.shape[-1], lean)
                self.seconds.append([boxes.pop(0) for _ in halves])
                self.thirds.append([boxes.pop(0) for _ in halves])
                mine = part.at[:, spot["c"]]
            else:
                for boxed in (self.cores, self.seconds, self.thirds):
                    boxed.append(None)
                mine = part.at[spot["z"]]
            if n < self.full:
                self.fourths.append(boxes.pop(0))
                self.results.append(boxes.pop(0))
            else:
                self.fourths.append(None)
                self.results.append(self.sums[n].at[spot["y"], :, spot["x"]])
            copy = pltpu.make_async_copy(mine, self.sums[n], own_sem[n])
            copy.start()
            self.own.append(copy)

    def run(self, out, feed):
        place, parts, sums = self.place, self.parts, self.sums
        cores, results = self.cores, self.results
        y, c, z, x = (self.spot[k] for k in "yczx")
        lines, _, levels, across = place.grid()
        filled = set()

        def halves(n):
            return enumerate(halves_of(parts[n].shape[-1], self.lean))

        def one(job, n, rows):
            out.go(
                (job, 1),
                "c",
                lambda peer: parts[n].at[:, peer["c"], :, :, rows],
                lambda step: cores[n].at[:, :, :, rows],
            )

        def two(job, n, rows):
            if n not in filled:
                filled.add(n)
                self.own[n].wait()
            out.landed((job, 1))
            if place.cores > 1:

                @pl.loop(0, lines * levels * across)
                def _(at):
                    where = (at // (levels * across), (at // across) % levels, at % across)
                    sums[n][where + (rows,)] = total(
                        [sums[n][where + (rows,)], cores[n][where + (rows,)]]
                    ).astype(sums[n].dtype)

            for half, (cols, order) in halves(n):
                box = self.seconds[n][half]
                if order == "xy":
                    out.go(
                        (job, half, 2),
                        "y",
                        lambda peer: sums[n].at[peer["y"], :, :, rows, cols],
                        lambda step: box.at[step - 1, :, :, rows],
                    )
                else:
                    out.go(
                        (job, half, 2),
                        "x",
                        lambda peer: sums[n].at[:, :, peer["x"], rows, cols],
                        lambda step: box.at[step - 1, :, :, rows],
                    )

        def three(job, n, rows):
            for half, (cols, order) in halves(n):
                out.landed((job, half, 2))
                box, later = self.seconds[n][half], self.thirds[n][half]
                if order == "xy":

                    @pl.loop(0, levels * across)
                    def _(at):
                        zz, xx = at // across, at % across
                        values = [sums[n][y, zz, xx, rows, cols]]
                        values += [box[k, zz, xx, rows] for k in range(lines - 1)]
                        sums[n][y, zz, xx, rows, cols] = total(values).astype(sums[n].dtype)

                    out.go(
                        (job, half, 3),
                        "x",
                        lambda peer: sums[n].at[y, :, peer["x"], rows, cols],
                        lambda step: later.at[step - 1, :, rows],
                    )
                else:

                    @pl.loop(0, lines * levels)
                    def _(at):
                        yy, zz = at // levels, at % levels
                        values = [sums[n][yy, zz, x, rows, cols]]
                        values += [box[k, yy, zz, rows] for k in range(across - 1)]
                        sums[n][yy, zz, x, rows, cols] = total(values).astype(sums[n].dtype)

                    out.go(
                        (job, half, 3),
                        "y",
                        lambda peer: sums[n].at[peer["y"], :, x, rows, cols],
                        lambda step: later.at[step - 1, :, rows],
                    )

        def four(job, n, rows):
            for half, (cols, order) in halves(n):
                out.landed((job, half, 3))
                box = self.thirds[n][half]

                @pl.loop(0, levels)
                def _(zz):
                    values = [sums[n][y, zz, x, rows, cols]]
                    values += [box[k, zz, rows] for k in range(box.shape[0])]
                    sums[n][y, zz, x, rows, cols] = total(values).astype(sums[n].dtype)

            if n < self.full:
                out.go(
                    (job, 4),
                    "z",
                    lambda peer: sums[n].at[y, peer["z"], x, rows],
                    lambda step: self.fourths[n].at[step - 1, rows],
                )

        def five(job, n, rows):
            if n >= self.full:
                return
            out.landed((job, 4))
            values = [sums[n][y, z, x, rows]]
            values += [self.fourths[n][k, rows] for k in range(levels - 1)]
            results[n][rows] = total(values)

        def first(n):
            out.go(
                ("tail", n),
                "z",
                lambda peer: parts[n].at[peer["z"]],
                lambda step: self.fourths[n].at[step - 1],
            )

        def final(n):
            self.own[n].wait()
            out.landed(("tail", n))
            values = [sums[n][...]] + [self.fourths[n][k] for k in range(levels - 1)]
            results[n][...] = total(values)

        jobs = [(("scatter", at),) + job for at, job in enumerate(self.jobs)]
        tails = [n for n, p in enumerate(parts) if len(p.shape) == 3]
        for n in tails:
            first(n)
        lag = LAG if self.lean else 1
        for step in range(len(jobs) + 4 * lag):
            if step > 2 and tails:
                final(tails.pop(0))
            for turn, stage in enumerate((one, two, three, four, five)):
                late = turn * lag
                if 0 <= step - late < len(jobs):
                    stage(*jobs[step - late])
            feed()
        last = []
        for n, result in enumerate(results):
            copy = pltpu.make_async_copy(result, self.totals[n], self.own_sem[n])
            copy.start()
            last.append(copy)
        for copy in last:
            copy.wait()


def scatter_boxes(place, part, lean, held):
    lines, _, levels, across = place.grid()
    rows, cols = part.shape[-2:]
    final = [
        pltpu.VMEM((levels - 1, rows, cols), part.dtype),
        pltpu.VMEM((rows, cols), jnp.float32),
    ]
    if part.ndim == 3:
        return [pltpu.VMEM((rows, cols), part.dtype)] + final
    block = pltpu.VMEM((lines, levels, across, rows, cols), part.dtype)
    first, later = [], []
    for piece, order in halves_of(cols, lean):
        size = (rows, piece.stop - piece.start)
        steps = (lines - 1, across - 1) if order == "xy" else (across - 1, lines - 1)
        middle = (levels, across) if order == "xy" else (lines, levels)
        first.append(pltpu.VMEM((steps[0],) + middle + size, part.dtype))
        later.append(pltpu.VMEM((steps[1], levels) + size, part.dtype))
    return [block, block] + first + later + ([] if held else final)


def move_kernel(place, counts, lean, tails, held, *refs):
    refs = list(refs)
    swaps, gathers, scatters = counts
    whole = swaps + gathers + scatters
    ins, outs, rest = refs[:whole], refs[whole : 2 * whole], refs[2 * whole :]
    own_sem, send_sem, recv_sem = rest[-3:]
    staged = swaps > 0 and whole > swaps
    relays, boxes = rest[: swaps * staged], rest[swaps * staged : -3]
    spot = place.here()
    dp, me = place.device(spot)
    devices = place.levels * place.across
    sent, got = ins[:swaps], outs[:swaps]
    own = []
    for n in range(swaps):
        copy = pltpu.make_async_copy(sent[n].at[me], got[n].at[me], own_sem.at[n])
        copy.start()
        own.append(copy)
    cut = swaps + gathers
    gather = Gather(
        place, spot, lean, tails, ins[swaps:cut], outs[swaps:cut], [own_sem.at[n] for n in range(swaps, cut)]
    )
    scatter = Scatter(
        place, spot, lean, held, ins[cut:], outs[cut:], boxes, [own_sem.at[n] for n in range(cut, whole)]
    )
    place.greet(spot, swaps > 0 and not staged)
    out = Sender(place, spot, send_sem, recv_sem)
    levels, across = place.levels, place.across
    z, x = spot["z"], spot["x"]

    def straight(n):
        for step in range(1, devices):
            peer = lax.rem(me + step, devices)
            out.put("swap", (dp, peer), sent[n].at[peer], got[n].at[me])

    def along_x(n):
        for skip in range(1, across):
            peer = place.shift(spot, "x", skip)
            device = place.device(peer)
            out.put("swap", device, sent[n].at[device[1]], got[n].at[me])
            for step in range(1, levels):
                piece = place.device(place.shift(peer, "z", step))[1]
                out.put(
                    ("relay", n), device, sent[n].at[piece], relays[n].at[skip - 1, step - 1]
                )

    def along_z(n):
        for step in range(1, levels):
            device = place.device(place.shift(spot, "z", step))
            out.put("swap", device, sent[n].at[device[1]], got[n].at[me])

    def pass_on(n):
        out.landed(("relay", n))
        for skip in range(1, across):
            source = place.device(place.shift(spot, "x", across - skip))[1]
            for step in range(1, levels):
                device = place.device(place.shift(spot, "z", step))
                out.put("swap", device, relays[n].at[skip - 1, step - 1], got[n].at[source])

    if staged:
        apart = 2 if gathers else 1
        pending = [[] for _ in range(apart * (swaps - 1) + LAG + 2)]
        for n in range(swaps):
            pending[0 if gathers else max(n - 1, 0)].append((along_z, n))
        for n in range(swaps):
            pending[apart * n].append((along_x, n))
            pending[apart * n + LAG + 1].append((pass_on, n))
    else:
        pending = [[(straight, n)] for n in range(swaps)]

    def feed():
        for act, n in pending.pop(0) if pending else ():
            act(n)

    if gathers:
        gather.run(out, feed)
    if scatters:
        scatter.run(out, feed)
    while pending:
        feed()
    for copy in own:
        copy.wait()
    if swaps:
        out.landed("swap")
    out.finish()


def move(place, collective_id, swaps=(), gathers=(), scatters=(), tails=0, held=0):
    lean = len(swaps) > 0
    lines, cores, levels, across = place.grid()
    copies = len(swaps) * (2 * levels * across - across - 1)
    boxes = []
    if len(swaps) > 0 and len(gathers) + len(scatters) > 0:
        boxes += [pltpu.VMEM((across - 1, levels - 1) + a.shape[1:], a.dtype) for a in swaps]
    shapes = [jax.ShapeDtypeStruct(a.shape, a.dtype) for a in swaps]
    for n, shard in enumerate(gathers):
        rows, cols = shard.shape[-2:]
        if shard.ndim == 2:
            copies += 2 * (levels - 1)
        grid = place.grid()
        if n < len(gathers) - tails:
            count = len(halves_of(cols, lean)) * (across + lines + cores - 3)
            copies += len(chunks_of(rows)) * count
        else:
            grid = (levels,)
        shapes.append(jax.ShapeDtypeStruct(grid + (rows, cols), shard.dtype))
    for n, part in enumerate(scatters):
        rows, cols = part.shape[-2:]
        keeps = n >= len(scatters) - held
        count = 0 if keeps else levels - 1
        if part.ndim > 3:
            count += (cores - 1) + len(halves_of(cols, lean)) * (lines + across - 2)
            count *= len(chunks_of(rows))
        copies += count
        boxes += scatter_boxes(place, part, lean, keeps)
        shapes.append(
            jax.ShapeDtypeStruct((levels, rows, cols), part.dtype)
            if keeps
            else jax.ShapeDtypeStruct((rows, cols), jnp.float32)
        )

    def is_result(a):
        return a.dtype == jnp.float32 and a.shape[-1] > 128

    return pl.pallas_call(
        functools.partial(
            move_kernel, place, (len(swaps), len(gathers), len(scatters)), lean, tails, held
        ),
        out_shape=shapes,
        in_specs=[pl.BlockSpec(memory_space=pl.ANY)] * len(shapes),
        out_specs=[
            pl.BlockSpec(memory_space=pltpu.HBM if is_result(a) else pl.ANY)
            for a in shapes
        ],
        scratch_shapes=boxes
        + [
            pltpu.SemaphoreType.DMA((len(shapes),)),
            pltpu.SemaphoreType.DMA((copies,)),
            pltpu.SemaphoreType.DMA((copies,)),
        ],
        compiler_params=pltpu.CompilerParams(
            collective_id=collective_id,
            has_side_effects=True,
            vmem_limit_bytes=VMEM_BYTES,
        ),
        name=f"move_{collective_id}",
    )(*swaps, *gathers, *scatters)


def side_by_side(ref):
    return jnp.concatenate([ref[s] for s in range(ref.shape[0])], axis=1)


def dot_first(left, right):
    return lax.dot_general(
        left, right, (((0,), (0,)), ((), ())), preferred_element_type=jnp.float32
    )


def dot_last(left, right):
    return lax.dot_general(
        left, right, (((1,), (1,)), ((), ())), preferred_element_type=jnp.float32
    )


def attend_kernel(q_ref, k_ref, v_ref, o_ref, full_ref, sum_ref):
    tokens = q_ref.shape[-1]
    each = ATT_BLOCK // tokens
    keys, values = side_by_side(k_ref), side_by_side(v_ref)
    for block in range(q_ref.shape[0] // each):
        first = block * each
        limit = (block + 1) * ATT_BLOCK
        queries = jnp.concatenate([q_ref[first + s] for s in range(each)], axis=1)
        weights = jnp.exp(dot_first(keys[:, :limit], queries))
        sums = jnp.sum(weights, axis=0, keepdims=True)
        mixed = jnp.dot(
            values[:, :limit],
            weights.astype(jnp.bfloat16),
            preferred_element_type=jnp.float32,
        )
        mixed = mixed / sums
        sum_ref[0, 0, :, pl.ds(block * ATT_BLOCK, ATT_BLOCK)] = sums
        for s in range(each):
            piece = mixed[:, s * tokens : (s + 1) * tokens]
            full_ref[first + s] = piece
            o_ref[first + s] = piece.astype(jnp.bfloat16)


def attend_specs(devices, tokens):
    piece = pl.BlockSpec((devices, HEAD_DIM, tokens), lambda m, h: (0, h, m))
    sums = pl.BlockSpec((1, 1, 1, devices * tokens), lambda m, h: (m, h, 0, 0))
    return piece, sums


def attend(queries, keys, values, tokens):
    devices, rows, cols = queries.shape
    grid = (cols // tokens, rows // HEAD_DIM)
    piece, sums = attend_specs(devices, tokens)
    return pl.pallas_call(
        attend_kernel,
        grid=grid,
        out_shape=[
            jax.ShapeDtypeStruct(queries.shape, jnp.bfloat16),
            jax.ShapeDtypeStruct(queries.shape, jnp.float32),
            jax.ShapeDtypeStruct(grid + (1, devices * tokens), jnp.float32),
        ],
        in_specs=[piece] * 3,
        out_specs=[piece, piece, sums],
        compiler_params=pltpu.CompilerParams(vmem_limit_bytes=VMEM_BYTES),
        name="attend",
    )(queries, keys, values)


def slopes_kernel(
    q_ref, k_ref, v_ref, do_ref, full_ref, sum_ref, rate_ref, dq_ref, dk_ref, dv_ref
):
    tokens = q_ref.shape[-1]
    each = ATT_BLOCK // tokens
    keys, values = side_by_side(k_ref), side_by_side(v_ref)
    rate = rate_ref[...]
    key_total = value_total = None
    for block in reversed(range(q_ref.shape[0] // each)):
        first = block * each
        limit = (block + 1) * ATT_BLOCK

        def pick(ref):
            return jnp.concatenate([ref[first + s] for s in range(each)], axis=1)

        queries = pick(q_ref)
        slope = pick(do_ref).astype(jnp.float32)
        sums = sum_ref[0, 0, :, pl.ds(block * ATT_BLOCK, ATT_BLOCK)]
        scaled = (slope / sums).astype(jnp.bfloat16)
        centre = jnp.sum(slope * pick(full_ref), axis=0, keepdims=True) / sums
        weights = jnp.exp(dot_first(keys[:, :limit], queries))
        dots = dot_first(values[:, :limit], scaled)
        slopes = (weights * (dots - centre)).astype(jnp.bfloat16)
        weights = weights.astype(jnp.bfloat16)
        query_part = jnp.dot(keys[:, :limit], slopes, preferred_element_type=jnp.float32)
        query_part = (query_part * rate).astype(jnp.bfloat16)
        for s in range(each):
            dq_ref[first + s] = query_part[:, s * tokens : (s + 1) * tokens]
        key_part = dot_last(queries, slopes)
        value_part = dot_last(scaled, weights)
        if key_total is None:
            key_total, value_total = key_part, value_part
        else:
            key_total = jnp.concatenate(
                [key_total[:, :limit] + key_part, key_total[:, limit:]], axis=1
            )
            value_total = jnp.concatenate(
                [value_total[:, :limit] + value_part, value_total[:, limit:]], axis=1
            )
    for s in range(q_ref.shape[0]):
        cols = slice(s * tokens, (s + 1) * tokens)
        dk_ref[s] = key_total[:, cols].astype(jnp.bfloat16)
        dv_ref[s] = value_total[:, cols].astype(jnp.bfloat16)


def slopes(queries, keys, values, slope, full, sums, rate, tokens):
    devices, rows, cols = queries.shape
    grid = (cols // tokens, rows // HEAD_DIM)
    piece, sum_spec = attend_specs(devices, tokens)
    return pl.pallas_call(
        slopes_kernel,
        grid=grid,
        out_shape=[jax.ShapeDtypeStruct(queries.shape, jnp.bfloat16)] * 3,
        in_specs=[piece] * 5
        + [sum_spec, pl.BlockSpec((HEAD_DIM, 1), lambda m, h: (0, 0))],
        out_specs=[piece] * 3,
        compiler_params=pltpu.CompilerParams(vmem_limit_bytes=VMEM_BYTES),
        name="slopes",
    )(queries, keys, values, slope, full, sums, rate)


def rms_scale(values):
    return lax.rsqrt(jnp.mean(values * values, axis=-1, keepdims=True) + EPSILON)


def contract(spec, left, right):
    return jnp.einsum(spec, left, right, preferred_element_type=jnp.float32)


def on_device(place, devices, *args):
    inputs, cotangent = args[:2]
    (
        norm_one,
        query_mat,
        query_add,
        key_mat,
        value_mat,
        value_add,
        output_mat,
        output_add,
        norm_two,
        hidden_mat,
        hidden_add,
        project_mat,
        project_add,
    ) = args[2:15]
    depth = args[15].astype(jnp.float32)
    micro, tokens, seqs, width = inputs.shape
    rows = micro * tokens * seqs
    vectors = (norm_one, query_add, value_add, output_add, norm_two, hidden_add, project_add)
    share = norm_one.shape[0]
    small = jnp.pad(jnp.stack(vectors), ((0, 16 - len(vectors)), (0, 128 - share)))
    query_mat, key_mat, value_mat, small, output_mat, hidden_mat, project_mat = move(
        place,
        0,
        gathers=(query_mat, key_mat, value_mat, small, output_mat, hidden_mat, project_mat),
        tails=3,
    )
    small = small.reshape(-1, 16, 128)[:, : len(vectors), :share]
    small = small.transpose(1, 0, 2).reshape(len(vectors), width).astype(jnp.float32)
    gain_one, query_add, value_add, output_add, gain_two, hidden_add, project_add = small
    query_mat, key_mat, value_mat = (
        g.reshape(width, width) for g in (query_mat, key_mat, value_mat)
    )

    def to_rows(array):
        return array.transpose(0, 2, 1, 3).reshape(rows, width)

    def from_rows(array):
        return array.reshape(micro, seqs, tokens, width).transpose(0, 2, 1, 3)

    rate = SOFT_BASE / math.sqrt(HEAD_DIM) * jax.nn.softplus(depth)
    rate_full = jnp.tile(rate, HEADS)[:, None]
    xfloat = to_rows(inputs).astype(jnp.float32)
    inv_one = rms_scale(xfloat)
    normed = (xfloat * inv_one * gain_one).astype(jnp.bfloat16)
    query_pre = contract("df,rd->fr", query_mat, normed) + query_add[:, None]
    queries = (query_pre * rate_full).astype(jnp.bfloat16)
    keys = contract("df,rd->fr", key_mat, normed).astype(jnp.bfloat16)
    values = (contract("df,rd->fr", value_mat, normed) + value_add[:, None]).astype(jnp.bfloat16)

    def split(array):
        return array.reshape(devices, width // devices, rows)

    q_in, k_in, v_in, output_mat, hidden_mat, project_mat = move(
        place,
        1,
        (split(queries), split(keys), split(values)),
        (output_mat, hidden_mat, project_mat),
    )
    output_mat, hidden_mat, project_mat = (
        g.reshape(width, width) for g in (output_mat, hidden_mat, project_mat)
    )
    mixed, full, sums = attend(q_in, k_in, v_in, tokens)
    (mixed,) = move(place, 2, (mixed,))
    mixed = mixed.reshape(width, rows)
    residual = xfloat + (contract("fr,fd->rd", mixed, output_mat) + output_add)
    inv_two = rms_scale(residual)
    second = (residual * inv_two * gain_two).astype(jnp.bfloat16)
    hidden_pre = contract("rd,df->rf", second, hidden_mat) + hidden_add
    active = jax.nn.silu(hidden_pre).astype(jnp.bfloat16)
    result = residual + (contract("rf,fd->rd", active, project_mat) + project_add)
    result = from_rows(result.astype(jnp.bfloat16))

    upper = to_rows(cotangent)
    project_grad = contract("rf,rd->fd", active, upper)
    project_bias_grad = jnp.sum(upper.astype(jnp.float32), axis=0)
    active_grad = contract("rd,fd->rf", upper, project_mat)
    logistic = jax.nn.sigmoid(hidden_pre)
    hidden_grad = (active_grad * logistic * (1.0 + hidden_pre * (1.0 - logistic))).astype(
        jnp.bfloat16
    )
    hidden_mat_grad = contract("rd,rf->df", second, hidden_grad)
    hidden_bias_grad = jnp.sum(hidden_grad.astype(jnp.float32), axis=0)
    second_grad = contract("rf,df->rd", hidden_grad, hidden_mat)
    normal_two = residual * inv_two
    scaled_two = second_grad * gain_two
    norm_two_grad = jnp.sum(second_grad * normal_two, axis=0)
    residual_grad = upper.astype(jnp.float32) + inv_two * (
        scaled_two - normal_two * jnp.mean(scaled_two * normal_two, axis=-1, keepdims=True)
    )
    branch_grad = residual_grad.astype(jnp.bfloat16)
    output_mat_grad = contract("fr,rd->fd", mixed, branch_grad)
    output_bias_grad = jnp.sum(branch_grad.astype(jnp.float32), axis=0)
    mixed_grad = contract("fd,rd->fr", output_mat, branch_grad).astype(jnp.bfloat16)

    def as_parts(*grads):
        return tuple(
            g.astype(jnp.bfloat16).reshape(place.grid() + (share, width)) for g in grads
        )

    merged = share % 8 == 0
    (do_in,) = move(place, 3, (split(mixed_grad),))
    slopes_out = slopes(q_in, k_in, v_in, do_in, full, sums, rate[:, None], tokens)
    early = as_parts(output_mat_grad, hidden_mat_grad, project_grad) if merged else ()
    query_slope, key_grad, value_grad, *early = move(
        place, 4, slopes_out, (), early, held=2 if merged else 0
    )
    query_slope, key_grad, value_grad = (
        a.reshape(width, rows) for a in (query_slope, key_grad, value_grad)
    )
    query_float = query_slope.astype(jnp.float32)
    scale_part = jnp.sum(query_float / rate_full * query_pre, axis=1)
    scale_part = jnp.sum(scale_part.reshape(HEADS, HEAD_DIM), axis=0)
    query_mat_grad = contract("rd,fr->df", normed, query_slope)
    query_bias_grad = jnp.sum(query_float, axis=1)
    key_mat_grad = contract("rd,fr->df", normed, key_grad)
    value_mat_grad = contract("rd,fr->df", normed, value_grad)
    value_bias_grad = jnp.sum(value_grad.astype(jnp.float32), axis=1)
    normed_grad = (
        contract("fr,df->rd", query_slope, query_mat)
        + contract("fr,df->rd", key_grad, key_mat)
        + contract("fr,df->rd", value_grad, value_mat)
    )
    normal_one = xfloat * inv_one
    scaled_one = normed_grad * gain_one
    norm_one_grad = jnp.sum(normed_grad * normal_one, axis=0)
    source_grad = residual_grad + inv_one * (
        scaled_one - normal_one * jnp.mean(scaled_one * normal_one, axis=-1, keepdims=True)
    )
    source_grad = from_rows(source_grad.astype(jnp.bfloat16))

    vector_grads = jnp.stack(
        (
            norm_one_grad,
            query_bias_grad,
            value_bias_grad,
            output_bias_grad,
            norm_two_grad,
            hidden_bias_grad,
            project_bias_grad,
        )
    )
    vector_grads = vector_grads.reshape(7, -1, share).transpose(1, 0, 2)
    vector_grads = jnp.pad(vector_grads, ((0, 0), (0, 0), (0, 128 - share)))
    scale_row = jnp.pad(scale_part, (0, 128 - HEAD_DIM))
    scale_row = jnp.broadcast_to(scale_row, (vector_grads.shape[0], 1, 128))
    vector_grads = jnp.concatenate([vector_grads, scale_row], axis=1)
    vector_grads = vector_grads.reshape(place.grid() + (8, 128))
    late = as_parts(query_mat_grad, key_mat_grad, value_mat_grad)
    if merged:
        output_mat_grad, *early = early
        hidden_mat_grad, project_grad, *late, vector_sums = move(
            place, 5, scatters=(*early, *late, vector_grads)
        )
    else:
        (vector_sums,) = move(place, 5, scatters=(vector_grads,))
        early = as_parts(output_mat_grad, hidden_mat_grad, project_grad)
        early = [move(place, 6, scatters=(p,))[0] for p in early]
        output_mat_grad, hidden_mat_grad, project_grad = early
        late = [move(place, 6, scatters=(p,))[0] for p in late]
    query_mat_grad, key_mat_grad, value_mat_grad = late
    g_one, g_query, g_value, g_output, g_two, g_hidden, g_project = (
        vector_sums[n, :share] for n in range(7)
    )
    scale_summed = vector_sums[7, :HEAD_DIM]
    depth_grad = scale_summed * (SOFT_BASE / math.sqrt(HEAD_DIM)) * jax.nn.sigmoid(depth)
    return (
        result,
        source_grad,
        g_one,
        query_mat_grad,
        g_query,
        key_mat_grad,
        value_mat_grad,
        g_value,
        output_mat_grad,
        g_output,
        g_two,
        hidden_mat_grad,
        g_hidden,
        project_grad,
        g_project,
        depth_grad,
    )


def solution(mesh):
    both = ("dp", "seq")
    token, vector, matrix = P(None, "seq", "dp", None), P(both), P(both, None)
    weights = (
        vector,
        matrix,
        vector,
        matrix,
        matrix,
        vector,
        matrix,
        vector,
        vector,
        matrix,
        vector,
        matrix,
        vector,
    )
    specs = (token, token) + weights + (P(),)
    place = Place(mesh.shape["dp"], mesh.shape["seq"])
    return jax.shard_map(
        functools.partial(on_device, place, mesh.shape["seq"]),
        mesh=mesh,
        in_specs=specs,
        out_specs=specs,
        check_vma=False,
    )
```
